32 devices in a mesh: dp: 2 (over x), row: 4 (over z), col: 4 (over y, core).
Axes of the slice: x: 2, y: 2, z: 4, core: 2. Of those that a mesh axis runs over, the one named last changes fastest.
Arguments:
- x_in: bfloat16 [4, 1024, 2560], P('dp', None, ('row', 'col')), parts along dimension 0
- ln_gain: bfloat16 [2, 2560], P(None, ('row', 'col'))
- w_in: bfloat16 [2, 2560, 23040], P(None, 'row', 'col')
- w_kv: bfloat16 [2, 2560, 160], P(None, 'row', 'col')
- w_out: bfloat16 [2, 12800, 2560], P(None, 'col', 'row')
Outputs:
- output 1: bfloat16 [4, 1024, 2560], P('dp', None, ('row', 'col')), parts along dimension 0
- output 2: bfloat16 [2, 2, 4, 1024, 80], P(None, None, 'dp', ('row', 'col')), parts along dimension 2
There are 2 independent parts. The reference program is written for one: setup_inputs(seed, part) draws one part's arguments, and reference() takes and returns one part's arrays. A program takes and returns all parts, laid end to end along the dimension named above; an argument that names none is the same for every part.
All inputs are finite; a program needn't handle non-finite values.
Results may differ from the reference program's by a relative error of at most 0.015362.
Values are sent between devices in bfloat16 or wider.
A program may use at most 1 GiB of HBM per device.

```python
import jax
import jax.numpy as jnp
from jax import lax

D_MODEL = 2560
HEADS = 32
HEAD_DIM = 80
FF_WIDTH = 10240
BATCH = 2
SEQ_LEN = 1024
COL_SHARDS = 4
LAYERS = 2

LN_EPS = 1e-6
E_WIDTH = HEADS * HEAD_DIM + 2 * FF_WIDTH
R_WIDTH = HEADS * HEAD_DIM + FF_WIDTH
E_BLOCK = E_WIDTH // COL_SHARDS
Q_BLOCK = HEADS * HEAD_DIM // COL_SHARDS
F_BLOCK = FF_WIDTH // COL_SHARDS
HALF_DIM = HEAD_DIM // 2


def setup_inputs(seed: int = 0, part: int = 0) -> dict:
    root_key = jax.random.key(seed)
    shared_root, part_root = jax.random.split(root_key)
    part_key = jax.random.fold_in(part_root, part)
    key_x, key_off = jax.random.split(part_key)
    key_g, key_in, key_kv, key_out = jax.random.split(shared_root, 4)
    slope_part = 2.0 * (jnp.arange(D_MODEL, dtype=jnp.float32) / D_MODEL - 0.5)
    offset = slope_part + 0.5 * jax.random.normal(key_off, (D_MODEL,), jnp.float32)
    x_in = (jax.random.normal(key_x, (BATCH, SEQ_LEN, D_MODEL), jnp.float32) + offset).astype(jnp.bfloat16)
    ln_gain = (1.0 + 0.3 * jax.random.normal(key_g, (LAYERS, D_MODEL), jnp.float32)).astype(jnp.bfloat16)
    w_in = (jax.random.normal(key_in, (LAYERS, D_MODEL, E_WIDTH), jnp.float32) * D_MODEL ** -0.5).astype(jnp.bfloat16)
    w_kv = (jax.random.normal(key_kv, (LAYERS, D_MODEL, 2 * HEAD_DIM), jnp.float32) * D_MODEL ** -0.5).astype(jnp.bfloat16)
    w_out = (jax.random.normal(key_out, (LAYERS, R_WIDTH, D_MODEL), jnp.float32) * R_WIDTH ** -0.5).astype(jnp.bfloat16)
    return {"x_in": x_in, "ln_gain": ln_gain, "w_in": w_in, "w_kv": w_kv, "w_out": w_out}


def layer_norm(hidden, gain_row):
    hidden_f32 = hidden.astype(jnp.float32)
    mean_val = jnp.mean(hidden_f32, axis=-1, keepdims=True)
    centered = hidden_f32 - mean_val
    variance = jnp.mean(centered * centered, axis=-1, keepdims=True)
    return (centered * lax.rsqrt(variance + LN_EPS) * gain_row.astype(jnp.float32)).astype(jnp.bfloat16)


def rope_tables(positions):
    inv_freq = 1.0 / (10000.0 ** (jnp.arange(HALF_DIM, dtype=jnp.float32) * 2.0 / HEAD_DIM))
    angles = positions.astype(jnp.float32)[:, None] * inv_freq[None, :]
    return jnp.cos(angles), jnp.sin(angles)


def apply_rope(values, cos_tab, sin_tab):
    lower_half = values[..., :HALF_DIM]
    upper_half = values[..., HALF_DIM:]
    return jnp.concatenate([lower_half * cos_tab - upper_half * sin_tab, upper_half * cos_tab + lower_half * sin_tab], axis=-1)


def one_layer(hidden, params):
    gain_row, w_in_layer, w_kv_layer, w_out_layer = params
    normed = layer_norm(hidden, gain_row)
    projected = jnp.dot(normed, w_in_layer, preferred_element_type=jnp.float32).astype(jnp.bfloat16).reshape(SEQ_LEN, COL_SHARDS, E_BLOCK)
    kv_proj = jnp.dot(normed, w_kv_layer, preferred_element_type=jnp.float32).astype(jnp.bfloat16)
    query = projected[:, :, :Q_BLOCK].reshape(SEQ_LEN, HEADS, HEAD_DIM)
    gate_val = projected[:, :, Q_BLOCK:Q_BLOCK + F_BLOCK]
    up_val = projected[:, :, Q_BLOCK + F_BLOCK:]
    positions = jnp.arange(SEQ_LEN)
    cos_tab, sin_tab = rope_tables(positions)
    q_rot = (apply_rope(query.astype(jnp.float32), cos_tab[:, None, :], sin_tab[:, None, :]) * HEAD_DIM ** -0.5).astype(jnp.bfloat16)
    k_rot = apply_rope(kv_proj[:, :HEAD_DIM].astype(jnp.float32), cos_tab, sin_tab).astype(jnp.bfloat16)
    v_val = kv_proj[:, HEAD_DIM:]
    scores = jnp.einsum("qhd,kd->hqk", q_rot.astype(jnp.float32), k_rot.astype(jnp.float32))
    causal = positions[None, :] <= positions[:, None]
    scores = jnp.where(causal[None, :, :], scores, -1e30)
    attn_prob = jax.nn.softmax(scores, axis=-1).astype(jnp.bfloat16)
    attn_out = jnp.einsum("hqk,kd->qhd", attn_prob.astype(jnp.float32), v_val.astype(jnp.float32)).astype(jnp.bfloat16)
    mlp_out = (jax.nn.silu(gate_val.astype(jnp.float32)) * up_val.astype(jnp.float32)).astype(jnp.bfloat16)
    joined = jnp.concatenate([attn_out.reshape(SEQ_LEN, COL_SHARDS, Q_BLOCK), mlp_out], axis=2).reshape(SEQ_LEN, R_WIDTH)
    update = jnp.dot(joined, w_out_layer, preferred_element_type=jnp.float32).astype(jnp.bfloat16)
    return hidden + update, jnp.stack([k_rot, v_val])


def reference(x_in, ln_gain, w_in, w_kv, w_out):
    def one_sequence(seq_x):
        return lax.scan(one_layer, seq_x, (ln_gain, w_in, w_kv, w_out))
    y_out, kv_all = lax.map(one_sequence, x_in)
    return y_out, jnp.transpose(kv_all, (1, 2, 0, 3, 4))
```

```python
import functools

import jax
import jax.numpy as jnp
from jax import lax
from jax.experimental import pallas as pl
from jax.experimental.pallas import tpu as pltpu
from jax.sharding import PartitionSpec as P

BF = jnp.bfloat16
F32 = jnp.float32
MESH_ID = pl.DeviceIdType.MESH
LN_EPS = 1e-6

D = 2560
SH = 160
RW = 640
FB = 640
HD = 80
HALF = HD // 2
SEQ = 1024
T = 2 * SEQ
CW = 512
NT = T // CW
NE = 512 // CW
NC = NE + NT
GP = 4
GR = RW // GP
QB = 256


def rope_tables():
    inv_freq = 1.0 / (10000.0 ** (jnp.arange(HALF, dtype=F32) * 2.0 / HD))
    angles = inv_freq[:, None] * jnp.arange(SEQ).astype(F32)[None, :]
    return jnp.stack([jnp.cos(angles), jnp.sin(angles)])


def dot_ta(a, b):
    return lax.dot_general(a, b, (((0,), (0,)), ((), ())), preferred_element_type=F32)


def kernel(xin, wq, w_in, w_out, cs, yT, kvo, XA, GU, WQ, WKV, WO, GB, MT, QT, KT, VT, XO, RC, RY, RU, RD, SC, SY, SZ,
           zsu, zsd, ysn, csn, zrc, yrc, crc, rcs, rcr, rys, ryr, rzu, rzd, rsu, rsd, ws, wr, xs, xr, own):
    x = lax.axis_index("dp")
    z = lax.axis_index("row")
    c = lax.axis_index("col")
    y, k = c // 2, lax.rem(c, 2)
    me = 4 * z + c
    up = (x, jnp.minimum(z + 1, 3), c)
    down = (x, jnp.maximum(z - 1, 0), c)
    ypeer = (x, z, lax.rem(c + 2, 4))
    cpeer = (x, z, c + 1 - 2 * k)
    xpeer = (1 - x, z, c)
    zpeer = [(x, lax.rem(z + h, 4), c) for h in (1, 2, 3)]

    def rcopy(src, dst, ss, rs, dev):
        return pltpu.make_async_remote_copy(src_ref=src, dst_ref=dst, send_sem=ss, recv_sem=rs, device_id=dev, device_id_type=MESH_ID)

    def wait_for(ref, sem):
        pltpu.make_async_copy(ref, ref, sem).wait()

    def rows(s):
        return pl.ds(pl.multiple_of(s * SH, SH), SH)

    def loop(n, body):
        def step(i, carry):
            body(i)
            return carry
        lax.fori_loop(0, n, step, 0)

    barrier = pltpu.get_barrier_semaphore()
    for dev in zpeer + [ypeer, cpeer, xpeer]:
        pl.semaphore_signal(barrier, inc=1, device_id=dev, device_id_type=MESH_ID)
    pl.semaphore_wait(barrier, 6)

    def act(ch, s):
        return XA.at[ch, rows(s)]

    def ext(ch, s):
        i = 16 * ch + s
        return MT.at[i // 5, rows(lax.rem(i, 5))]

    def gather_own(src, buf, ch, o):
        q = ch + o
        dst = buf(ch, me)

        @pl.when(z < 3)
        def _():
            rcopy(src, dst, zsu.at[q], zrc.at[q, 0, 0], up).start()

        @pl.when(z > 0)
        def _():
            rcopy(src, dst, zsd.at[q], zrc.at[q, 1, 0], down).start()

        rcopy(src, dst, ysn.at[q], yrc.at[q], ypeer).start()
        rcopy(src, dst, csn.at[q], crc.at[q], cpeer).start()

    def gather_hop(buf, ch, o, hop):
        q = ch + o

        @pl.when(z - hop >= 0)
        def _():
            ref = buf(ch, jnp.maximum(me - 4 * hop, 0))
            wait_for(ref, zrc.at[q, 0, hop - 1])
            if hop < 3:
                @pl.when(z < 3)
                def _():
                    rcopy(ref, ref, zsu.at[q], zrc.at[q, 0, hop], up).start()
            rcopy(ref, ref, ysn.at[q], yrc.at[q], ypeer).start()
            rcopy(ref, ref, csn.at[q], crc.at[q], cpeer).start()

        @pl.when(z + hop <= 3)
        def _():
            ref = buf(ch, jnp.minimum(me + 4 * hop, 15))
            wait_for(ref, zrc.at[q, 1, hop - 1])
            if hop < 3:
                @pl.when(z > 0)
                def _():
                    rcopy(ref, ref, zsd.at[q], zrc.at[q, 1, hop], down).start()
            rcopy(ref, ref, ysn.at[q], yrc.at[q], ypeer).start()
            rcopy(ref, ref, csn.at[q], crc.at[q], cpeer).start()

    def gather_cross(buf, ch, o):
        q = ch + o
        wait_for(XA.at[0, pl.ds(0, 4 * SH)], yrc.at[q])
        for zz in range(4):
            ref = buf(ch, 4 * zz + lax.rem(c + 2, 4))
            rcopy(ref, ref, csn.at[q], crc.at[q], cpeer).start()

    def gather_end(buf, ch, o):
        q = ch + o
        wait_for(XA.at[0, pl.ds(0, 8 * SH)], crc.at[q])
        for zz in range(3):
            @pl.when(z == zz)
            def _():
                wait_for(XA.at[0, pl.ds(0, (zz + 1) * SH)], zsu.at[q])

            @pl.when(z == 3 - zz)
            def _():
                wait_for(XA.at[0, pl.ds(0, (zz + 1) * SH)], zsd.at[q])
        wait_for(XA.at[0, pl.ds(0, 4 * SH)], ysn.at[q])
        wait_for(XA.at[0, pl.ds(0, 8 * SH)], csn.at[q])

    NPC = GP + 3

    def lane(zz):
        return pl.ds(pl.multiple_of(zz * RW, 128), RW)

    def w_ref(l, p, zz, half):
        if p == 0:
            return WQ.at[l, pl.ds(pl.multiple_of(80 * half, 16), 80), lane(zz)]
        if p <= GP:
            return GU.at[l, half, pl.ds(pl.multiple_of(zz * RW + GR * (p - 1), 16), GR), :]
        if p == GP + 1:
            return WO.at[l, pl.ds(pl.multiple_of(400 * half, 16), 160), lane(zz)]
        return WO.at[l, pl.ds(pl.multiple_of(160 + 400 * half, 16), 240), lane(zz)]

    def w_src(l, p, t):
        if p == 0:
            return wq.at[l, pl.ds(pl.multiple_of(SH * t + 80 * x, 16), 80), :]
        if p <= GP:
            return w_in.at[l, pl.ds(GR * (p - 1), GR), pl.ds(pl.multiple_of(RW + D * x + FB * t, 128), FB)]
        if p == GP + 1:
            row = jnp.where(x == 0, SH * t, RW + FB * t + 240)
            return w_out.at[l, pl.ds(pl.multiple_of(row, 16), 160), :]
        return w_out.at[l, pl.ds(pl.multiple_of(RW + FB * t + 400 * x, 16), 240), :]

    def w_send(l, p):
        for h in (1, 2, 3):
            t = lax.rem(z + h, 4)
            rcopy(w_src(l, p, t), w_ref(l, p, z, x), ws.at[l, p], wr.at[l, p, h - 1], zpeer[h - 1]).start()

    def w_forward(l, p):
        for h in (1, 2, 3):
            ref = w_ref(l, p, lax.rem(z - h + 4, 4), x)
            wait_for(ref, wr.at[l, p, h - 1])
            rcopy(ref, ref, xs.at[l, p], xr.at[l, p], xpeer).start()

    def w_size(l, p):
        if p == 0:
            return WQ.at[l, pl.ds(0, 80), pl.ds(0, 3 * RW)]
        if p <= GP:
            return GU.at[l, 0, pl.ds(0, 3 * GR), :]
        if p == GP + 1:
            return WO.at[l, pl.ds(0, 160), pl.ds(0, 3 * RW)]
        return WO.at[l, pl.ds(0, 240), pl.ds(0, 3 * RW)]

    def w_arrive(l, p):
        wait_for(w_size(l, p), xr.at[l, p])

    def w_own(l):
        return [
            pltpu.make_async_copy(wq.at[l, pl.ds(pl.multiple_of(SH * z, 16), SH), :], WQ.at[l, :, lane(z)], own.at[l, 0]),
            pltpu.make_async_copy(w_in.at[l, :, pl.ds(pl.multiple_of(RW + FB * z, 128), FB)], GU.at[l, 0, pl.ds(pl.multiple_of(z * RW, 16), RW), :], own.at[l, 1]),
            pltpu.make_async_copy(w_in.at[l, :, pl.ds(pl.multiple_of(RW + D + FB * z, 128), FB)], GU.at[l, 1, pl.ds(pl.multiple_of(z * RW, 16), RW), :], own.at[l, 2]),
            pltpu.make_async_copy(w_out.at[l, pl.ds(pl.multiple_of(SH * z, 16), SH), :], WO.at[l, pl.ds(0, SH), lane(z)], own.at[l, 3]),
            pltpu.make_async_copy(w_out.at[l, pl.ds(pl.multiple_of(RW + FB * z, 16), FB), :], WO.at[l, pl.ds(SH, FB), lane(z)], own.at[l, 4]),
        ]

    for ch in range(NE):
        gather_own(xin.at[ch], ext, ch, 0)
    for ch in range(NT):
        gather_own(xin.at[NE + ch], act, ch, NE)
    for ch in range(NE):
        ext(ch, me)[...] = xin[ch]

    def put_own(ch):
        XA[ch, rows(me)] = xin[NE + ch]
    loop(NT, put_own)
    w_send(0, 0)
    w_send(0, 1)
    for l in range(2):
        for cp in w_own(l):
            cp.start()
    for hop in (1, 2, 3):
        loop(NE, lambda ch: gather_hop(ext, ch, 0, hop))
    loop(NE, lambda ch: gather_cross(ext, ch, 0))

    def unpack():
        loop(NE, lambda ch: gather_end(ext, ch, 0))

        def shard(s):
            zz, cc = s // 4, lax.rem(s, 4)
            for b in range(5):
                lo = 128 * (b // 2)
                i = 16 * (lo // CW) + s
                blk = MT[i // 5, pl.ds(pl.multiple_of(lax.rem(i, 5) * SH + 80 * (b % 2), 16), 80), lo % CW:lo % CW + 128].astype(F32)
                for l in range(2):
                    WKV[l, pl.ds(pl.multiple_of(48 * cc, 16), 40), pl.ds(pl.multiple_of(zz * RW + 128 * b, 128), 128)] = blk[40 * l:40 * l + 40].astype(BF)
            i = 16 * (NE - 1) + s
            blk = MT[i // 5, rows(lax.rem(i, 5)), CW - 128:CW].astype(F32)
            for l in range(2):
                GB[l, rows(s), :] = jnp.broadcast_to(blk[:, l:l + 1], (SH, 128)).astype(BF)
        loop(16, shard)
        for l in range(2):
            for cc in range(4):
                WKV[l, 48 * cc + 40:48 * cc + 48, :] = jnp.zeros((8, D), BF)

    BR = 32

    def norm(l, n):
        def fold(v):
            return v.reshape(BR // 8, 8, CW).sum(0)

        def load(i):
            return XA[n, pl.ds(pl.multiple_of(i * BR, BR), BR), :].astype(F32)

        tot = lax.fori_loop(0, D // BR, lambda i, a: a + fold(load(i)), jnp.zeros((8, CW), F32), unroll=4)
        mean = jnp.sum(tot, axis=0, keepdims=True) / D

        def square(i, a):
            d = load(i) - mean
            return a + fold(d * d)
        var = jnp.sum(lax.fori_loop(0, D // BR, square, jnp.zeros((8, CW), F32), unroll=4), axis=0, keepdims=True) / D
        scale = lax.rsqrt(var + LN_EPS)

        def put(i, a):
            g = jnp.concatenate([GB[l, pl.ds(pl.multiple_of(i * BR, BR), BR), :].astype(F32)] * (CW // 128), axis=1)
            XA[n, pl.ds(pl.multiple_of(i * BR, BR), BR), :] = ((load(i) - mean) * scale * g).astype(BF)
            return a
        lax.fori_loop(0, D // BR, put, 0, unroll=4)

    def tok(n):
        return pl.ds(pl.multiple_of(n * CW, 128), CW)

    def qkv(l, n):
        pos = pl.ds(pl.multiple_of(lax.rem(n * CW, SEQ), 128), CW)
        co, si = cs[0, :, pos], cs[1, :, pos]
        h = XA[n]
        kv = jnp.dot(WKV[l], h, preferred_element_type=F32).astype(BF).astype(F32)

        def rot(lo, hi):
            return jnp.concatenate([lo * co - hi * si, hi * co + lo * si], axis=0)
        KT[:, tok(n)] = rot(kv[0:40], kv[48:88]).astype(BF)
        VT[:, tok(n)] = jnp.concatenate([kv[96:136], kv[144:184]], axis=0).astype(BF)
        qq = jnp.dot(WQ[l], h, preferred_element_type=F32).astype(BF).astype(F32)
        for hd in range(2):
            QT[HD * hd:HD * hd + HD, tok(n)] = (rot(qq[HD * hd:HD * hd + HALF], qq[HD * hd + HALF:HD * hd + HD]) * HD ** -0.5).astype(BF)

    def attention():
        def body(bh):
            b, hd = bh // 2, lax.rem(bh, 2)
            hr = pl.ds(pl.multiple_of(hd * HD, 16), HD)
            for i in range(SEQ // QB):
                nk = QB * (i + 1)
                ks = pl.ds(pl.multiple_of(b * SEQ, 128), nk)
                qs = pl.ds(pl.multiple_of(b * SEQ + QB * i, 128), QB)
                s = dot_ta(KT[:, ks], QT[hr, qs])
                keep = lax.broadcasted_iota(jnp.int32, (QB, QB), 0) <= lax.broadcasted_iota(jnp.int32, (QB, QB), 1)
                last = jnp.where(keep, s[nk - QB:], -1e30)
                s = jnp.concatenate([s[:nk - QB], last], axis=0) if i else last
                e = jnp.exp(s - jnp.max(s, axis=0, keepdims=True))
                pr = (e * (1.0 / jnp.sum(e, axis=0, keepdims=True))).astype(BF)
                MT[b * (SEQ // CW) + QB * i // CW, hr, QB * i % CW:QB * i % CW + QB] = jnp.dot(VT[:, ks], pr, preferred_element_type=F32).astype(BF)
        loop(4, body)

    def gate_up(l, n):
        h = XA[n]
        g = dot_ta(GU[l, 0], h).astype(BF).astype(F32)
        u = dot_ta(GU[l, 1], h).astype(BF).astype(F32)
        MT[n, SH:SH + FB, :] = (g * lax.logistic(g) * u).astype(BF)

    def f(ref_value):
        return ref_value.astype(F32)

    def red_a(l, n):
        m = MT[n]
        slot = lax.rem(n, 2)

        @pl.when(n >= 2)
        def _():
            wait_for(RC.at[0], rcs.at[n - 2])

        def blk(zz):
            XA[n, pl.ds(pl.multiple_of(zz * RW, RW), RW), :] = dot_ta(WO[l, :, lane(zz)], m).astype(BF)
            for yy in range(2):
                SC[slot, 2 * zz + yy] = XA[n, rows(4 * zz + 2 * yy + 1 - k)]
                rcopy(SC.at[slot, 2 * zz + yy], RC.at[n, 2 * zz + yy], rcs.at[n], rcr.at[n], cpeer).start()
        loop(4, blk)

    def red_b(n):
        slot = lax.rem(n, 2)
        wait_for(RC.at[n], rcr.at[n])

        @pl.when(n >= 2)
        def _():
            wait_for(RY.at[0], rys.at[n - 2])

        for zz in (3, 0, 2, 1):
            SY[slot, zz] = (f(XA[n, rows(4 * zz + 2 * (1 - y) + k)]) + f(RC[n, 2 * zz + 1 - y])).astype(BF)
            rcopy(SY.at[slot, zz], RY.at[n, zz], rys.at[n], ryr.at[n], ypeer).start()

    def red_c(n):
        wait_for(RY.at[n], ryr.at[n])

        def part(zz):
            return f(XA[n, rows(4 * zz + c)]) + f(RC[n, 2 * zz + y]) + f(RY[n, zz])

        for zz in (3, 0, 2, 1):
            SZ[n, zz] = part(zz).astype(BF)

        @pl.when(z == 0)
        def _():
            for zz in (3, 2, 1):
                send_up(n, zz)

        @pl.when(z == 3)
        def _():
            for zz in (0, 1, 2):
                send_down(n, zz)

    def send_up(n, zz):
        rcopy(SZ.at[n, zz], RU.at[n, zz - 1], rsu.at[n], rzu.at[n, zz - 1], up).start()

    def send_down(n, zz):
        rcopy(SZ.at[n, zz], RD.at[n, zz], rsd.at[n], rzd.at[n, zz], down).start()

    def relay_up(n, zz):
        wait_for(RU.at[n, zz - 1], rzu.at[n, zz - 1])
        SZ[n, zz] = (f(SZ[n, zz]) + f(RU[n, zz - 1])).astype(BF)
        send_up(n, zz)

    def relay_down(n, zz):
        wait_for(RD.at[n, zz], rzd.at[n, zz])
        SZ[n, zz] = (f(SZ[n, zz]) + f(RD[n, zz])).astype(BF)
        send_down(n, zz)

    def red_d(n):
        @pl.when(z == 1)
        def _():
            for zz in (3, 2):
                relay_up(n, zz)

        @pl.when(z == 2)
        def _():
            for zz in (0, 1):
                relay_down(n, zz)

    def red_e(n):
        @pl.when(z == 2)
        def _():
            relay_up(n, 3)

        @pl.when(z == 1)
        def _():
            relay_down(n, 0)

    def red_f(l, n):
        s = rows(me)

        def finish(u):
            u = u.astype(BF)

            @pl.when(l == 0)
            def _():
                out = (f(xin[NE + n]) + f(u)).astype(BF)
                XO[n] = out
                XA[n, s] = out

            @pl.when(l == 1)
            def _():
                yT[n] = (f(XO[n]) + f(u)).astype(BF)

        @pl.when(z == 0)
        def _():
            wait_for(RD.at[n, 0], rzd.at[n, 0])
            finish(f(SZ[n, 0]) + f(RD[n, 0]))

        @pl.when(z == 3)
        def _():
            wait_for(RU.at[n, 2], rzu.at[n, 2])
            finish(f(SZ[n, 3]) + f(RU[n, 2]))

        for zz in (1, 2):
            @pl.when(z == zz)
            def _():
                wait_for(RU.at[n, zz - 1], rzu.at[n, zz - 1])
                wait_for(RD.at[n, zz], rzd.at[n, zz])
                finish(f(SZ[n, zz]) + f(RU[n, zz - 1]) + f(RD[n, zz]))

        @pl.when(n >= NT - 2)
        def _():
            wait_for(RC.at[0], rcs.at[n])
            wait_for(RY.at[0], rys.at[n])

        for zz in range(3):
            @pl.when(z == zz)
            def _():
                wait_for(RU.at[n, pl.ds(0, 3 - zz)], rsu.at[n])

            @pl.when(z == 3 - zz)
            def _():
                wait_for(RD.at[n, pl.ds(0, 3 - zz)], rsd.at[n])

        @pl.when(l == 0)
        def _():
            gather_own(XO.at[n], act, n, NE)

    shard = me

    def layer(l):
        for hop in (1, 2, 3):
            loop(NT, lambda n: gather_hop(act, n, NE, hop))
        loop(NT, lambda n: gather_cross(act, n, NE))

        for p in range(2, NPC):
            w_send(l, p)

        @pl.when(l == 0)
        def _():
            unpack()
        w_forward(l, 0)
        for i in range(5):
            wait_own(l, i)

        def first(n):
            gather_end(act, n, NE)
            norm(l, n)
            @pl.when(n == 0)
            def _():
                w_arrive(l, 0)
            qkv(l, n)
        loop(NT, first)
        w_forward(l, 1)
        w_forward(l, 2)
        attention()
        for b in range(2):
            off = pl.ds(pl.multiple_of(b * SEQ + 128 * (shard // 2), 128), 128)
            kvo[l, 0, b] = KT[:, off]
            kvo[l, 1, b] = VT[:, off]
        for p in range(3, GP + 1):
            w_forward(l, p)
        for p in range(1, GP + 1):
            w_arrive(l, p)
        loop(NT, lambda n: gate_up(l, n))
        for p in (GP + 1, GP + 2):
            w_forward(l, p)
        for p in (GP + 1, GP + 2):
            w_arrive(l, p)

        @pl.when(l == 0)
        def _():
            for p in range(2):
                w_send(1, p)

        def step(i):
            @pl.when(i < NT)
            def _():
                red_a(l, i)
            for lag, stage in ((1, red_b), (2, red_c), (3, red_d), (4, red_e), (5, functools.partial(red_f, l))):
                @pl.when((i >= lag) & (i < NT + lag))
                def _():
                    stage(i - lag)
        loop(NT + 5, step)

    def wait_own(l, i):
        ref = [WQ.at[0, :, pl.ds(0, RW)], GU.at[0, 0, pl.ds(0, RW)], GU.at[0, 0, pl.ds(0, RW)], WO.at[0, pl.ds(0, SH), pl.ds(0, RW)], WO.at[0, pl.ds(0, FB), pl.ds(0, RW)]][i]
        wait_for(ref, own.at[l, i])

    loop(2, layer)

    for l in range(2):
        for p in range(NPC):
            wait_for(w_size(l, p), ws.at[l, p])
            wait_for(w_size(l, p), xs.at[l, p])


def solution(mesh):
    act_spec = P("dp", None, ("row", "col"))
    weight_spec = P(None, "row", "col")

    def device_fn(x_loc, gain_loc, w_in_loc, w_kv_loc, w_out_loc):
        me = lax.axis_index("row") * 4 + lax.axis_index("col")
        xt = x_loc.reshape(T, SH).T
        kv = jnp.transpose(w_kv_loc, (0, 2, 1)).reshape(HD, 5, 128)
        kv = jnp.concatenate([kv, jnp.zeros((HD, 1, 128), BF)], axis=1).reshape(HD, 3, 2, 128)
        kv = jnp.transpose(kv, (2, 0, 1, 3)).reshape(SH, 384)
        gain = jnp.pad(gain_loc.T, ((0, 0), (0, 126)))
        xin = jnp.concatenate([kv, gain, xt], axis=1)
        xin = jnp.transpose(xin.reshape(SH, NC, CW), (1, 0, 2))
        wq = jnp.transpose(w_in_loc[:, :, :RW], (0, 2, 1))
        NPC = GP + 3
        dma = pltpu.SemaphoreType.DMA
        hbm = pl.BlockSpec(memory_space=pl.ANY)
        vmem = pl.BlockSpec(memory_space=pltpu.VMEM)
        y_t, kvo = pl.pallas_call(
            kernel,
            out_shape=(jax.ShapeDtypeStruct((NT, SH, CW), BF), jax.ShapeDtypeStruct((2, 2, 2, HD, 128), BF)),
            in_specs=[vmem, hbm, hbm, hbm, vmem],
            out_specs=(vmem, vmem),
            scratch_shapes=[
                pltpu.VMEM((NT, D, CW), BF),
                pltpu.VMEM((2, 2, D, FB), BF),
                pltpu.VMEM((2, SH, D), BF),
                pltpu.VMEM((2, 192, D), BF),
                pltpu.VMEM((2, SH + FB, D), BF),
                pltpu.VMEM((2, D, 128), BF),
                pltpu.VMEM((NT, SH + FB, CW), BF),
                pltpu.VMEM((SH, T), BF),
                pltpu.VMEM((HD, T), BF),
                pltpu.VMEM((HD, T), BF),
                pltpu.VMEM((NT, SH, CW), BF),
                pltpu.VMEM((NT, 8, SH, CW), BF),
                pltpu.VMEM((NT, 4, SH, CW), BF),
                pltpu.VMEM((NT, 3, SH, CW), BF),
                pltpu.VMEM((NT, 3, SH, CW), BF),
                pltpu.VMEM((2, 8, SH, CW), BF),
                pltpu.VMEM((2, 4, SH, CW), BF),
                pltpu.VMEM((NT, 4, SH, CW), BF),
                dma((NC,)), dma((NC,)), dma((NC,)), dma((NC,)),
                dma((NC, 2, 3)), dma((NC,)), dma((NC,)),
                dma((NT,)), dma((NT,)), dma((NT,)), dma((NT,)),
                dma((NT, 3)), dma((NT, 3)), dma((NT,)), dma((NT,)),
                dma((2, NPC)), dma((2, NPC, 3)), dma((2, NPC)), dma((2, NPC)),
                dma((2, 5)),
            ],
            compiler_params=pltpu.CompilerParams(collective_id=0, has_side_effects=True, vmem_limit_bytes=67043328),
        )(xin, wq, w_in_loc, w_out_loc, rope_tables())
        y = jnp.transpose(y_t, (0, 2, 1)).reshape(2, SEQ, SH)
        kv_out = lax.dynamic_slice_in_dim(kvo, 64 * lax.rem(me, 2), 64, axis=4)
        return y, jnp.transpose(kv_out, (0, 1, 2, 4, 3))

    return jax.shard_map(device_fn, mesh=mesh, in_specs=(act_spec, P(None, ("row", "col")), weight_spec, weight_spec, P(None, "col", "row")), out_specs=(act_spec, P(None, None, "dp", ("row", "col"), None)), check_vma=False)
```

```python
import functools

import jax
import jax.numpy as jnp
from jax import lax
from jax.experimental import pallas as pl
from jax.experimental.pallas import tpu as pltpu
from jax.sharding import PartitionSpec as P

BF = jnp.bfloat16
F32 = jnp.float32
MESH_ID = pl.DeviceIdType.MESH
LN_EPS = 1e-6

D = 2560
SH = 160
RW = 640
FB = 640
HD = 80
HALF = HD // 2
SEQ = 1024
T = 2 * SEQ
CW = 512
NT = T // CW
NE = 512 // CW
NC = NE + NT
GP = 8
GR = RW // GP
LANES = 128
HOPS = (1, 2, 3)
QB = 256
SCN, SYN = 4, 6
MR = 16
LAGS = (1, 3, 8, 12, 16)
PM = GR // MR
AG0 = 1
RQ = 0
RG = ((1, 11, 2),)
AG1 = (2,) * 10 + (0, 0)
UFW, EFW = 24, 5


def weight_plan():
    sent, when = 0, []
    for lo, hi, each in RG:
        for i in range(lo, hi):
            when += [i] * each
            sent += each
    units = [[] for _ in range(4 * NT + LAGS[-1])]
    events = [[] for _ in range(3 * NT)]
    late = list(range(1, GP + 1))
    ev = []
    for e in range(3 * NT):
        ev += [e] * AG1[e]
    for p in range(1, GP + 1):
        last = PM * p - 1
        if last < sent:
            if when[last] + UFW < len(units):
                units[when[last] + UFW].append(p)
                late.remove(p)
                continue
            e = max(0, when[last] + UFW - len(units))
        elif last < sent + len(ev):
            e = ev[last - sent] + EFW
        else:
            continue
        if e < 3 * NT:
            events[e].append(p)
            late.remove(p)
    return sent, units, events, late[0] if late else GP + 1


RS0, UNITS, EVENTS, LATE = weight_plan()


def rope_tables():
    inv_freq = 1.0 / (10000.0 ** (jnp.arange(HALF, dtype=F32) * 2.0 / HD))
    angles = inv_freq[:, None] * jnp.arange(SEQ).astype(F32)[None, :]
    return jnp.stack([jnp.cos(angles), jnp.sin(angles)])


def sub(start, size):
    return pl.ds(pl.multiple_of(start, 16), size)


def lan(start, size):
    return pl.ds(pl.multiple_of(start, LANES), size)


def dot_ta(a, b):
    return lax.dot_general(a, b, (((0,), (0,)), ((), ())), preferred_element_type=F32)


def kernel(xin, wq, w_in, w_out, cs, yT, kvo, XA, GU, WQ, WKV, WO, GB, MT, QT, KT, VT, XO, RC, RY, RU, RD, SC, SY, SZ,
           zsu, zsd, ysn, csn, zrc, yrc, crc, rcs, rcr, rys, ryr, rzu, rzd, rsz, ws, wr, xs, xr, own):
    x = lax.axis_index("dp")
    z = lax.axis_index("row")
    c = lax.axis_index("col")
    y, k = c // 2, lax.rem(c, 2)
    me = 4 * z + c
    up = (x, jnp.minimum(z + 1, 3), c)
    down = (x, jnp.maximum(z - 1, 0), c)
    ypeer = (x, z, lax.rem(c + 2, 4))
    cpeer = (x, z, c + 1 - 2 * k)
    xpeer = (1 - x, z, c)
    zpeer = [(x, lax.rem(z + h, 4), c) for h in HOPS]

    def rcopy(src, dst, ss, rs, dev):
        return pltpu.make_async_remote_copy(src_ref=src, dst_ref=dst, send_sem=ss, recv_sem=rs, device_id=dev, device_id_type=MESH_ID)

    def wait_for(ref, sem):
        pltpu.make_async_copy(ref, ref, sem).wait()

    def rows(s):
        return sub(s * SH, SH)

    def loop(n, body):
        def step(i, carry):
            body(i)
            return carry
        lax.fori_loop(0, n, step, 0)

    barrier = pltpu.get_barrier_semaphore()
    for dev in zpeer + [ypeer, cpeer, xpeer]:
        pl.semaphore_signal(barrier, inc=1, device_id=dev, device_id_type=MESH_ID)
    pl.semaphore_wait(barrier, 6)

    def act(ch, s):
        return XA.at[ch, rows(s)]

    def ext(ch, s):
        i = 16 * ch + s
        return MT.at[i // 5, rows(lax.rem(i, 5))]

    @jax.named_scope("gather_own")
    def gather_own(src, buf, ch, o):
        q = ch + o
        dst = buf(ch, me)

        @pl.when(z < 3)
        def _():
            rcopy(src, dst, zsu.at[q], zrc.at[q, 0, 0], up).start()

        @pl.when(z > 0)
        def _():
            rcopy(src, dst, zsd.at[q], zrc.at[q, 1, 0], down).start()

        rcopy(src, dst, ysn.at[q], yrc.at[q], ypeer).start()
        rcopy(src, dst, csn.at[q], crc.at[q], cpeer).start()

    @jax.named_scope("gather_hop")
    def gather_hop(buf, ch, o, hop):
        q = ch + o

        @pl.when(z - hop >= 0)
        def _():
            ref = buf(ch, jnp.maximum(me - 4 * hop, 0))
            wait_for(ref, zrc.at[q, 0, hop - 1])
            if hop < 3:
                @pl.when(z < 3)
                def _():
                    rcopy(ref, ref, zsu.at[q], zrc.at[q, 0, hop], up).start()
            rcopy(ref, ref, ysn.at[q], yrc.at[q], ypeer).start()
            rcopy(ref, ref, csn.at[q], crc.at[q], cpeer).start()

        @pl.when(z + hop <= 3)
        def _():
            ref = buf(ch, jnp.minimum(me + 4 * hop, 15))
            wait_for(ref, zrc.at[q, 1, hop - 1])
            if hop < 3:
                @pl.when(z > 0)
                def _():
                    rcopy(ref, ref, zsd.at[q], zrc.at[q, 1, hop], down).start()
            rcopy(ref, ref, ysn.at[q], yrc.at[q], ypeer).start()
            rcopy(ref, ref, csn.at[q], crc.at[q], cpeer).start()

    @jax.named_scope("gather_cross")
    def gather_cross(buf, ch, o):
        q = ch + o
        wait_for(XA.at[0, pl.ds(0, 4 * SH)], yrc.at[q])
        for zz in range(4):
            ref = buf(ch, 4 * zz + lax.rem(c + 2, 4))
            rcopy(ref, ref, csn.at[q], crc.at[q], cpeer).start()

    @jax.named_scope("gather_end")
    def gather_end(buf, ch, o):
        q = ch + o
        wait_for(XA.at[0, pl.ds(0, 8 * SH)], crc.at[q])
        for zz in range(3):
            @pl.when(z == zz)
            def _():
                wait_for(XA.at[0, pl.ds(0, (zz + 1) * SH)], zsu.at[q])

            @pl.when(z == 3 - zz)
            def _():
                wait_for(XA.at[0, pl.ds(0, (zz + 1) * SH)], zsd.at[q])
        wait_for(XA.at[0, pl.ds(0, 4 * SH)], ysn.at[q])
        wait_for(XA.at[0, pl.ds(0, 8 * SH)], csn.at[q])

    NPC = GP + 3

    def lane(zz):
        return lan(zz * RW, RW)

    PQ, PA, PB = 0, GP + 1, GP + 2

    def kind(p):
        return p if isinstance(p, int) and (p == PQ or p > GP) else 1

    def w_ref(l, p, zz, half):
        if kind(p) == PQ:
            return WQ.at[l, sub(80 * half, 80), lane(zz)]
        if kind(p) == PA:
            return WO.at[l, sub(400 * half, 160), lane(zz)]
        if kind(p) == PB:
            return WO.at[l, sub(160 + 400 * half, 240), lane(zz)]
        return GU.at[l, half, sub(zz * RW + GR * (p - 1), GR), :]

    def w_send(l, kind_, m, mr=MR):
        r = mr * m
        for h in HOPS:
            t = lax.rem(z + h, 4)
            if kind_ == "q":
                p, src = PQ, wq.at[l, sub(SH * t + 80 * x + r, mr), :]
                dst = WQ.at[l, sub(80 * x + r, mr), lane(z)]
            elif kind_ == "g":
                p, src = 1 + r // GR, w_in.at[l, sub(r, mr), lan(RW + D * x + FB * t, FB)]
                dst = GU.at[l, x, sub(z * RW + r, mr), :]
            elif kind_ == "a":
                p, src = PA, w_out.at[l, sub(jnp.where(x == 0, SH * t, RW + FB * t + 240) + r, mr), :]
                dst = WO.at[l, sub(400 * x + r, mr), lane(z)]
            else:
                p, src = PB, w_out.at[l, sub(RW + FB * t + 400 * x + r, mr), :]
                dst = WO.at[l, sub(160 + 400 * x + r, mr), lane(z)]
            rcopy(src, dst, ws.at[l, p], wr.at[l, p, h - 1], zpeer[h - 1]).start()

    def rest_send(l, m):
        whole = -(-m // PM)
        for v in range(m, whole * PM):
            w_send(l, "g", v)
        for v in range(whole, GP):
            w_send(l, "g", v, GR)

    NQ, NG, NA, NB = 80 // MR, RW // MR, 160 // MR, 240 // MR

    @jax.named_scope("w_forward")
    def w_forward(l, p):
        for h in HOPS:
            ref = w_ref(l, p, lax.rem(z - h + 4, 4), x)
            wait_for(ref, wr.at[l, p, h - 1])
            rcopy(ref, ref, xs.at[l, p], xr.at[l, p, h - 1], xpeer).start()

    def w_size(l, p):
        if kind(p) == PQ:
            return WQ.at[l, pl.ds(0, 80), pl.ds(0, 3 * RW)]
        if kind(p) == PA:
            return WO.at[l, pl.ds(0, 160), pl.ds(0, 3 * RW)]
        if kind(p) == PB:
            return WO.at[l, pl.ds(0, 240), pl.ds(0, 3 * RW)]
        return GU.at[l, 0, pl.ds(0, 3 * GR), :]

    @jax.named_scope("w_arrive")
    def w_arrive(l, p):
        for h in HOPS:
            wait_for(w_ref(l, p, 0, 0), xr.at[l, p, h - 1])

    def w_own(l):
        return [
            pltpu.make_async_copy(wq.at[l, sub(SH * z, SH), :], WQ.at[l, :, lane(z)], own.at[l, 0]),
            pltpu.make_async_copy(w_in.at[l, :, lan(RW + FB * z, FB)], GU.at[l, 0, sub(z * RW, RW), :], own.at[l, 1]),
            pltpu.make_async_copy(w_in.at[l, :, lan(RW + D + FB * z, FB)], GU.at[l, 1, sub(z * RW, RW), :], own.at[l, 2]),
            pltpu.make_async_copy(w_out.at[l, sub(SH * z, SH), :], WO.at[l, pl.ds(0, SH), lane(z)], own.at[l, 3]),
            pltpu.make_async_copy(w_out.at[l, sub(RW + FB * z, FB), :], WO.at[l, pl.ds(SH, FB), lane(z)], own.at[l, 4]),
        ]

    for ch in range(NE):
        gather_own(xin.at[ch], ext, ch, 0)
    for ch in range(NT):
        gather_own(xin.at[NE + ch], act, ch, NE)
    for ch in range(NE):
        ext(ch, me)[...] = xin[ch]

    def put_own(ch):
        XA[ch, rows(me)] = xin[NE + ch]
    loop(NT, put_own)
    w_send(0, "q", 0, 80)
    for l in range(2):
        for cp in w_own(l):
            cp.start()
    for hop in HOPS:
        loop(NE, lambda ch: gather_hop(ext, ch, 0, hop))

        def tokens(n):
            gather_hop(act, n, NE, hop)
            for v in range(AG0):
                w_send(0, "g", AG0 * ((hop - 1) * NT + n) + v)
        loop(NT, tokens)
    loop(NE, lambda ch: gather_cross(ext, ch, 0))
    loop(NT, lambda n: gather_cross(act, n, NE))

    @jax.named_scope("unpack")
    def unpack():
        loop(NE, lambda ch: gather_end(ext, ch, 0))

        def shard(s):
            zz, cc = s // 4, lax.rem(s, 4)
            for b in range(5):
                lo = 128 * (b // 2)
                i = 16 * (lo // CW) + s
                blk = MT[i // 5, sub(lax.rem(i, 5) * SH + 80 * (b % 2), 80), lo % CW:lo % CW + 128].astype(F32)
                for l in range(2):
                    WKV[l, sub(48 * cc, 40), lan(zz * RW + 128 * b, 128)] = blk[40 * l:40 * l + 40].astype(BF)
            i = 16 * (NE - 1) + s
            blk = MT[i // 5, rows(lax.rem(i, 5)), CW - 128:CW].astype(F32)
            for l in range(2):
                GB[l, rows(s), :] = jnp.broadcast_to(blk[:, l:l + 1], (SH, 128)).astype(BF)
        loop(16, shard)
        for l in range(2):
            for cc in range(4):
                WKV[l, 48 * cc + 40:48 * cc + 48, :] = jnp.zeros((8, D), BF)

    BR = 32

    @jax.named_scope("norm")
    def norm(l, n):
        def fold(v):
            return v.reshape(BR // 8, 8, CW).sum(0)

        def load(i):
            return XA[n, sub(i * BR, BR), :].astype(F32)

        tot = lax.fori_loop(0, D // BR, lambda i, a: a + fold(load(i)), jnp.zeros((8, CW), F32), unroll=4)
        mean = jnp.sum(tot, axis=0, keepdims=True) / D

        def square(i, a):
            d = load(i) - mean
            return a + fold(d * d)
        var = jnp.sum(lax.fori_loop(0, D // BR, square, jnp.zeros((8, CW), F32), unroll=4), axis=0, keepdims=True) / D
        scale = lax.rsqrt(var + LN_EPS)

        def put(i, a):
            g = jnp.concatenate([GB[l, sub(i * BR, BR), :].astype(F32)] * (CW // 128), axis=1)
            XA[n, sub(i * BR, BR), :] = ((load(i) - mean) * scale * g).astype(BF)
            return a
        lax.fori_loop(0, D // BR, put, 0, unroll=4)

    def tok(n):
        return lan(n * CW, CW)

    @jax.named_scope("qkv")
    def qkv(l, n):
        pos = lan(lax.rem(n * CW, SEQ), CW)
        co, si = cs[0, :, pos], cs[1, :, pos]
        h = XA[n]
        kv = jnp.dot(WKV[l], h, preferred_element_type=F32).astype(BF).astype(F32)

        def rot(lo, hi):
            return jnp.concatenate([lo * co - hi * si, hi * co + lo * si], axis=0)
        KT[:, tok(n)] = rot(kv[0:40], kv[48:88]).astype(BF)
        VT[:, tok(n)] = jnp.concatenate([kv[96:136], kv[144:184]], axis=0).astype(BF)
        qq = jnp.dot(WQ[l], h, preferred_element_type=F32).astype(BF).astype(F32)
        for hd in range(2):
            QT[HD * hd:HD * hd + HD, tok(n)] = (rot(qq[HD * hd:HD * hd + HALF], qq[HD * hd + HALF:HD * hd + HD]) * HD ** -0.5).astype(BF)

    @jax.named_scope("attention")
    def attention():
        def body(bh):
            b, hd = bh // 2, lax.rem(bh, 2)
            hr = sub(hd * HD, HD)
            for i in range(SEQ // QB):
                nk = QB * (i + 1)
                ks = lan(b * SEQ, nk)
                qs = lan(b * SEQ + QB * i, QB)
                s = dot_ta(KT[:, ks], QT[hr, qs])
                keep = lax.broadcasted_iota(jnp.int32, (QB, QB), 0) <= lax.broadcasted_iota(jnp.int32, (QB, QB), 1)
                last = jnp.where(keep, s[nk - QB:], -1e30)
                s = jnp.concatenate([s[:nk - QB], last], axis=0) if i else last
                e = jnp.exp(s - jnp.max(s, axis=0, keepdims=True))
                pr = (e * (1.0 / jnp.sum(e, axis=0, keepdims=True))).astype(BF)
                MT[b * (SEQ // CW) + QB * i // CW, hr, QB * i % CW:QB * i % CW + QB] = jnp.dot(VT[:, ks], pr, preferred_element_type=F32).astype(BF)
        loop(4, body)

    @jax.named_scope("gate_up")
    def gate_up(l, n):
        h = XA[n]
        g = dot_ta(GU[l, 0], h).astype(BF).astype(F32)
        u = dot_ta(GU[l, 1], h).astype(BF).astype(F32)
        MT[n, SH:SH + FB, :] = (g * lax.logistic(g) * u).astype(BF)

    def f(ref_value):
        return ref_value.astype(F32)

    NU = 4 * NT

    def unit(i):
        j = i // NT
        return jnp.where(j == 0, 3, jnp.where(j == 1, 0, jnp.where(j == 2, 2, 1))), lax.rem(i, NT)

    @jax.named_scope("red_a")
    def red_a(l, i):
        zz, n = unit(i)
        slot = lax.rem(i, SCN)

        @pl.when(i >= SCN)
        def _():
            wait_for(SC.at[slot], rcs.at[i - SCN])

        XA[n, sub(zz * RW, RW), :] = dot_ta(WO[l, :, lane(zz)], MT[n]).astype(BF)
        for yy in range(2):
            SC[slot, yy] = XA[n, rows(4 * zz + 2 * yy + 1 - k)]
        for yy in range(2):
            rcopy(SC.at[slot, yy], RC.at[n, 2 * zz + yy], rcs.at[i], rcr.at[i], cpeer).start()

    @jax.named_scope("red_b")
    def red_b(i):
        zz, n = unit(i)
        slot = lax.rem(i, SYN)
        wait_for(RC.at[n, pl.ds(2 * zz, 2)], rcr.at[i])

        @pl.when(i >= SYN)
        def _():
            wait_for(SY.at[slot], rys.at[i - SYN])

        SY[slot] = (f(XA[n, rows(4 * zz + 2 * (1 - y) + k)]) + f(RC[n, 2 * zz + 1 - y])).astype(BF)
        rcopy(SY.at[slot], RY.at[n, zz], rys.at[i], ryr.at[i], ypeer).start()

    def send_up(n, zz, i):
        rcopy(SZ.at[n, zz], RU.at[n, zz - 1], rsz.at[i], rzu.at[i], up).start()

    def send_down(n, zz, i):
        rcopy(SZ.at[n, zz], RD.at[n, zz], rsz.at[i], rzd.at[i], down).start()

    @jax.named_scope("red_c")
    def red_c(i):
        zz, n = unit(i)
        wait_for(RY.at[n, zz], ryr.at[i])
        SZ[n, zz] = (f(XA[n, rows(4 * zz + c)]) + f(RC[n, 2 * zz + y]) + f(RY[n, zz])).astype(BF)

        @pl.when((z == 0) & (zz > 0))
        def _():
            send_up(n, zz, i)

        @pl.when((z == 3) & (zz < 3))
        def _():
            send_down(n, zz, i)

    def relay_up(i):
        zz, n = unit(i)
        wait_for(RU.at[n, zz - 1], rzu.at[i])
        SZ[n, zz] = (f(SZ[n, zz]) + f(RU[n, zz - 1])).astype(BF)
        send_up(n, zz, i)

    def relay_down(i):
        zz, n = unit(i)
        wait_for(RD.at[n, zz], rzd.at[i])
        SZ[n, zz] = (f(SZ[n, zz]) + f(RD[n, zz])).astype(BF)
        send_down(n, zz, i)

    @jax.named_scope("red_d")
    def red_d(i):
        zz, _ = unit(i)

        @pl.when((z == 1) & (zz > 1))
        def _():
            relay_up(i)

        @pl.when((z == 2) & (zz < 2))
        def _():
            relay_down(i)

    @jax.named_scope("red_e")
    def red_e(i):
        zz, _ = unit(i)

        @pl.when((z == 2) & (zz > 2))
        def _():
            relay_up(i)

        @pl.when((z == 1) & (zz < 1))
        def _():
            relay_down(i)

    @jax.named_scope("red_f")
    def red_f(l, i):
        zz, n = unit(i)

        def finish(u):
            u = u.astype(BF)

            @pl.when(l == 0)
            def _():
                out = (f(xin[NE + n]) + f(u)).astype(BF)
                XO[n] = out
                XA[n, rows(me)] = out
                gather_own(XO.at[n], act, n, NE)

            @pl.when(l == 1)
            def _():
                yT[n] = (f(XO[n]) + f(u)).astype(BF)

        @pl.when((z == 0) & (zz == 0))
        def _():
            wait_for(RD.at[n, 0], rzd.at[i])
            finish(f(SZ[n, 0]) + f(RD[n, 0]))

        @pl.when((z == 3) & (zz == 3))
        def _():
            wait_for(RU.at[n, 2], rzu.at[i])
            finish(f(SZ[n, 3]) + f(RU[n, 2]))

        for v in (1, 2):
            @pl.when((z == v) & (zz == v))
            def _():
                wait_for(RU.at[n, v - 1], rzu.at[i])
                wait_for(RD.at[n, v], rzd.at[i])
                finish(f(SZ[n, v]) + f(RU[n, v - 1]) + f(RD[n, v]))

        @pl.when(i >= NU - SCN)
        def _():
            wait_for(SC.at[0], rcs.at[i])

        @pl.when(i >= NU - SYN)
        def _():
            wait_for(SY.at[0], rys.at[i])

        @pl.when(zz != z)
        def _():
            wait_for(SZ.at[n, zz], rsz.at[i])

    shard = me

    def o_forward(l, j):
        zz = unit(NT * j)[0]
        h = lax.rem(z - zz + 4, 4)

        @pl.when(h > 0)
        def _():
            for p in (PA, PB):
                ref = w_ref(l, p, zz, x)
                wait_for(ref, wr.at[l, p, h - 1])
                rcopy(ref, ref, xs.at[l, p], xr.at[l, p, h - 1], xpeer).start()

    def o_arrive(l, j):
        zz = unit(NT * j)[0]
        h = lax.rem(z - zz + 4, 4)

        @pl.when(h > 0)
        def _():
            for p in (PA, PB):
                wait_for(w_ref(l, p, zz, 1 - x), xr.at[l, p, h - 1])

    def layer(l):
        @pl.when(l == 0)
        def _():
            rest_send(0, 3 * NT * AG0)
            unpack()

        @pl.when(l == 1)
        def _():
            done = RS0
            for e in range(3 * NT):
                gather_hop(act, e % NT, NE, e // NT + 1)
                for v in range(AG1[e]):
                    w_send(1, "g", done)
                    done += 1
                for p in EVENTS[e]:
                    w_forward(1, p)
            loop(NT, lambda n: gather_cross(act, n, NE))
            rest_send(1, RS0 + sum(AG1))
            w_send(1, "a", 0, 160)
            w_send(1, "b", 0, 240)

        @pl.when(l == 0)
        def _():
            w_forward(0, PQ)
        for cp in w_own(l):
            cp.wait()

        def first(n):
            gather_end(act, n, NE)
            norm(l, n)
            @pl.when(n == 0)
            def _():
                w_arrive(l, PQ)
            qkv(l, n)

            late = jnp.where(l == 0, 1, LATE) + n

            @pl.when(late <= GP)
            def _():
                w_forward(l, late)
        loop(NT, first)

        @pl.when(l == 0)
        def _():
            w_send(0, "a", 0, 160)
            w_send(0, "b", 0, 240)
        attention()
        for b in range(2):
            off = lan(b * SEQ + 128 * (shard // 2), 128)
            kvo[l, 0, b] = KT[:, off]
            kvo[l, 1, b] = VT[:, off]
        fwd = jnp.where(l == 0, NT, min(GP, LATE - 1 + NT))
        loop(GP - fwd, lambda p: w_forward(l, fwd + 1 + p))
        loop(GP, lambda p: w_arrive(l, p + 1))
        o_forward(l, 0)

        def step(i):
            @pl.when(i < NU)
            def _():
                @pl.when(lax.rem(i, NT) == 0)
                def _():
                    o_arrive(l, i // NT)

                    @pl.when(i < NU - NT)
                    def _():
                        o_forward(l, i // NT + 1)

                @pl.when(i < NT)
                def _():
                    gate_up(l, i)
                red_a(l, i)
            for lag, stage in zip(LAGS, (red_b, red_c, red_d, red_e, functools.partial(red_f, l))):
                @pl.when((i >= lag) & (i < NU + lag))
                def _():
                    stage(i - lag)

            @pl.when(l == 0)
            def _():
                @pl.when(i == RQ)
                def _():
                    w_send(1, "q", 0, 80)

                @pl.when(i == RQ + 12)
                def _():
                    w_forward(1, PQ)

                base = 0
                for lo, hi, each in RG:
                    @pl.when((i >= lo) & (i < hi))
                    def _():
                        for v in range(each):
                            w_send(1, "g", base + (i - lo) * each + v)
                    base += (hi - lo) * each

                for u, ps in enumerate(UNITS):
                    if ps:
                        @pl.when(i == u)
                        def _():
                            for p in ps:
                                w_forward(1, p)
        loop(NU + LAGS[-1], step)

    loop(2, layer)

    for l in range(2):
        for p in range(NPC):
            wait_for(w_size(l, p), ws.at[l, p])
            wait_for(w_size(l, p), xs.at[l, p])


def solution(mesh):
    act_spec = P("dp", None, ("row", "col"))
    weight_spec = P(None, "row", "col")

    def device_fn(x_loc, gain_loc, w_in_loc, w_kv_loc, w_out_loc):
        me = lax.axis_index("row") * 4 + lax.axis_index("col")
        xt = x_loc.reshape(T, SH).T
        kv = jnp.transpose(w_kv_loc, (0, 2, 1)).reshape(HD, 5, 128)
        kv = jnp.concatenate([kv, jnp.zeros((HD, 1, 128), BF)], axis=1).reshape(HD, 3, 2, 128)
        kv = jnp.transpose(kv, (2, 0, 1, 3)).reshape(SH, 384)
        gain = jnp.pad(gain_loc.T, ((0, 0), (0, 126)))
        xin = jnp.concatenate([kv, gain, xt], axis=1)
        xin = jnp.transpose(xin.reshape(SH, NC, CW), (1, 0, 2))
        wq = jnp.transpose(w_in_loc[:, :, :RW], (0, 2, 1))
        NPC = GP + 3
        dma = pltpu.SemaphoreType.DMA
        hbm = pl.BlockSpec(memory_space=pl.ANY)
        vmem = pl.BlockSpec(memory_space=pltpu.VMEM)
        y_t, kvo = pl.pallas_call(
            kernel,
            out_shape=(jax.ShapeDtypeStruct((NT, SH, CW), BF), jax.ShapeDtypeStruct((2, 2, 2, HD, 128), BF)),
            in_specs=[vmem, hbm, hbm, hbm, vmem],
            out_specs=(vmem, vmem),
            scratch_shapes=[
                pltpu.VMEM((NT, D, CW), BF),
                pltpu.VMEM((2, 2, D, FB), BF),
                pltpu.VMEM((2, SH, D), BF),
                pltpu.VMEM((2, 192, D), BF),
                pltpu.VMEM((2, SH + FB, D), BF),
                pltpu.VMEM((2, D, 128), BF),
                pltpu.VMEM((NT, SH + FB, CW), BF),
                pltpu.VMEM((SH, T), BF),
                pltpu.VMEM((HD, T), BF),
                pltpu.VMEM((HD, T), BF),
                pltpu.VMEM((NT, SH, CW), BF),
                pltpu.VMEM((NT, 8, SH, CW), BF),
                pltpu.VMEM((NT, 4, SH, CW), BF),
                pltpu.VMEM((NT, 3, SH, CW), BF),
                pltpu.VMEM((NT, 3, SH, CW), BF),
                pltpu.VMEM((SCN, 2, SH, CW), BF),
                pltpu.VMEM((SYN, SH, CW), BF),
                pltpu.VMEM((NT, 4, SH, CW), BF),
                dma((NC,)), dma((NC,)), dma((NC,)), dma((NC,)),
                dma((NC, 2, 3)), dma((NC,)), dma((NC,)),
                dma((4 * NT,)), dma((4 * NT,)), dma((4 * NT,)), dma((4 * NT,)),
                dma((4 * NT,)), dma((4 * NT,)), dma((4 * NT,)),
                dma((2, NPC)), dma((2, NPC, 3)), dma((2, NPC)), dma((2, NPC, 3)),
                dma((2, 5)),
            ],
            compiler_params=pltpu.CompilerParams(collective_id=0, has_side_effects=True, vmem_limit_bytes=67043328),
        )(xin, wq, w_in_loc, w_out_loc, rope_tables())
        y = jnp.transpose(y_t, (0, 2, 1)).reshape(2, SEQ, SH)
        kv_out = lax.dynamic_slice_in_dim(kvo, 64 * lax.rem(me, 2), 64, axis=4)
        return y, jnp.transpose(kv_out, (0, 1, 2, 4, 3))

    return jax.shard_map(device_fn, mesh=mesh, in_specs=(act_spec, P(None, ("row", "col")), weight_spec, weight_spec, P(None, "col", "row")), out_specs=(act_spec, P(None, None, "dp", ("row", "col"), None)), check_vma=False)
```

```python
import functools

import jax
import jax.numpy as jnp
from jax import lax
from jax.experimental import pallas as pl
from jax.experimental.pallas import tpu as pltpu
from jax.sharding import PartitionSpec as P

BF = jnp.bfloat16
F32 = jnp.float32
MESH_ID = pl.DeviceIdType.MESH
LN_EPS = 1e-6

D = 2560
SH = 160
RW = 640
FB = 640
HD = 80
HALF = HD // 2
SEQ = 1024
T = 2 * SEQ
CW = 512
NT = T // CW
NE = 512 // CW
NC = NE + NT
SPC = SEQ // CW
GP = 8
GR = RW // GP
LANES = 128
HOPS = (1, 2, 3)
QB = 256
SCN, SYN = 4, 6
MR = 16
LAGS = (1, 4, 7, 12, 15)
PM = GR // MR
S0 = (1,) * 8
GH0, GH1 = 1, 3
OEND = (4, 0)
OMID = (4, 0)
OF = (0, 4, 8)
RQ = 0
SU = (0,) + (2,) * 10
AG1 = (1,) * 8
UFW, EFW = 30, 12


def weight_plan():
    sent, when = 0, []
    for i, each in enumerate(SU):
        when += [i] * each
        sent += each
    units = [[] for _ in range(4 * NT + LAGS[-1])]
    events = [[] for _ in range(3 * NT)]
    late = list(range(1, GP + 1))
    ev = []
    for e in range(2 * NT):
        ev += [e] * AG1[e]
    for p in range(1, GP + 1):
        last = PM * p - 1
        if last < sent:
            if when[last] + UFW < len(units):
                units[when[last] + UFW].append(p)
                late.remove(p)
                continue
            e = max(0, when[last] + UFW - len(units))
        elif last < sent + len(ev):
            e = ev[last - sent] + EFW
        else:
            continue
        if e < 3 * NT:
            events[e].append(p)
            late.remove(p)
    return sent, units, events, late[0] if late else GP + 1


RS0, UNITS, EVENTS, LATE = weight_plan()


def rope_tables():
    inv_freq = 1.0 / (10000.0 ** (jnp.arange(HALF, dtype=F32) * 2.0 / HD))
    angles = inv_freq[:, None] * jnp.arange(SEQ).astype(F32)[None, :]
    return jnp.stack([jnp.cos(angles), jnp.sin(angles)])


def sub(start, size):
    return pl.ds(pl.multiple_of(start, 16), size)


def lan(start, size):
    return pl.ds(pl.multiple_of(start, LANES), size)


def dot_ta(a, b):
    return lax.dot_general(a, b, (((0,), (0,)), ((), ())), preferred_element_type=F32)


def kernel(xin, ein, w_in, w_out, cs, yT, kvo, KVT, WT, XA, GU, WQ, WKV, WO, GB, MT, QT, KT, VT, XO, RC, RY, RU, RD, SC, SY, SZ,
           zsu, zsd, ysn, csn, zrc, yrc, crc, rcs, rcr, rys, ryr, rzu, rzd, rsz, ws, wr, xs, xr, own):
    x = lax.axis_index("dp")
    z = lax.axis_index("row")
    c = lax.axis_index("col")
    y, k = c // 2, lax.rem(c, 2)
    me = 4 * z + c
    up = (x, jnp.minimum(z + 1, 3), c)
    down = (x, jnp.maximum(z - 1, 0), c)
    ypeer = (x, z, lax.rem(c + 2, 4))
    cpeer = (x, z, c + 1 - 2 * k)
    xpeer = (1 - x, z, c)
    zpeer = [(x, lax.rem(z + h, 4), c) for h in HOPS]

    def rcopy(src, dst, ss, rs, dev):
        return pltpu.make_async_remote_copy(src_ref=src, dst_ref=dst, send_sem=ss, recv_sem=rs, device_id=dev, device_id_type=MESH_ID)

    def wait_for(ref, sem):
        pltpu.make_async_copy(ref, ref, sem).wait()

    def rows(s):
        return sub(s * SH, SH)

    def loop(n, body):
        def step(i, carry):
            body(i)
            return carry
        lax.fori_loop(0, n, step, 0)

    barrier = pltpu.get_barrier_semaphore()
    for dev in zpeer + [ypeer, cpeer, xpeer]:
        pl.semaphore_signal(barrier, inc=1, device_id=dev, device_id_type=MESH_ID)
    pl.semaphore_wait(barrier, 6)

    def act(ch, s):
        return XA.at[ch, rows(s)]

    def ext(ch, s):
        i = 16 * ch + s
        return MT.at[i // 5, rows(lax.rem(i, 5))]

    @jax.named_scope("gather_own")
    def gather_own(src, buf, ch, o):
        q = ch + o
        dst = buf(ch, me)

        @pl.when(z < 3)
        def _():
            rcopy(src, dst, zsu.at[q], zrc.at[q, 0, 0], up).start()

        @pl.when(z > 0)
        def _():
            rcopy(src, dst, zsd.at[q], zrc.at[q, 1, 0], down).start()

        rcopy(src, dst, ysn.at[q], yrc.at[q], ypeer).start()
        rcopy(src, dst, csn.at[q], crc.at[q], cpeer).start()

    @jax.named_scope("gather_hop")
    def gather_hop(buf, ch, o, hop):
        q = ch + o

        @pl.when(z - hop >= 0)
        def _():
            ref = buf(ch, jnp.maximum(me - 4 * hop, 0))
            wait_for(ref, zrc.at[q, 0, hop - 1])
            if hop < 3:
                @pl.when(z < 3)
                def _():
                    rcopy(ref, ref, zsu.at[q], zrc.at[q, 0, hop], up).start()
            rcopy(ref, ref, ysn.at[q], yrc.at[q], ypeer).start()
            rcopy(ref, ref, csn.at[q], crc.at[q], cpeer).start()

        @pl.when(z + hop <= 3)
        def _():
            ref = buf(ch, jnp.minimum(me + 4 * hop, 15))
            wait_for(ref, zrc.at[q, 1, hop - 1])
            if hop < 3:
                @pl.when(z > 0)
                def _():
                    rcopy(ref, ref, zsd.at[q], zrc.at[q, 1, hop], down).start()
            rcopy(ref, ref, ysn.at[q], yrc.at[q], ypeer).start()
            rcopy(ref, ref, csn.at[q], crc.at[q], cpeer).start()

    @jax.named_scope("gather_cross")
    def gather_cross(buf, ch, o):
        q = ch + o
        wait_for(XA.at[0, pl.ds(0, 4 * SH)], yrc.at[q])
        for zz in range(4):
            ref = buf(ch, 4 * zz + lax.rem(c + 2, 4))
            rcopy(ref, ref, csn.at[q], crc.at[q], cpeer).start()

    @jax.named_scope("gather_end")
    def gather_end(buf, ch, o):
        q = ch + o
        wait_for(XA.at[0, pl.ds(0, 8 * SH)], crc.at[q])
        for zz in range(3):
            @pl.when(z == zz)
            def _():
                wait_for(XA.at[0, pl.ds(0, (zz + 1) * SH)], zsu.at[q])

            @pl.when(z == 3 - zz)
            def _():
                wait_for(XA.at[0, pl.ds(0, (zz + 1) * SH)], zsd.at[q])
        wait_for(XA.at[0, pl.ds(0, 4 * SH)], ysn.at[q])
        wait_for(XA.at[0, pl.ds(0, 8 * SH)], csn.at[q])

    NPC = GP + 3

    def lane(zz):
        return lan(zz * RW, RW)

    PQ, PA, PB = 0, GP + 1, GP + 2

    def kind(p):
        return p if isinstance(p, int) and (p == PQ or p > GP) else 1

    def w_ref(l, p, zz, half):
        if kind(p) == PQ:
            return WQ.at[l, sub(80 * half, 80), lane(zz)]
        if kind(p) == PA:
            return WO.at[l, sub(400 * half, 160), lane(zz)]
        if kind(p) == PB:
            return WO.at[l, sub(160 + 400 * half, 240), lane(zz)]
        return GU.at[l, half, sub(zz * RW + GR * (p - 1), GR), :]

    def w_send(l, kind_, m, mr=MR):
        r = mr * m
        for h in HOPS:
            t = lax.rem(z + h, 4)
            if kind_ == "q":
                p, src = PQ, WT.at[l, sub(SH * t + 80 * x + r, mr), :]
                dst = WQ.at[l, sub(80 * x + r, mr), lane(z)]
            elif kind_ == "g":
                p, src = 1 + r // GR, w_in.at[l, sub(r, mr), lan(RW + D * x + FB * t, FB)]
                dst = GU.at[l, x, sub(z * RW + r, mr), :]
            elif kind_ == "a":
                p, src = PA, w_out.at[l, sub(jnp.where(x == 0, SH * t, RW + FB * t + 240) + r, mr), :]
                dst = WO.at[l, sub(400 * x + r, mr), lane(z)]
            else:
                p, src = PB, w_out.at[l, sub(RW + FB * t + 400 * x + r, mr), :]
                dst = WO.at[l, sub(160 + 400 * x + r, mr), lane(z)]
            rcopy(src, dst, ws.at[l, p], wr.at[l, p, h - 1], zpeer[h - 1]).start()

    def rest_send(l, m):
        whole = -(-m // PM)
        for v in range(m, whole * PM):
            w_send(l, "g", v)
        for v in range(whole, GP):
            w_send(l, "g", v, GR)

    NQ, NG, NA, NB = 80 // MR, RW // MR, 160 // MR, 240 // MR

    @jax.named_scope("w_forward")
    def w_forward(l, p):
        for h in HOPS:
            ref = w_ref(l, p, lax.rem(z - h + 4, 4), x)
            wait_for(ref, wr.at[l, p, h - 1])
            rcopy(ref, ref, xs.at[l, p], xr.at[l, p, h - 1], xpeer).start()

    def w_size(l, p):
        if kind(p) == PQ:
            return WQ.at[l, pl.ds(0, 80), pl.ds(0, 3 * RW)]
        if kind(p) == PA:
            return WO.at[l, pl.ds(0, 160), pl.ds(0, 3 * RW)]
        if kind(p) == PB:
            return WO.at[l, pl.ds(0, 240), pl.ds(0, 3 * RW)]
        return GU.at[l, 0, pl.ds(0, 3 * GR), :]

    @jax.named_scope("w_arrive")
    def w_arrive(l, p):
        for h in HOPS:
            wait_for(w_ref(l, p, 0, 0), xr.at[l, p, h - 1])

    def w_own(l):
        return [
            None,
            pltpu.make_async_copy(w_in.at[l, :, lan(RW + FB * z, FB)], GU.at[l, 0, sub(z * RW, RW), :], own.at[l, 1]),
            pltpu.make_async_copy(w_in.at[l, :, lan(RW + D + FB * z, FB)], GU.at[l, 1, sub(z * RW, RW), :], own.at[l, 2]),
            pltpu.make_async_copy(w_out.at[l, sub(SH * z, SH), :], WO.at[l, pl.ds(0, SH), lane(z)], own.at[l, 3]),
            pltpu.make_async_copy(w_out.at[l, sub(RW + FB * z, FB), :], WO.at[l, pl.ds(SH, FB), lane(z)], own.at[l, 4]),
        ]

    def seq_part(ref, n):
        return ref.at[n // SPC, :, lan(lax.rem(n, SPC) * CW, CW)]

    q_in = [pltpu.make_async_copy(w_in.at[l, :, pl.ds(0, RW)], GU.at[1, l, sub(z * RW, RW), :], own.at[l, 5]) for l in range(2)]
    for cp in q_in:
        cp.start()
    gather_own(ein, ext, 0, 0)
    for ch in range(NT):
        gather_own(seq_part(xin, ch), act, ch, NE)
    ext(0, me)[...] = ein[...]

    def put_own(ch):
        XA[ch, rows(me)] = seq_part(xin, ch)[...]
    loop(NT, put_own)
    for cp in w_own(0)[1:]:
        cp.start()
    for l in range(2):
        q_in[l].wait()
        WT[l] = GU[1, l, sub(z * RW, RW), :].T
        WQ[l, :, lane(z)] = WT[l, sub(SH * z, SH), :]
    w_send(0, "q", 0, 80)
    for cp in w_own(1)[1:]:
        cp.start()
    done = 0
    for e in range(2 * NT):
        if e % NT == 0:
            gather_hop(ext, 0, 0, e // NT + 1)
        gather_hop(act, e % NT, NE, e // NT + 1)
        for v in range(S0[e]):
            w_send(0, "g", done)
            done += 1

    @jax.named_scope("unpack")
    def unpack():
        loop(NE, lambda ch: gather_end(ext, ch, 0))

        def shard(s):
            zz, cc = s // 4, lax.rem(s, 4)
            for b in range(5):
                lo = 128 * (b // 2)
                i = 16 * (lo // CW) + s
                blk = MT[i // 5, sub(lax.rem(i, 5) * SH + 80 * (b % 2), 80), lo % CW:lo % CW + 128].astype(F32)
                for l in range(2):
                    WKV[l, sub(48 * cc, 40), lan(zz * RW + 128 * b, 128)] = blk[40 * l:40 * l + 40].astype(BF)
            i = 16 * (NE - 1) + s
            blk = MT[i // 5, rows(lax.rem(i, 5)), CW - 128:CW].astype(F32)
            for l in range(2):
                GB[l, rows(s), :] = jnp.broadcast_to(blk[:, l:l + 1], (SH, 128)).astype(BF)
        loop(16, shard)
        for l in range(2):
            for cc in range(4):
                WKV[l, 48 * cc + 40:48 * cc + 48, :] = jnp.zeros((8, D), BF)

    BR = 32

    @jax.named_scope("norm")
    def norm(l, n):
        def fold(v):
            return v.reshape(BR // 8, 8, CW).sum(0)

        def load(i):
            return XA[n, sub(i * BR, BR), :].astype(F32)

        tot = lax.fori_loop(0, D // BR, lambda i, a: a + fold(load(i)), jnp.zeros((8, CW), F32), unroll=4)
        mean = jnp.sum(tot, axis=0, keepdims=True) / D

        def square(i, a):
            d = load(i) - mean
            return a + fold(d * d)
        var = jnp.sum(lax.fori_loop(0, D // BR, square, jnp.zeros((8, CW), F32), unroll=4), axis=0, keepdims=True) / D
        scale = lax.rsqrt(var + LN_EPS)

        def put(i, a):
            g = jnp.concatenate([GB[l, sub(i * BR, BR), :].astype(F32)] * (CW // 128), axis=1)
            XA[n, sub(i * BR, BR), :] = ((load(i) - mean) * scale * g).astype(BF)
            return a
        lax.fori_loop(0, D // BR, put, 0, unroll=4)

    def tok(n):
        return lan(n * CW, CW)

    @jax.named_scope("qkv")
    def qkv(l, n):
        pos = lan(lax.rem(n * CW, SEQ), CW)
        co, si = cs[0, :, pos], cs[1, :, pos]
        h = XA[n]
        kv = jnp.dot(WKV[l], h, preferred_element_type=F32).astype(BF).astype(F32)

        def rot(lo, hi):
            return jnp.concatenate([lo * co - hi * si, hi * co + lo * si], axis=0)
        KT[:, tok(n)] = rot(kv[0:40], kv[48:88]).astype(BF)
        VT[:, tok(n)] = jnp.concatenate([kv[96:136], kv[144:184]], axis=0).astype(BF)
        qq = jnp.dot(WQ[l], h, preferred_element_type=F32).astype(BF).astype(F32)
        for hd in range(2):
            QT[HD * hd:HD * hd + HD, tok(n)] = (rot(qq[HD * hd:HD * hd + HALF], qq[HD * hd + HALF:HD * hd + HD]) * HD ** -0.5).astype(BF)

    @jax.named_scope("attention")
    def attention(b):
        def body(hd):
            hr = sub(hd * HD, HD)
            for i in range(SEQ // QB):
                nk = QB * (i + 1)
                ks = lan(b * SEQ, nk)
                qs = lan(b * SEQ + QB * i, QB)
                s = dot_ta(KT[:, ks], QT[hr, qs])
                keep = lax.broadcasted_iota(jnp.int32, (QB, QB), 0) <= lax.broadcasted_iota(jnp.int32, (QB, QB), 1)
                last = jnp.where(keep, s[nk - QB:], -1e30)
                s = jnp.concatenate([s[:nk - QB], last], axis=0) if i else last
                e = jnp.exp(s - jnp.max(s, axis=0, keepdims=True))
                pr = (e * (1.0 / jnp.sum(e, axis=0, keepdims=True))).astype(BF)
                MT[b * (SEQ // CW) + QB * i // CW, hr, QB * i % CW:QB * i % CW + QB] = jnp.dot(VT[:, ks], pr, preferred_element_type=F32).astype(BF)
        loop(2, body)

    @jax.named_scope("gate_up")
    def gate_up(l, n):
        h = XA[n]
        g = dot_ta(GU[l, 0], h).astype(BF).astype(F32)
        u = dot_ta(GU[l, 1], h).astype(BF).astype(F32)
        MT[n, SH:SH + FB, :] = (g * lax.logistic(g) * u).astype(BF)

    def f(ref_value):
        return ref_value.astype(F32)

    NU = 4 * NT

    def unit(i):
        j = i // NT
        return jnp.where(j == 0, 3, jnp.where(j == 1, 0, jnp.where(j == 2, 2, 1))), lax.rem(i, NT)

    @jax.named_scope("red_a")
    def red_a(l, i):
        zz, n = unit(i)
        slot = lax.rem(i, SCN)

        @pl.when(i >= SCN)
        def _():
            wait_for(SC.at[slot], rcs.at[i - SCN])

        XA[n, sub(zz * RW, RW), :] = dot_ta(WO[l, :, lane(zz)], MT[n]).astype(BF)
        for yy in range(2):
            SC[slot, yy] = XA[n, rows(4 * zz + 2 * yy + 1 - k)]
        for yy in range(2):
            rcopy(SC.at[slot, yy], RC.at[n, 2 * zz + yy], rcs.at[i], rcr.at[i], cpeer).start()

    @jax.named_scope("red_b")
    def red_b(i):
        zz, n = unit(i)
        slot = lax.rem(i, SYN)
        wait_for(RC.at[n, pl.ds(2 * zz, 2)], rcr.at[i])

        @pl.when(i >= SYN)
        def _():
            wait_for(SY.at[slot], rys.at[i - SYN])

        SY[slot] = (f(XA[n, rows(4 * zz + 2 * (1 - y) + k)]) + f(RC[n, 2 * zz + 1 - y])).astype(BF)
        rcopy(SY.at[slot], RY.at[n, zz], rys.at[i], ryr.at[i], ypeer).start()

    def send_up(n, zz, i):
        rcopy(SZ.at[n, zz], RU.at[n, zz - 1], rsz.at[i], rzu.at[i], up).start()

    def send_down(n, zz, i):
        rcopy(SZ.at[n, zz], RD.at[n, zz], rsz.at[i], rzd.at[i], down).start()

    @jax.named_scope("red_c")
    def red_c(i):
        zz, n = unit(i)
        wait_for(RY.at[n, zz], ryr.at[i])
        SZ[n, zz] = (f(XA[n, rows(4 * zz + c)]) + f(RC[n, 2 * zz + y]) + f(RY[n, zz])).astype(BF)

        @pl.when((z == 0) & (zz > 0))
        def _():
            send_up(n, zz, i)

        @pl.when((z == 3) & (zz < 3))
        def _():
            send_down(n, zz, i)

    def relay_up(i):
        zz, n = unit(i)
        wait_for(RU.at[n, zz - 1], rzu.at[i])
        SZ[n, zz] = (f(SZ[n, zz]) + f(RU[n, zz - 1])).astype(BF)
        send_up(n, zz, i)

    def relay_down(i):
        zz, n = unit(i)
        wait_for(RD.at[n, zz], rzd.at[i])
        SZ[n, zz] = (f(SZ[n, zz]) + f(RD[n, zz])).astype(BF)
        send_down(n, zz, i)

    @jax.named_scope("red_d")
    def red_d(i):
        zz, _ = unit(i)

        @pl.when((z == 1) & (zz > 1))
        def _():
            relay_up(i)

        @pl.when((z == 2) & (zz < 2))
        def _():
            relay_down(i)

    @jax.named_scope("red_e")
    def red_e(i):
        zz, _ = unit(i)

        @pl.when((z == 2) & (zz > 2))
        def _():
            relay_up(i)

        @pl.when((z == 1) & (zz < 1))
        def _():
            relay_down(i)

    @jax.named_scope("red_f")
    def red_f(l, i):
        zz, n = unit(i)

        def finish(u):
            u = u.astype(BF)

            @pl.when(l == 0)
            def _():
                out = (f(seq_part(xin, n)[...]) + f(u)).astype(BF)
                XO[n] = out
                XA[n, rows(me)] = out
                gather_own(XO.at[n], act, n, NE)

            @pl.when(l == 1)
            def _():
                seq_part(yT, n)[...] = (f(XO[n]) + f(u)).astype(BF)

        @pl.when((z == 0) & (zz == 0))
        def _():
            wait_for(RD.at[n, 0], rzd.at[i])
            finish(f(SZ[n, 0]) + f(RD[n, 0]))

        @pl.when((z == 3) & (zz == 3))
        def _():
            wait_for(RU.at[n, 2], rzu.at[i])
            finish(f(SZ[n, 3]) + f(RU[n, 2]))

        for v in (1, 2):
            @pl.when((z == v) & (zz == v))
            def _():
                wait_for(RU.at[n, v - 1], rzu.at[i])
                wait_for(RD.at[n, v], rzd.at[i])
                finish(f(SZ[n, v]) + f(RU[n, v - 1]) + f(RD[n, v]))

        @pl.when(i >= NU - SCN)
        def _():
            wait_for(SC.at[0], rcs.at[i])

        @pl.when(i >= NU - SYN)
        def _():
            wait_for(SY.at[0], rys.at[i])

        @pl.when(zz != z)
        def _():
            wait_for(SZ.at[n, zz], rsz.at[i])

    shard = me

    def o_forward(l, j):
        zz = unit(NT * j)[0]
        h = lax.rem(z - zz + 4, 4)

        @pl.when(h > 0)
        def _():
            for p in (PA, PB):
                ref = w_ref(l, p, zz, x)
                wait_for(ref, wr.at[l, p, h - 1])
                rcopy(ref, ref, xs.at[l, p], xr.at[l, p, h - 1], xpeer).start()

    def o_arrive(l, j):
        zz = unit(NT * j)[0]
        h = lax.rem(z - zz + 4, 4)

        @pl.when(h > 0)
        def _():
            for p in (PA, PB):
                wait_for(w_ref(l, p, zz, 1 - x), xr.at[l, p, h - 1])

    def o_at(l, place):
        for ll in range(2):
            for at, cond in ((OEND[ll], (z == 0) | (z == 3)), (OMID[ll], (z == 1) | (z == 2))):
                if isinstance(place, int):
                    if place == at:
                        @pl.when((l == ll) & cond)
                        def _():
                            o_send(l)
                elif 0 < at <= NT:
                    @pl.when((l == ll) & cond & (place == at))
                    def _():
                        o_send(l)

    def o_send(l):
        w_send(l, "a", 0, 160)
        w_send(l, "b", 0, 240)

    def layer(l):
        @pl.when(l == 1)
        def _():
            done = RS0
            for e in range(2 * NT):
                gather_hop(act, e % NT, NE, e // NT + 1)
                for v in range(AG1[e]):
                    w_send(1, "g", done)
                    done += 1
                for p in EVENTS[e]:
                    w_forward(1, p)

        for ll, sent in enumerate((sum(S0), RS0 + sum(AG1))):
            @pl.when(l == ll)
            def _():
                rest_send(ll, sent)
        o_at(l, 0)

        def last(n):
            @pl.when(n < NT)
            def _():
                @pl.when((l == 0) & (n == 0))
                def _():
                    gather_hop(ext, 0, 0, len(HOPS))
                gather_hop(act, n, NE, len(HOPS))
                for v in range(NT):
                    if EVENTS[2 * NT + v]:
                        @pl.when((l == 1) & (n == v))
                        def _():
                            for p in EVENTS[2 * NT + v]:
                                w_forward(1, p)

                @pl.when((l == 0) & (n == 0))
                def _():
                    gather_cross(ext, 0, 0)
                gather_cross(act, n, NE)

            @pl.when(n > 0)
            def _():
                chunk(n - 1)

        def chunk(n):
            @pl.when(n == 0)
            def _():
                @pl.when(l == 0)
                def _():
                    unpack()
                    w_forward(0, PQ)
                for cp in w_own(l)[1:]:
                    cp.wait()
            gather_end(act, n, NE)
            norm(l, n)

            @pl.when(n == 0)
            def _():
                w_arrive(l, PQ)
            qkv(l, n)

            late = jnp.where(l == 0, 1, LATE) + n

            @pl.when(late <= GP)
            def _():
                w_forward(l, late)

            @pl.when(lax.rem(n, SPC) == SPC - 1)
            def _():
                attention(n // SPC)
            o_at(l, n + 1)
        loop(NT + 1, last)
        o_at(l, NT + 1)
        for b in range(2):
            off = lan(b * SEQ + LANES * (shard // 2), LANES)
            for v, ref in enumerate((KT, VT)):
                KVT[...] = ref[:, off].astype(F32).T
                kvo[l, v, b] = KVT[sub(64 * lax.rem(shard, 2), 64), :].astype(BF)
        fwd = jnp.where(l == 0, NT, min(GP, LATE - 1 + NT))
        loop(GP - fwd, lambda p: w_forward(l, fwd + 1 + p))
        o_at(l, NT + 2)
        loop(GP, lambda p: w_arrive(l, p + 1))
        o_forward(l, 0)
        gh = jnp.where(l == 0, GH0, GH1)
        loop(gh, lambda n: gate_up(l, n))

        def step(i):
            @pl.when(i < NU)
            def _():
                for j, u in enumerate(OF):
                    @pl.when(i == u)
                    def _():
                        o_forward(l, j + 1)

                @pl.when(lax.rem(i, NT) == 0)
                def _():
                    o_arrive(l, i // NT)

                @pl.when((i >= gh) & (i < NT))
                def _():
                    gate_up(l, i)
                red_a(l, i)
            for lag, stage in zip(LAGS, (red_b, red_c, red_d, red_e, functools.partial(red_f, l))):
                @pl.when((i >= lag) & (i < NU + lag))
                def _():
                    stage(i - lag)

            @pl.when(l == 0)
            def _():
                @pl.when(i == RQ)
                def _():
                    w_send(1, "q", 0, 80)

                @pl.when(i == RQ + 12)
                def _():
                    w_forward(1, PQ)

                for u, each in enumerate(SU):
                    if each:
                        @pl.when(i == u)
                        def _():
                            loop(each, lambda v: w_send(1, "g", sum(SU[:u]) + v))

                for u, ps in enumerate(UNITS):
                    if ps:
                        @pl.when(i == u)
                        def _():
                            for p in ps:
                                w_forward(1, p)
        loop(NU + LAGS[-1], step)

    loop(2, layer)

    for l in range(2):
        for p in range(NPC):
            wait_for(w_size(l, p), ws.at[l, p])
            wait_for(w_size(l, p), xs.at[l, p])


def solution(mesh):
    act_spec = P("dp", None, ("row", "col"))
    weight_spec = P(None, "row", "col")

    def device_fn(x_loc, gain_loc, w_in_loc, w_kv_loc, w_out_loc):
        kv = jnp.transpose(w_kv_loc, (0, 2, 1)).reshape(HD, RW)
        kv = jnp.concatenate([jnp.concatenate([kv[:, v:v + LANES], kv[:, v + LANES:v + 2 * LANES]], axis=0) for v in (0, 2 * LANES)] + [jnp.pad(kv[:, 4 * LANES:], ((0, SH - HD), (0, 0)))], axis=1)
        gain = jnp.pad(gain_loc.T, ((0, 0), (0, LANES - 2)))
        ein = jnp.concatenate([kv, gain], axis=1)
        NPC = GP + 3
        dma = pltpu.SemaphoreType.DMA
        hbm = pl.BlockSpec(memory_space=pl.ANY)
        vmem = pl.BlockSpec(memory_space=pltpu.VMEM)
        y_t, kvo = pl.pallas_call(
            kernel,
            out_shape=(jax.ShapeDtypeStruct((2, SH, SEQ), BF), jax.ShapeDtypeStruct((2, 2, 2, SEQ // 16, HD), BF)),
            in_specs=[vmem, vmem, hbm, hbm, vmem],
            out_specs=(vmem, vmem),
            scratch_shapes=[
                pltpu.VMEM((LANES, HD), F32),
                pltpu.VMEM((2, RW, RW), BF),
                pltpu.VMEM((NT, D, CW), BF),
                pltpu.VMEM((2, 2, D, FB), BF),
                pltpu.VMEM((2, SH, D), BF),
                pltpu.VMEM((2, 192, D), BF),
                pltpu.VMEM((2, SH + FB, D), BF),
                pltpu.VMEM((2, D, 128), BF),
                pltpu.VMEM((NT, SH + FB, CW), BF),
                pltpu.VMEM((SH, T), BF),
                pltpu.VMEM((HD, T), BF),
                pltpu.VMEM((HD, T), BF),
                pltpu.VMEM((NT, SH, CW), BF),
                pltpu.VMEM((NT, 8, SH, CW), BF),
                pltpu.VMEM((NT, 4, SH, CW), BF),
                pltpu.VMEM((NT, 3, SH, CW), BF),
                pltpu.VMEM((NT, 3, SH, CW), BF),
                pltpu.VMEM((SCN, 2, SH, CW), BF),
                pltpu.VMEM((SYN, SH, CW), BF),
                pltpu.VMEM((NT, 4, SH, CW), BF),
                dma((NC,)), dma((NC,)), dma((NC,)), dma((NC,)),
                dma((NC, 2, 3)), dma((NC,)), dma((NC,)),
                dma((4 * NT,)), dma((4 * NT,)), dma((4 * NT,)), dma((4 * NT,)),
                dma((4 * NT,)), dma((4 * NT,)), dma((4 * NT,)),
                dma((2, NPC)), dma((2, NPC, 3)), dma((2, NPC)), dma((2, NPC, 3)),
                dma((2, 6)),
            ],
            compiler_params=pltpu.CompilerParams(collective_id=0, has_side_effects=True, vmem_limit_bytes=67043328),
        )(jnp.transpose(x_loc, (0, 2, 1)), ein, w_in_loc, w_out_loc, rope_tables())
        return jnp.transpose(y_t, (0, 2, 1)), kvo

    return jax.shard_map(device_fn, mesh=mesh, in_specs=(act_spec, P(None, ("row", "col")), weight_spec, weight_spec, P(None, "col", "row")), out_specs=(act_spec, P(None, None, "dp", ("row", "col"), None)), check_vma=False)
```

```python
import functools

import jax
import jax.numpy as jnp
from jax import lax
from jax.experimental import pallas as pl
from jax.experimental.pallas import tpu as pltpu
from jax.sharding import PartitionSpec as P

BF = jnp.bfloat16
F32 = jnp.float32
MESH_ID = pl.DeviceIdType.MESH
LN_EPS = 1e-6

D = 2560
SH = 160
RW = 640
FB = 640
HD = 80
HALF = HD // 2
SEQ = 1024
T = 2 * SEQ
CW = 512
NT = T // CW
NE = 512 // CW
NC = NE + NT
SPC = SEQ // CW
GP = 8
GR = RW // GP
LANES = 128
HOPS = (1, 2, 3)
QB = 256
SCN, SYN = 4, 6
MR = 16
LAGS = (1, 4, 7, 12, 15)
PM = GR // MR
S0 = (1,) * 8
GH0, GH1 = 1, 3
OEND = (4, 0)
OMID = (5, 5)
OF = (0, 4, 8)
RQ = 0
SU = (0,) + (2,) * 10
AG1 = (0,) * 8
UFW, EFW = 30, 12


def weight_plan():
    sent, when = 0, []
    for i, each in enumerate(SU):
        when += [i] * each
        sent += each
    units = [[] for _ in range(4 * NT + LAGS[-1])]
    events = [[] for _ in range(3 * NT)]
    late = list(range(1, GP + 1))
    ev = []
    for e in range(2 * NT):
        ev += [e] * AG1[e]
    for p in range(1, GP + 1):
        last = PM * p - 1
        if last < sent:
            if when[last] + UFW < len(units):
                units[when[last] + UFW].append(p)
                late.remove(p)
                continue
            e = max(0, when[last] + UFW - len(units))
        elif last < sent + len(ev):
            e = ev[last - sent] + EFW
        else:
            continue
        if e < 3 * NT:
            events[e].append(p)
            late.remove(p)
    return sent, units, events, late[0] if late else GP + 1


RS0, UNITS, EVENTS, LATE = weight_plan()


def rope_tables():
    inv_freq = 1.0 / (10000.0 ** (jnp.arange(HALF, dtype=F32) * 2.0 / HD))
    angles = inv_freq[:, None] * jnp.arange(SEQ).astype(F32)[None, :]
    return jnp.stack([jnp.cos(angles), jnp.sin(angles)])


def sub(start, size):
    return pl.ds(pl.multiple_of(start, 16), size)


def lan(start, size):
    return pl.ds(pl.multiple_of(start, LANES), size)


def dot_ta(a, b):
    return lax.dot_general(a, b, (((0,), (0,)), ((), ())), preferred_element_type=F32)


def kernel(xin, ein, w_in, w_out, cs, yT, kvo, KVT, WT, XA, GU, WQ, WKV, WO, GB, MT, QT, KT, VT, XO, RC, RY, RU, RD, SC, SY, SZ,
           zsu, zsd, ysn, csn, zrc, yrc, crc, rcs, rcr, rys, ryr, rzu, rzd, rsz, ws, wr, xs, xr, own):
    x = lax.axis_index("dp")
    z = lax.axis_index("row")
    c = lax.axis_index("col")
    y, k = c // 2, lax.rem(c, 2)
    me = 4 * z + c
    up = (x, jnp.minimum(z + 1, 3), c)
    down = (x, jnp.maximum(z - 1, 0), c)
    ypeer = (x, z, lax.rem(c + 2, 4))
    cpeer = (x, z, c + 1 - 2 * k)
    xpeer = (1 - x, z, c)
    zpeer = [(x, lax.rem(z + h, 4), c) for h in HOPS]

    def rcopy(src, dst, ss, rs, dev):
        return pltpu.make_async_remote_copy(src_ref=src, dst_ref=dst, send_sem=ss, recv_sem=rs, device_id=dev, device_id_type=MESH_ID)

    def wait_for(ref, sem):
        pltpu.make_async_copy(ref, ref, sem).wait()

    def rows(s):
        return sub(s * SH, SH)

    def loop(n, body):
        def step(i, carry):
            body(i)
            return carry
        lax.fori_loop(0, n, step, 0)

    barrier = pltpu.get_barrier_semaphore()
    for dev in zpeer + [ypeer, cpeer, xpeer]:
        pl.semaphore_signal(barrier, inc=1, device_id=dev, device_id_type=MESH_ID)
    pl.semaphore_wait(barrier, 6)

    def act(ch, s):
        return XA.at[ch, rows(s)]

    def ext(ch, s):
        i = 16 * ch + s
        return MT.at[i // 5, rows(lax.rem(i, 5))]

    @jax.named_scope("gather_own")
    def gather_own(src, buf, ch, o):
        q = ch + o
        dst = buf(ch, me)

        @pl.when(z < 3)
        def _():
            rcopy(src, dst, zsu.at[q], zrc.at[q, 0, 0], up).start()

        @pl.when(z > 0)
        def _():
            rcopy(src, dst, zsd.at[q], zrc.at[q, 1, 0], down).start()

        rcopy(src, dst, ysn.at[q], yrc.at[q], ypeer).start()
        rcopy(src, dst, csn.at[q], crc.at[q], cpeer).start()

    @jax.named_scope("gather_hop")
    def gather_hop(buf, ch, o, hop):
        q = ch + o

        @pl.when(z - hop >= 0)
        def _():
            ref = buf(ch, jnp.maximum(me - 4 * hop, 0))
            wait_for(ref, zrc.at[q, 0, hop - 1])
            if hop < 3:
                @pl.when(z < 3)
                def _():
                    rcopy(ref, ref, zsu.at[q], zrc.at[q, 0, hop], up).start()
            rcopy(ref, ref, ysn.at[q], yrc.at[q], ypeer).start()
            rcopy(ref, ref, csn.at[q], crc.at[q], cpeer).start()

        @pl.when(z + hop <= 3)
        def _():
            ref = buf(ch, jnp.minimum(me + 4 * hop, 15))
            wait_for(ref, zrc.at[q, 1, hop - 1])
            if hop < 3:
                @pl.when(z > 0)
                def _():
                    rcopy(ref, ref, zsd.at[q], zrc.at[q, 1, hop], down).start()
            rcopy(ref, ref, ysn.at[q], yrc.at[q], ypeer).start()
            rcopy(ref, ref, csn.at[q], crc.at[q], cpeer).start()

    @jax.named_scope("gather_cross")
    def gather_cross(buf, ch, o):
        q = ch + o
        wait_for(XA.at[0, pl.ds(0, 4 * SH)], yrc.at[q])
        for zz in range(4):
            ref = buf(ch, 4 * zz + lax.rem(c + 2, 4))
            rcopy(ref, ref, csn.at[q], crc.at[q], cpeer).start()

    @jax.named_scope("gather_end")
    def gather_end(buf, ch, o):
        q = ch + o
        wait_for(XA.at[0, pl.ds(0, 8 * SH)], crc.at[q])
        for zz in range(3):
            @pl.when(z == zz)
            def _():
                wait_for(XA.at[0, pl.ds(0, (zz + 1) * SH)], zsu.at[q])

            @pl.when(z == 3 - zz)
            def _():
                wait_for(XA.at[0, pl.ds(0, (zz + 1) * SH)], zsd.at[q])
        wait_for(XA.at[0, pl.ds(0, 4 * SH)], ysn.at[q])
        wait_for(XA.at[0, pl.ds(0, 8 * SH)], csn.at[q])

    NPC = GP + 3

    def lane(zz):
        return lan(zz * RW, RW)

    PQ, PA, PB = 0, GP + 1, GP + 2

    def kind(p):
        return p if isinstance(p, int) and (p == PQ or p > GP) else 1

    def w_ref(l, p, zz, half):
        if kind(p) == PQ:
            return WQ.at[l, sub(80 * half, 80), lane(zz)]
        if kind(p) == PA:
            return WO.at[l, sub(400 * half, 160), lane(zz)]
        if kind(p) == PB:
            return WO.at[l, sub(160 + 400 * half, 240), lane(zz)]
        return GU.at[l, half, sub(zz * RW + GR * (p - 1), GR), :]

    def w_send(l, kind_, m, mr=MR):
        r = mr * m
        for h in HOPS:
            t = lax.rem(z + h, 4)
            if kind_ == "q":
                p, src = PQ, WT.at[l, sub(SH * t + 80 * x + r, mr), :]
                dst = WQ.at[l, sub(80 * x + r, mr), lane(z)]
            elif kind_ == "g":
                p, src = 1 + r // GR, w_in.at[l, sub(r, mr), lan(RW + D * x + FB * t, FB)]
                dst = GU.at[l, x, sub(z * RW + r, mr), :]
            elif kind_ == "a":
                p, src = PA, w_out.at[l, sub(jnp.where(x == 0, SH * t, RW + FB * t + 240) + r, mr), :]
                dst = WO.at[l, sub(400 * x + r, mr), lane(z)]
            else:
                p, src = PB, w_out.at[l, sub(RW + FB * t + 400 * x + r, mr), :]
                dst = WO.at[l, sub(160 + 400 * x + r, mr), lane(z)]
            rcopy(src, dst, ws.at[l, p], wr.at[l, p, h - 1], zpeer[h - 1]).start()

    def rest_send(l, m):
        whole = -(-m // PM)
        for v in range(m, whole * PM):
            w_send(l, "g", v)
        for v in range(whole, GP):
            w_send(l, "g", v, GR)

    NQ, NG, NA, NB = 80 // MR, RW // MR, 160 // MR, 240 // MR

    @jax.named_scope("w_forward")
    def w_forward(l, p):
        for h in HOPS:
            ref = w_ref(l, p, lax.rem(z - h + 4, 4), x)
            wait_for(ref, wr.at[l, p, h - 1])
            rcopy(ref, ref, xs.at[l, p], xr.at[l, p, h - 1], xpeer).start()

    def w_size(l, p):
        if kind(p) == PQ:
            return WQ.at[l, pl.ds(0, 80), pl.ds(0, 3 * RW)]
        if kind(p) == PA:
            return WO.at[l, pl.ds(0, 160), pl.ds(0, 3 * RW)]
        if kind(p) == PB:
            return WO.at[l, pl.ds(0, 240), pl.ds(0, 3 * RW)]
        return GU.at[l, 0, pl.ds(0, 3 * GR), :]

    @jax.named_scope("w_arrive")
    def w_arrive(l, p):
        for h in HOPS:
            wait_for(w_ref(l, p, 0, 0), xr.at[l, p, h - 1])

    def w_own(l):
        return [
            None,
            pltpu.make_async_copy(w_in.at[l, :, lan(RW + FB * z, FB)], GU.at[l, 0, sub(z * RW, RW), :], own.at[l, 1]),
            pltpu.make_async_copy(w_in.at[l, :, lan(RW + D + FB * z, FB)], GU.at[l, 1, sub(z * RW, RW), :], own.at[l, 2]),
            pltpu.make_async_copy(w_out.at[l, sub(SH * z, SH), :], WO.at[l, pl.ds(0, SH), lane(z)], own.at[l, 3]),
            pltpu.make_async_copy(w_out.at[l, sub(RW + FB * z, FB), :], WO.at[l, pl.ds(SH, FB), lane(z)], own.at[l, 4]),
        ]

    def seq_part(ref, n):
        return ref.at[n // SPC, :, lan(lax.rem(n, SPC) * CW, CW)]

    q_in = [pltpu.make_async_copy(w_in.at[l, :, pl.ds(0, RW)], GU.at[1, l, sub(z * RW, RW), :], own.at[l, 5]) for l in range(2)]
    for cp in q_in:
        cp.start()
    gather_own(ein, ext, 0, 0)
    for ch in range(NT):
        gather_own(seq_part(xin, ch), act, ch, NE)
    ext(0, me)[...] = ein[...]

    def put_own(ch):
        XA[ch, rows(me)] = seq_part(xin, ch)[...]
    loop(NT, put_own)
    for cp in w_own(0)[1:]:
        cp.start()
    for l in range(2):
        q_in[l].wait()
        WT[l] = GU[1, l, sub(z * RW, RW), :].T
        WQ[l, :, lane(z)] = WT[l, sub(SH * z, SH), :]
    w_send(0, "q", 0, 80)
    for cp in w_own(1)[1:]:
        cp.start()
    done = 0
    for e in range(2 * NT):
        if e % NT == 0:
            gather_hop(ext, 0, 0, e // NT + 1)
        gather_hop(act, e % NT, NE, e // NT + 1)
        for v in range(S0[e]):
            w_send(0, "g", done)
            done += 1

    @jax.named_scope("unpack")
    def unpack():
        loop(NE, lambda ch: gather_end(ext, ch, 0))

        def shard(s):
            zz, cc = s // 4, lax.rem(s, 4)
            for b in range(5):
                lo = 128 * (b // 2)
                i = 16 * (lo // CW) + s
                blk = MT[i // 5, sub(lax.rem(i, 5) * SH + 80 * (b % 2), 80), lo % CW:lo % CW + 128].astype(F32)
                for l in range(2):
                    WKV[l, sub(48 * cc, 40), lan(zz * RW + 128 * b, 128)] = blk[40 * l:40 * l + 40].astype(BF)
            i = 16 * (NE - 1) + s
            blk = MT[i // 5, rows(lax.rem(i, 5)), CW - 128:CW].astype(F32)
            for l in range(2):
                GB[l, rows(s), :] = jnp.broadcast_to(blk[:, l:l + 1], (SH, 128)).astype(BF)
        loop(16, shard)
        for l in range(2):
            for cc in range(4):
                WKV[l, 48 * cc + 40:48 * cc + 48, :] = jnp.zeros((8, D), BF)

    BR = 32

    @jax.named_scope("norm")
    def norm(l, n):
        def fold(v):
            return v.reshape(BR // 8, 8, CW).sum(0)

        def load(i):
            return XA[n, sub(i * BR, BR), :].astype(F32)

        tot = lax.fori_loop(0, D // BR, lambda i, a: a + fold(load(i)), jnp.zeros((8, CW), F32), unroll=4)
        mean = jnp.sum(tot, axis=0, keepdims=True) / D

        def square(i, a):
            d = load(i) - mean
            return a + fold(d * d)
        var = jnp.sum(lax.fori_loop(0, D // BR, square, jnp.zeros((8, CW), F32), unroll=4), axis=0, keepdims=True) / D
        scale = lax.rsqrt(var + LN_EPS)

        def put(i, a):
            g = jnp.concatenate([GB[l, sub(i * BR, BR), :].astype(F32)] * (CW // 128), axis=1)
            XA[n, sub(i * BR, BR), :] = ((load(i) - mean) * scale * g).astype(BF)
            return a
        lax.fori_loop(0, D // BR, put, 0, unroll=4)

    def tok(n):
        return lan(n * CW, CW)

    @jax.named_scope("qkv")
    def qkv(l, n):
        pos = lan(lax.rem(n * CW, SEQ), CW)
        co, si = cs[0, :, pos], cs[1, :, pos]
        h = XA[n]
        kv = jnp.dot(WKV[l], h, preferred_element_type=F32).astype(BF).astype(F32)

        def rot(lo, hi):
            return jnp.concatenate([lo * co - hi * si, hi * co + lo * si], axis=0)
        KT[:, tok(n)] = rot(kv[0:40], kv[48:88]).astype(BF)
        VT[:, tok(n)] = jnp.concatenate([kv[96:136], kv[144:184]], axis=0).astype(BF)
        qq = jnp.dot(WQ[l], h, preferred_element_type=F32).astype(BF).astype(F32)
        for hd in range(2):
            QT[HD * hd:HD * hd + HD, tok(n)] = (rot(qq[HD * hd:HD * hd + HALF], qq[HD * hd + HALF:HD * hd + HD]) * HD ** -0.5).astype(BF)

    @jax.named_scope("attention")
    def attention(b):
        def body(hd):
            hr = sub(hd * HD, HD)
            for i in range(SEQ // QB):
                nk = QB * (i + 1)
                ks = lan(b * SEQ, nk)
                qs = lan(b * SEQ + QB * i, QB)
                s = dot_ta(KT[:, ks], QT[hr, qs])
                keep = lax.broadcasted_iota(jnp.int32, (QB, QB), 0) <= lax.broadcasted_iota(jnp.int32, (QB, QB), 1)
                last = jnp.where(keep, s[nk - QB:], -1e30)
                s = jnp.concatenate([s[:nk - QB], last], axis=0) if i else last
                e = jnp.exp(s - jnp.max(s, axis=0, keepdims=True))
                pr = (e * (1.0 / jnp.sum(e, axis=0, keepdims=True))).astype(BF)
                MT[b * (SEQ // CW) + QB * i // CW, hr, QB * i % CW:QB * i % CW + QB] = jnp.dot(VT[:, ks], pr, preferred_element_type=F32).astype(BF)
        loop(2, body)

    @jax.named_scope("gate_up")
    def gate_up(l, n):
        h = XA[n]
        g = dot_ta(GU[l, 0], h).astype(BF).astype(F32)
        u = dot_ta(GU[l, 1], h).astype(BF).astype(F32)
        MT[n, SH:SH + FB, :] = (g * lax.logistic(g) * u).astype(BF)

    def f(ref_value):
        return ref_value.astype(F32)

    NU = 4 * NT

    def unit(i):
        j = i // NT
        return jnp.where(j == 0, 3, jnp.where(j == 1, 0, jnp.where(j == 2, 2, 1))), lax.rem(i, NT)

    @jax.named_scope("red_a")
    def red_a(l, i):
        zz, n = unit(i)
        slot = lax.rem(i, SCN)

        @pl.when(i >= SCN)
        def _():
            wait_for(SC.at[slot], rcs.at[i - SCN])

        XA[n, sub(zz * RW, RW), :] = dot_ta(WO[l, :, lane(zz)], MT[n]).astype(BF)
        for yy in range(2):
            SC[slot, yy] = XA[n, rows(4 * zz + 2 * yy + 1 - k)]
        for yy in range(2):
            rcopy(SC.at[slot, yy], RC.at[n, 2 * zz + yy], rcs.at[i], rcr.at[i], cpeer).start()

    @jax.named_scope("red_b")
    def red_b(i):
        zz, n = unit(i)
        slot = lax.rem(i, SYN)
        wait_for(RC.at[n, pl.ds(2 * zz, 2)], rcr.at[i])

        @pl.when(i >= SYN)
        def _():
            wait_for(SY.at[slot], rys.at[i - SYN])

        SY[slot] = (f(XA[n, rows(4 * zz + 2 * (1 - y) + k)]) + f(RC[n, 2 * zz + 1 - y])).astype(BF)
        rcopy(SY.at[slot], RY.at[n, zz], rys.at[i], ryr.at[i], ypeer).start()

    def send_up(n, zz, i):
        rcopy(SZ.at[n, zz], RU.at[n, zz - 1], rsz.at[i], rzu.at[i], up).start()

    def send_down(n, zz, i):
        rcopy(SZ.at[n, zz], RD.at[n, zz], rsz.at[i], rzd.at[i], down).start()

    @jax.named_scope("red_c")
    def red_c(i):
        zz, n = unit(i)
        wait_for(RY.at[n, zz], ryr.at[i])
        SZ[n, zz] = (f(XA[n, rows(4 * zz + c)]) + f(RC[n, 2 * zz + y]) + f(RY[n, zz])).astype(BF)

        @pl.when((z == 0) & (zz > 0))
        def _():
            send_up(n, zz, i)

        @pl.when((z == 3) & (zz < 3))
        def _():
            send_down(n, zz, i)

    def relay_up(i):
        zz, n = unit(i)
        wait_for(RU.at[n, zz - 1], rzu.at[i])
        SZ[n, zz] = (f(SZ[n, zz]) + f(RU[n, zz - 1])).astype(BF)
        send_up(n, zz, i)

    def relay_down(i):
        zz, n = unit(i)
        wait_for(RD.at[n, zz], rzd.at[i])
        SZ[n, zz] = (f(SZ[n, zz]) + f(RD[n, zz])).astype(BF)
        send_down(n, zz, i)

    @jax.named_scope("red_d")
    def red_d(i):
        zz, _ = unit(i)

        @pl.when((z == 1) & (zz > 1))
        def _():
            relay_up(i)

        @pl.when((z == 2) & (zz < 2))
        def _():
            relay_down(i)

    @jax.named_scope("red_e")
    def red_e(i):
        zz, _ = unit(i)

        @pl.when((z == 2) & (zz > 2))
        def _():
            relay_up(i)

        @pl.when((z == 1) & (zz < 1))
        def _():
            relay_down(i)

    @jax.named_scope("red_f")
    def red_f(l, i):
        zz, n = unit(i)

        def finish(u):
            u = u.astype(BF)

            @pl.when(l == 0)
            def _():
                out = (f(seq_part(xin, n)[...]) + f(u)).astype(BF)
                XO[n] = out
                XA[n, rows(me)] = out
                gather_own(XO.at[n], act, n, NE)

            @pl.when(l == 1)
            def _():
                seq_part(yT, n)[...] = (f(XO[n]) + f(u)).astype(BF)

        @pl.when((z == 0) & (zz == 0))
        def _():
            wait_for(RD.at[n, 0], rzd.at[i])
            finish(f(SZ[n, 0]) + f(RD[n, 0]))

        @pl.when((z == 3) & (zz == 3))
        def _():
            wait_for(RU.at[n, 2], rzu.at[i])
            finish(f(SZ[n, 3]) + f(RU[n, 2]))

        for v in (1, 2):
            @pl.when((z == v) & (zz == v))
            def _():
                wait_for(RU.at[n, v - 1], rzu.at[i])
                wait_for(RD.at[n, v], rzd.at[i])
                finish(f(SZ[n, v]) + f(RU[n, v - 1]) + f(RD[n, v]))

        @pl.when(i >= NU - SCN)
        def _():
            wait_for(SC.at[0], rcs.at[i])

        @pl.when(i >= NU - SYN)
        def _():
            wait_for(SY.at[0], rys.at[i])

        @pl.when(zz != z)
        def _():
            wait_for(SZ.at[n, zz], rsz.at[i])

    shard = me

    def o_forward(l, j):
        zz = unit(NT * j)[0]
        h = lax.rem(z - zz + 4, 4)

        @pl.when(h > 0)
        def _():
            for p in (PA, PB):
                ref = w_ref(l, p, zz, x)
                wait_for(ref, wr.at[l, p, h - 1])
                rcopy(ref, ref, xs.at[l, p], xr.at[l, p, h - 1], xpeer).start()

    def o_arrive(l, j):
        zz = unit(NT * j)[0]
        h = lax.rem(z - zz + 4, 4)

        @pl.when(h > 0)
        def _():
            for p in (PA, PB):
                wait_for(w_ref(l, p, zz, 1 - x), xr.at[l, p, h - 1])

    def o_at(l, place):
        for ll in range(2):
            for at, cond in ((OEND[ll], (z == 0) | (z == 3)), (OMID[ll], (z == 1) | (z == 2))):
                if isinstance(place, int):
                    if place == at:
                        @pl.when((l == ll) & cond)
                        def _():
                            o_send(l)
                elif 0 < at <= NT:
                    @pl.when((l == ll) & cond & (place == at))
                    def _():
                        o_send(l)

    def o_send(l):
        w_send(l, "a", 0, 160)
        w_send(l, "b", 0, 240)

    def layer(l):
        @pl.when(l == 1)
        def _():
            done = RS0
            for e in range(2 * NT):
                gather_hop(act, e % NT, NE, e // NT + 1)
                for v in range(AG1[e]):
                    w_send(1, "g", done)
                    done += 1
                for p in EVENTS[e]:
                    w_forward(1, p)

        for ll, sent in enumerate((sum(S0), RS0 + sum(AG1))):
            @pl.when(l == ll)
            def _():
                rest_send(ll, sent)
        o_at(l, 0)

        def last(n):
            @pl.when(n < NT)
            def _():
                @pl.when((l == 0) & (n == 0))
                def _():
                    gather_hop(ext, 0, 0, len(HOPS))
                gather_hop(act, n, NE, len(HOPS))
                for v in range(NT):
                    if EVENTS[2 * NT + v]:
                        @pl.when((l == 1) & (n == v))
                        def _():
                            for p in EVENTS[2 * NT + v]:
                                w_forward(1, p)

                @pl.when((l == 0) & (n == 0))
                def _():
                    gather_cross(ext, 0, 0)
                gather_cross(act, n, NE)

            @pl.when(n > 0)
            def _():
                chunk(n - 1)

        def chunk(n):
            @pl.when(n == 0)
            def _():
                @pl.when(l == 0)
                def _():
                    unpack()
                    w_forward(0, PQ)
                for cp in w_own(l)[1:]:
                    cp.wait()
            gather_end(act, n, NE)
            norm(l, n)

            @pl.when(n == 0)
            def _():
                w_arrive(l, PQ)
            qkv(l, n)

            late = jnp.where(l == 0, 1, LATE) + n

            @pl.when(late <= GP)
            def _():
                w_forward(l, late)

            @pl.when(lax.rem(n, SPC) == SPC - 1)
            def _():
                attention(n // SPC)
            o_at(l, n + 1)
        loop(NT + 1, last)
        o_at(l, NT + 1)
        for b in range(2):
            off = lan(b * SEQ + LANES * (shard // 2), LANES)
            for v, ref in enumerate((KT, VT)):
                KVT[...] = ref[:, off].astype(F32).T
                kvo[l, v, b] = KVT[sub(64 * lax.rem(shard, 2), 64), :].astype(BF)
        fwd = jnp.where(l == 0, NT, min(GP, LATE - 1 + NT))
        loop(GP - fwd, lambda p: w_forward(l, fwd + 1 + p))
        o_at(l, NT + 2)
        loop(GP, lambda p: w_arrive(l, p + 1))
        o_forward(l, 0)
        gh = jnp.where(l == 0, GH0, GH1)
        loop(gh, lambda n: gate_up(l, n))

        def step(i):
            @pl.when(i < NU)
            def _():
                for j, u in enumerate(OF):
                    @pl.when(i == u)
                    def _():
                        o_forward(l, j + 1)

                @pl.when(lax.rem(i, NT) == 0)
                def _():
                    o_arrive(l, i // NT)

                @pl.when((i >= gh) & (i < NT))
                def _():
                    gate_up(l, i)
                red_a(l, i)
            for lag, stage in zip(LAGS, (red_b, red_c, red_d, red_e, functools.partial(red_f, l))):
                @pl.when((i >= lag) & (i < NU + lag))
                def _():
                    stage(i - lag)

            @pl.when(l == 0)
            def _():
                @pl.when(i == RQ)
                def _():
                    w_send(1, "q", 0, 80)

                @pl.when(i == RQ + 12)
                def _():
                    w_forward(1, PQ)

                for u, each in enumerate(SU):
                    if each:
                        @pl.when(i == u)
                        def _():
                            loop(each, lambda v: w_send(1, "g", sum(SU[:u]) + v))

                for u, ps in enumerate(UNITS):
                    if ps:
                        @pl.when(i == u)
                        def _():
                            for p in ps:
                                w_forward(1, p)
        loop(NU + LAGS[-1], step)

    loop(2, layer)

    for l in range(2):
        for p in range(NPC):
            wait_for(w_size(l, p), ws.at[l, p])
            wait_for(w_size(l, p), xs.at[l, p])


def solution(mesh):
    act_spec = P("dp", None, ("row", "col"))
    weight_spec = P(None, "row", "col")

    def device_fn(x_loc, gain_loc, w_in_loc, w_kv_loc, w_out_loc):
        kv = jnp.transpose(w_kv_loc, (0, 2, 1)).reshape(HD, RW)
        kv = jnp.concatenate([jnp.concatenate([kv[:, v:v + LANES], kv[:, v + LANES:v + 2 * LANES]], axis=0) for v in (0, 2 * LANES)] + [jnp.pad(kv[:, 4 * LANES:], ((0, SH - HD), (0, 0)))], axis=1)
        gain = jnp.pad(gain_loc.T, ((0, 0), (0, LANES - 2)))
        ein = jnp.concatenate([kv, gain], axis=1)
        NPC = GP + 3
        dma = pltpu.SemaphoreType.DMA
        hbm = pl.BlockSpec(memory_space=pl.ANY)
        vmem = pl.BlockSpec(memory_space=pltpu.VMEM)
        y_t, kvo = pl.pallas_call(
            kernel,
            out_shape=(jax.ShapeDtypeStruct((2, SH, SEQ), BF), jax.ShapeDtypeStruct((2, 2, 2, SEQ // 16, HD), BF)),
            in_specs=[vmem, vmem, hbm, hbm, vmem],
            out_specs=(vmem, vmem),
            scratch_shapes=[
                pltpu.VMEM((LANES, HD), F32),
                pltpu.VMEM((2, RW, RW), BF),
                pltpu.VMEM((NT, D, CW), BF),
                pltpu.VMEM((2, 2, D, FB), BF),
                pltpu.VMEM((2, SH, D), BF),
                pltpu.VMEM((2, 192, D), BF),
                pltpu.VMEM((2, SH + FB, D), BF),
                pltpu.VMEM((2, D, 128), BF),
                pltpu.VMEM((NT, SH + FB, CW), BF),
                pltpu.VMEM((SH, T), BF),
                pltpu.VMEM((HD, T), BF),
                pltpu.VMEM((HD, T), BF),
                pltpu.VMEM((NT, SH, CW), BF),
                pltpu.VMEM((NT, 8, SH, CW), BF),
                pltpu.VMEM((NT, 4, SH, CW), BF),
                pltpu.VMEM((NT, 3, SH, CW), BF),
                pltpu.VMEM((NT, 3, SH, CW), BF),
                pltpu.VMEM((SCN, 2, SH, CW), BF),
                pltpu.VMEM((SYN, SH, CW), BF),
                pltpu.VMEM((NT, 4, SH, CW), BF),
                dma((NC,)), dma((NC,)), dma((NC,)), dma((NC,)),
                dma((NC, 2, 3)), dma((NC,)), dma((NC,)),
                dma((4 * NT,)), dma((4 * NT,)), dma((4 * NT,)), dma((4 * NT,)),
                dma((4 * NT,)), dma((4 * NT,)), dma((4 * NT,)),
                dma((2, NPC)), dma((2, NPC, 3)), dma((2, NPC)), dma((2, NPC, 3)),
                dma((2, 6)),
            ],
            compiler_params=pltpu.CompilerParams(collective_id=0, has_side_effects=True, vmem_limit_bytes=67043328),
        )(jnp.transpose(x_loc, (0, 2, 1)), ein, w_in_loc, w_out_loc, rope_tables())
        return jnp.transpose(y_t, (0, 2, 1)), kvo

    return jax.shard_map(device_fn, mesh=mesh, in_specs=(act_spec, P(None, ("row", "col")), weight_spec, weight_spec, P(None, "col", "row")), out_specs=(act_spec, P(None, None, "dp", ("row", "col"), None)), check_vma=False)
```

```python
import functools

import jax
import jax.numpy as jnp
from jax import lax
from jax.experimental import pallas as pl
from jax.experimental.pallas import tpu as pltpu
from jax.sharding import PartitionSpec as P

BF = jnp.bfloat16
F32 = jnp.float32
MESH_ID = pl.DeviceIdType.MESH
LN_EPS = 1e-6

D = 2560
SH = 160
RW = 640
FB = 640
HD = 80
HALF = HD // 2
SEQ = 1024
T = 2 * SEQ
CW = 512
NT = T // CW
NE = 512 // CW
NC = NE + NT
SPC = SEQ // CW
GP = 8
GR = RW // GP
LANES = 128
EW = 3 * LANES
HOPS = (1, 2, 3)
QB = 256
SCN, SYN = 4, 6
MR = 16
LAGS = (1, 4, 7, 12, 15)
PM = GR // MR
S0 = (1,) * 8
GH0, GH1 = 1, 3
OEND = (4, 0)
OMID = (5, 5)
OF = (0, 4, 8)
RQ = 0
SU = (0,) + (2,) * 10
AG1 = (0,) * 8
UFW, EFW = 30, 12


def weight_plan():
    sent, when = 0, []
    for i, each in enumerate(SU):
        when += [i] * each
        sent += each
    units = [[] for _ in range(4 * NT + LAGS[-1])]
    events = [[] for _ in range(3 * NT)]
    late = list(range(1, GP + 1))
    ev = []
    for e in range(2 * NT):
        ev += [e] * AG1[e]
    for p in range(1, GP + 1):
        last = PM * p - 1
        if last < sent:
            if when[last] + UFW < len(units):
                units[when[last] + UFW].append(p)
                late.remove(p)
                continue
            e = max(0, when[last] + UFW - len(units))
        elif last < sent + len(ev):
            e = ev[last - sent] + EFW
        else:
            continue
        if e < 3 * NT:
            events[e].append(p)
            late.remove(p)
    return sent, units, events, late[0] if late else GP + 1


RS0, UNITS, EVENTS, LATE = weight_plan()


def rope_tables():
    inv_freq = 1.0 / (10000.0 ** (jnp.arange(HALF, dtype=F32) * 2.0 / HD))
    angles = inv_freq[:, None] * jnp.arange(SEQ).astype(F32)[None, :]
    return jnp.cos(angles), jnp.sin(angles)


def sub(start, size):
    return pl.ds(pl.multiple_of(start, 16), size)


def lan(start, size):
    return pl.ds(pl.multiple_of(start, LANES), size)


def dot_ta(a, b):
    return lax.dot_general(a, b, (((0,), (0,)), ((), ())), preferred_element_type=F32)


def kernel(xin, kvw, gn, w_in, w_out, cos, sin, yT, kvo, EIN, KVT, WT, XA, GU, WQ, WKV, WO, GB, MT, QT, KT, VT, XO, RC, RY, RU, RD, SC, SY, SZ,
           zsu, zsd, ysn, csn, zrc, yrc, crc, rcs, rcr, rys, ryr, rzu, rzd, rsz, ws, wr, xs, xr, own):
    x = lax.axis_index("dp")
    z = lax.axis_index("row")
    c = lax.axis_index("col")
    y, k = c // 2, lax.rem(c, 2)
    me = 4 * z + c
    up = (x, jnp.minimum(z + 1, 3), c)
    down = (x, jnp.maximum(z - 1, 0), c)
    ypeer = (x, z, lax.rem(c + 2, 4))
    cpeer = (x, z, c + 1 - 2 * k)
    xpeer = (1 - x, z, c)
    zpeer = [(x, lax.rem(z + h, 4), c) for h in HOPS]

    def rcopy(src, dst, ss, rs, dev):
        return pltpu.make_async_remote_copy(src_ref=src, dst_ref=dst, send_sem=ss, recv_sem=rs, device_id=dev, device_id_type=MESH_ID)

    def wait_for(ref, sem):
        pltpu.make_async_copy(ref, ref, sem).wait()

    def rows(s):
        return sub(s * SH, SH)

    def loop(n, body):
        def step(i, carry):
            body(i)
            return carry
        lax.fori_loop(0, n, step, 0)

    barrier = pltpu.get_barrier_semaphore()
    for dev in zpeer + [ypeer, cpeer, xpeer]:
        pl.semaphore_signal(barrier, inc=1, device_id=dev, device_id_type=MESH_ID)
    pl.semaphore_wait(barrier, 6)

    def act(ch, s):
        return XA.at[ch, rows(s)]

    def ext(ch, s):
        i = 16 * ch + s
        return MT.at[i // 5, rows(lax.rem(i, 5)), pl.ds(0, EW)]

    @jax.named_scope("gather_own")
    def size(o, shards):
        return XA.at[0, pl.ds(0, shards * SH), pl.ds(0, CW if o else EW)]

    @jax.named_scope("gather_own")
    def gather_own(src, buf, ch, o):
        q = ch + o
        dst = buf(ch, me)

        @pl.when(z < 3)
        def _():
            rcopy(src, dst, zsu.at[q], zrc.at[q, 0, 0], up).start()

        @pl.when(z > 0)
        def _():
            rcopy(src, dst, zsd.at[q], zrc.at[q, 1, 0], down).start()

        rcopy(src, dst, ysn.at[q], yrc.at[q], ypeer).start()
        rcopy(src, dst, csn.at[q], crc.at[q], cpeer).start()

    @jax.named_scope("gather_hop")
    def gather_hop(buf, ch, o, hop):
        q = ch + o

        @pl.when(z - hop >= 0)
        def _():
            ref = buf(ch, jnp.maximum(me - 4 * hop, 0))
            wait_for(ref, zrc.at[q, 0, hop - 1])
            if hop < 3:
                @pl.when(z < 3)
                def _():
                    rcopy(ref, ref, zsu.at[q], zrc.at[q, 0, hop], up).start()
            rcopy(ref, ref, ysn.at[q], yrc.at[q], ypeer).start()
            rcopy(ref, ref, csn.at[q], crc.at[q], cpeer).start()

        @pl.when(z + hop <= 3)
        def _():
            ref = buf(ch, jnp.minimum(me + 4 * hop, 15))
            wait_for(ref, zrc.at[q, 1, hop - 1])
            if hop < 3:
                @pl.when(z > 0)
                def _():
                    rcopy(ref, ref, zsd.at[q], zrc.at[q, 1, hop], down).start()
            rcopy(ref, ref, ysn.at[q], yrc.at[q], ypeer).start()
            rcopy(ref, ref, csn.at[q], crc.at[q], cpeer).start()

    @jax.named_scope("gather_cross")
    def gather_cross(buf, ch, o):
        q = ch + o
        wait_for(size(o, 4), yrc.at[q])
        for zz in range(4):
            ref = buf(ch, 4 * zz + lax.rem(c + 2, 4))
            rcopy(ref, ref, csn.at[q], crc.at[q], cpeer).start()

    @jax.named_scope("gather_end")
    def gather_end(buf, ch, o):
        q = ch + o
        wait_for(size(o, 8), crc.at[q])
        for zz in range(3):
            @pl.when(z == zz)
            def _():
                wait_for(size(o, zz + 1), zsu.at[q])

            @pl.when(z == 3 - zz)
            def _():
                wait_for(size(o, zz + 1), zsd.at[q])
        wait_for(size(o, 4), ysn.at[q])
        wait_for(size(o, 8), csn.at[q])

    NPC = GP + 3

    def lane(zz):
        return lan(zz * RW, RW)

    PQ, PA, PB = 0, GP + 1, GP + 2

    def kind(p):
        return p if isinstance(p, int) and (p == PQ or p > GP) else 1

    def w_ref(l, p, zz, half):
        if kind(p) == PQ:
            return WQ.at[l, sub(80 * half, 80), lane(zz)]
        if kind(p) == PA:
            return WO.at[l, sub(400 * half, 160), lane(zz)]
        if kind(p) == PB:
            return WO.at[l, sub(160 + 400 * half, 240), lane(zz)]
        return GU.at[l, half, sub(zz * RW + GR * (p - 1), GR), :]

    def w_send(l, kind_, m, mr=MR):
        r = mr * m
        for h in HOPS:
            t = lax.rem(z + h, 4)
            if kind_ == "q":
                p, src = PQ, WT.at[l, sub(SH * t + 80 * x + r, mr), :]
                dst = WQ.at[l, sub(80 * x + r, mr), lane(z)]
            elif kind_ == "g":
                p, src = 1 + r // GR, w_in.at[l, sub(r, mr), lan(RW + D * x + FB * t, FB)]
                dst = GU.at[l, x, sub(z * RW + r, mr), :]
            elif kind_ == "a":
                p, src = PA, w_out.at[l, sub(jnp.where(x == 0, SH * t, RW + FB * t + 240) + r, mr), :]
                dst = WO.at[l, sub(400 * x + r, mr), lane(z)]
            else:
                p, src = PB, w_out.at[l, sub(RW + FB * t + 400 * x + r, mr), :]
                dst = WO.at[l, sub(160 + 400 * x + r, mr), lane(z)]
            rcopy(src, dst, ws.at[l, p], wr.at[l, p, h - 1], zpeer[h - 1]).start()

    def rest_send(l, m):
        whole = -(-m // PM)
        for v in range(m, whole * PM):
            w_send(l, "g", v)
        for v in range(whole, GP):
            w_send(l, "g", v, GR)

    NQ, NG, NA, NB = 80 // MR, RW // MR, 160 // MR, 240 // MR

    @jax.named_scope("w_forward")
    def w_forward(l, p):
        for h in HOPS:
            ref = w_ref(l, p, lax.rem(z - h + 4, 4), x)
            wait_for(ref, wr.at[l, p, h - 1])
            rcopy(ref, ref, xs.at[l, p], xr.at[l, p, h - 1], xpeer).start()

    def w_size(l, p):
        if kind(p) == PQ:
            return WQ.at[l, pl.ds(0, 80), pl.ds(0, 3 * RW)]
        if kind(p) == PA:
            return WO.at[l, pl.ds(0, 160), pl.ds(0, 3 * RW)]
        if kind(p) == PB:
            return WO.at[l, pl.ds(0, 240), pl.ds(0, 3 * RW)]
        return GU.at[l, 0, pl.ds(0, 3 * GR), :]

    @jax.named_scope("w_arrive")
    def w_arrive(l, p):
        for h in HOPS:
            wait_for(w_ref(l, p, 0, 0), xr.at[l, p, h - 1])

    def w_own(l):
        return [
            None,
            pltpu.make_async_copy(w_in.at[l, :, lan(RW + FB * z, FB)], GU.at[l, 0, sub(z * RW, RW), :], own.at[l, 1]),
            pltpu.make_async_copy(w_in.at[l, :, lan(RW + D + FB * z, FB)], GU.at[l, 1, sub(z * RW, RW), :], own.at[l, 2]),
            pltpu.make_async_copy(w_out.at[l, sub(SH * z, SH), :], WO.at[l, pl.ds(0, SH), lane(z)], own.at[l, 3]),
            pltpu.make_async_copy(w_out.at[l, sub(RW + FB * z, FB), :], WO.at[l, pl.ds(SH, FB), lane(z)], own.at[l, 4]),
        ]

    def seq_part(ref, n):
        return ref.at[n // SPC, :, lan(lax.rem(n, SPC) * CW, CW)]

    q_in = [pltpu.make_async_copy(w_in.at[l, :, pl.ds(0, RW)], GU.at[1, l, sub(z * RW, RW), :], own.at[l, 5]) for l in range(2)]
    for cp in q_in:
        cp.start()
    for b in range(5):
        blk = jnp.concatenate([kvw[l, :, LANES * b:LANES * (b + 1)].astype(F32) for l in range(2)], axis=0)
        EIN[HD * (b % 2):HD * (b % 2) + HD, LANES * (b // 2):LANES * (b // 2 + 1)] = blk.astype(BF)
    EIN[HD:, 2 * LANES:] = gn[...]
    ext(0, me)[...] = EIN[...]

    def put_own(ch):
        XA[ch, rows(me)] = seq_part(xin, ch)[...]
    loop(NT, put_own)
    gather_own(EIN, ext, 0, 0)
    for ch in range(NT):
        gather_own(seq_part(xin, ch), act, ch, NE)
    for cp in w_own(0)[1:]:
        cp.start()
    for l in range(2):
        q_in[l].wait()
        WT[l] = GU[1, l, sub(z * RW, RW), :].T
        WQ[l, :, lane(z)] = WT[l, sub(SH * z, SH), :]
    w_send(0, "q", 0, 80)
    for cp in w_own(1)[1:]:
        cp.start()
    done = 0
    for e in range(2 * NT):
        if e % NT == 0:
            gather_hop(ext, 0, 0, e // NT + 1)
        gather_hop(act, e % NT, NE, e // NT + 1)
        for v in range(S0[e]):
            w_send(0, "g", done)
            done += 1

    @jax.named_scope("unpack")
    def unpack():
        loop(NE, lambda ch: gather_end(ext, ch, 0))

        def shard(s):
            zz, cc = s // 4, lax.rem(s, 4)
            for b in range(5):
                lo = 128 * (b // 2)
                i = 16 * (lo // CW) + s
                blk = MT[i // 5, sub(lax.rem(i, 5) * SH + 80 * (b % 2), 80), lo % CW:lo % CW + 128].astype(F32)
                for l in range(2):
                    WKV[l, sub(48 * cc, 40), lan(zz * RW + 128 * b, 128)] = blk[40 * l:40 * l + 40].astype(BF)
            blk = MT[s // 5, sub(lax.rem(s, 5) * SH + HD, HD), 2 * LANES:EW].astype(F32)
            for l in range(2):
                for v in range(2):
                    GB[l, sub(s * SH + HD * v, HD), :] = jnp.broadcast_to(blk[:, l + 2 * v:l + 2 * v + 1], (HD, LANES)).astype(BF)
        loop(16, shard)
        for l in range(2):
            for cc in range(4):
                WKV[l, 48 * cc + 40:48 * cc + 48, :] = jnp.zeros((8, D), BF)

    BR = 32

    @jax.named_scope("norm")
    def norm(l, n):
        def fold(v):
            return v.reshape(BR // 8, 8, CW).sum(0)

        def load(i):
            return XA[n, sub(i * BR, BR), :].astype(F32)

        tot = lax.fori_loop(0, D // BR, lambda i, a: a + fold(load(i)), jnp.zeros((8, CW), F32), unroll=4)
        mean = jnp.sum(tot, axis=0, keepdims=True) / D

        def square(i, a):
            d = load(i) - mean
            return a + fold(d * d)
        var = jnp.sum(lax.fori_loop(0, D // BR, square, jnp.zeros((8, CW), F32), unroll=4), axis=0, keepdims=True) / D
        scale = lax.rsqrt(var + LN_EPS)

        def put(i, a):
            g = jnp.concatenate([GB[l, sub(i * BR, BR), :].astype(F32)] * (CW // 128), axis=1)
            XA[n, sub(i * BR, BR), :] = ((load(i) - mean) * scale * g).astype(BF)
            return a
        lax.fori_loop(0, D // BR, put, 0, unroll=4)

    def tok(n):
        return lan(n * CW, CW)

    @jax.named_scope("qkv")
    def qkv(l, n):
        pos = lan(lax.rem(n * CW, SEQ), CW)
        co, si = cos[:, pos], sin[:, pos]
        h = XA[n]
        kv = jnp.dot(WKV[l], h, preferred_element_type=F32).astype(BF).astype(F32)

        def rot(lo, hi):
            return jnp.concatenate([lo * co - hi * si, hi * co + lo * si], axis=0)
        KT[:, tok(n)] = rot(kv[0:40], kv[48:88]).astype(BF)
        VT[:, tok(n)] = jnp.concatenate([kv[96:136], kv[144:184]], axis=0).astype(BF)
        qq = jnp.dot(WQ[l], h, preferred_element_type=F32).astype(BF).astype(F32)
        for hd in range(2):
            QT[HD * hd:HD * hd + HD, tok(n)] = (rot(qq[HD * hd:HD * hd + HALF], qq[HD * hd + HALF:HD * hd + HD]) * HD ** -0.5).astype(BF)

    @jax.named_scope("attention")
    def attention(b):
        def body(hd):
            hr = sub(hd * HD, HD)
            for i in range(SEQ // QB):
                nk = QB * (i + 1)
                ks = lan(b * SEQ, nk)
                qs = lan(b * SEQ + QB * i, QB)
                s = dot_ta(KT[:, ks], QT[hr, qs])
                keep = lax.broadcasted_iota(jnp.int32, (QB, QB), 0) <= lax.broadcasted_iota(jnp.int32, (QB, QB), 1)
                last = jnp.where(keep, s[nk - QB:], -1e30)
                s = jnp.concatenate([s[:nk - QB], last], axis=0) if i else last
                e = jnp.exp(s - jnp.max(s, axis=0, keepdims=True))
                pr = (e * (1.0 / jnp.sum(e, axis=0, keepdims=True))).astype(BF)
                MT[b * (SEQ // CW) + QB * i // CW, hr, QB * i % CW:QB * i % CW + QB] = jnp.dot(VT[:, ks], pr, preferred_element_type=F32).astype(BF)
        loop(2, body)

    @jax.named_scope("gate_up")
    def gate_up(l, n):
        h = XA[n]
        g = dot_ta(GU[l, 0], h).astype(BF).astype(F32)
        u = dot_ta(GU[l, 1], h).astype(BF).astype(F32)
        MT[n, SH:SH + FB, :] = (g * lax.logistic(g) * u).astype(BF)

    def f(ref_value):
        return ref_value.astype(F32)

    NU = 4 * NT

    def unit(i):
        j = i // NT
        return jnp.where(j == 0, 3, jnp.where(j == 1, 0, jnp.where(j == 2, 2, 1))), lax.rem(i, NT)

    @jax.named_scope("red_a")
    def red_a(l, i):
        zz, n = unit(i)
        slot = lax.rem(i, SCN)

        @pl.when(i >= SCN)
        def _():
            wait_for(SC.at[slot], rcs.at[i - SCN])

        XA[n, sub(zz * RW, RW), :] = dot_ta(WO[l, :, lane(zz)], MT[n]).astype(BF)
        for yy in range(2):
            SC[slot, yy] = XA[n, rows(4 * zz + 2 * yy + 1 - k)]
        for yy in range(2):
            rcopy(SC.at[slot, yy], RC.at[n, 2 * zz + yy], rcs.at[i], rcr.at[i], cpeer).start()

    @jax.named_scope("red_b")
    def red_b(i):
        zz, n = unit(i)
        slot = lax.rem(i, SYN)
        wait_for(RC.at[n, pl.ds(2 * zz, 2)], rcr.at[i])

        @pl.when(i >= SYN)
        def _():
            wait_for(SY.at[slot], rys.at[i - SYN])

        SY[slot] = (f(XA[n, rows(4 * zz + 2 * (1 - y) + k)]) + f(RC[n, 2 * zz + 1 - y])).astype(BF)
        rcopy(SY.at[slot], RY.at[n, zz], rys.at[i], ryr.at[i], ypeer).start()

    def send_up(n, zz, i):
        rcopy(SZ.at[n, zz], RU.at[n, zz - 1], rsz.at[i], rzu.at[i], up).start()

    def send_down(n, zz, i):
        rcopy(SZ.at[n, zz], RD.at[n, zz], rsz.at[i], rzd.at[i], down).start()

    @jax.named_scope("red_c")
    def red_c(i):
        zz, n = unit(i)
        wait_for(RY.at[n, zz], ryr.at[i])
        SZ[n, zz] = (f(XA[n, rows(4 * zz + c)]) + f(RC[n, 2 * zz + y]) + f(RY[n, zz])).astype(BF)

        @pl.when((z == 0) & (zz > 0))
        def _():
            send_up(n, zz, i)

        @pl.when((z == 3) & (zz < 3))
        def _():
            send_down(n, zz, i)

    def relay_up(i):
        zz, n = unit(i)
        wait_for(RU.at[n, zz - 1], rzu.at[i])
        SZ[n, zz] = (f(SZ[n, zz]) + f(RU[n, zz - 1])).astype(BF)
        send_up(n, zz, i)

    def relay_down(i):
        zz, n = unit(i)
        wait_for(RD.at[n, zz], rzd.at[i])
        SZ[n, zz] = (f(SZ[n, zz]) + f(RD[n, zz])).astype(BF)
        send_down(n, zz, i)

    @jax.named_scope("red_d")
    def red_d(i):
        zz, _ = unit(i)

        @pl.when((z == 1) & (zz > 1))
        def _():
            relay_up(i)

        @pl.when((z == 2) & (zz < 2))
        def _():
            relay_down(i)

    @jax.named_scope("red_e")
    def red_e(i):
        zz, _ = unit(i)

        @pl.when((z == 2) & (zz > 2))
        def _():
            relay_up(i)

        @pl.when((z == 1) & (zz < 1))
        def _():
            relay_down(i)

    @jax.named_scope("red_f")
    def red_f(l, i):
        zz, n = unit(i)

        def finish(u):
            u = u.astype(BF)

            @pl.when(l == 0)
            def _():
                out = (f(seq_part(xin, n)[...]) + f(u)).astype(BF)
                XO[n] = out
                XA[n, rows(me)] = out
                gather_own(XO.at[n], act, n, NE)

            @pl.when(l == 1)
            def _():
                seq_part(yT, n)[...] = (f(XO[n]) + f(u)).astype(BF)

        @pl.when((z == 0) & (zz == 0))
        def _():
            wait_for(RD.at[n, 0], rzd.at[i])
            finish(f(SZ[n, 0]) + f(RD[n, 0]))

        @pl.when((z == 3) & (zz == 3))
        def _():
            wait_for(RU.at[n, 2], rzu.at[i])
            finish(f(SZ[n, 3]) + f(RU[n, 2]))

        for v in (1, 2):
            @pl.when((z == v) & (zz == v))
            def _():
                wait_for(RU.at[n, v - 1], rzu.at[i])
                wait_for(RD.at[n, v], rzd.at[i])
                finish(f(SZ[n, v]) + f(RU[n, v - 1]) + f(RD[n, v]))

        @pl.when(i >= NU - SCN)
        def _():
            wait_for(SC.at[0], rcs.at[i])

        @pl.when(i >= NU - SYN)
        def _():
            wait_for(SY.at[0], rys.at[i])

        @pl.when(zz != z)
        def _():
            wait_for(SZ.at[n, zz], rsz.at[i])

    shard = me

    def o_forward(l, j):
        zz = unit(NT * j)[0]
        h = lax.rem(z - zz + 4, 4)

        @pl.when(h > 0)
        def _():
            for p in (PA, PB):
                ref = w_ref(l, p, zz, x)
                wait_for(ref, wr.at[l, p, h - 1])
                rcopy(ref, ref, xs.at[l, p], xr.at[l, p, h - 1], xpeer).start()

    def o_arrive(l, j):
        zz = unit(NT * j)[0]
        h = lax.rem(z - zz + 4, 4)

        @pl.when(h > 0)
        def _():
            for p in (PA, PB):
                wait_for(w_ref(l, p, zz, 1 - x), xr.at[l, p, h - 1])

    def o_at(l, place):
        for ll in range(2):
            for at, cond in ((OEND[ll], (z == 0) | (z == 3)), (OMID[ll], (z == 1) | (z == 2))):
                if isinstance(place, int):
                    if place == at:
                        @pl.when((l == ll) & cond)
                        def _():
                            o_send(l)
                elif 0 < at <= NT:
                    @pl.when((l == ll) & cond & (place == at))
                    def _():
                        o_send(l)

    def o_send(l):
        w_send(l, "a", 0, 160)
        w_send(l, "b", 0, 240)

    def layer(l):
        @pl.when(l == 1)
        def _():
            done = RS0
            for e in range(2 * NT):
                gather_hop(act, e % NT, NE, e // NT + 1)
                for v in range(AG1[e]):
                    w_send(1, "g", done)
                    done += 1
                for p in EVENTS[e]:
                    w_forward(1, p)

        for ll, sent in enumerate((sum(S0), RS0 + sum(AG1))):
            @pl.when(l == ll)
            def _():
                rest_send(ll, sent)
        o_at(l, 0)

        def last(n):
            @pl.when(n < NT)
            def _():
                @pl.when((l == 0) & (n == 0))
                def _():
                    gather_hop(ext, 0, 0, len(HOPS))
                gather_hop(act, n, NE, len(HOPS))
                for v in range(NT):
                    if EVENTS[2 * NT + v]:
                        @pl.when((l == 1) & (n == v))
                        def _():
                            for p in EVENTS[2 * NT + v]:
                                w_forward(1, p)

                @pl.when((l == 0) & (n == 0))
                def _():
                    gather_cross(ext, 0, 0)
                gather_cross(act, n, NE)

            @pl.when(n > 0)
            def _():
                chunk(n - 1)

        def chunk(n):
            @pl.when(n == 0)
            def _():
                @pl.when(l == 0)
                def _():
                    unpack()
                    w_forward(0, PQ)
                for cp in w_own(l)[1:]:
                    cp.wait()
            gather_end(act, n, NE)
            norm(l, n)

            @pl.when(n == 0)
            def _():
                w_arrive(l, PQ)
            qkv(l, n)

            late = jnp.where(l == 0, 1, LATE) + n

            @pl.when(late <= GP)
            def _():
                w_forward(l, late)

            @pl.when(lax.rem(n, SPC) == SPC - 1)
            def _():
                attention(n // SPC)
            o_at(l, n + 1)
        loop(NT + 1, last)
        o_at(l, NT + 1)
        for b in range(2):
            off = lan(b * SEQ + LANES * (shard // 2), LANES)
            for v, ref in enumerate((KT, VT)):
                KVT[...] = ref[:, off].astype(F32).T
                kvo[l, v, b] = KVT[sub(64 * lax.rem(shard, 2), 64), :].astype(BF)
        fwd = jnp.where(l == 0, NT, min(GP, LATE - 1 + NT))
        loop(GP - fwd, lambda p: w_forward(l, fwd + 1 + p))
        o_at(l, NT + 2)
        loop(GP, lambda p: w_arrive(l, p + 1))
        o_forward(l, 0)
        gh = jnp.where(l == 0, GH0, GH1)
        loop(gh, lambda n: gate_up(l, n))

        def step(i):
            @pl.when(i < NU)
            def _():
                for j, u in enumerate(OF):
                    @pl.when(i == u)
                    def _():
                        o_forward(l, j + 1)

                @pl.when(lax.rem(i, NT) == 0)
                def _():
                    o_arrive(l, i // NT)

                @pl.when((i >= gh) & (i < NT))
                def _():
                    gate_up(l, i)
                red_a(l, i)
            for lag, stage in zip(LAGS, (red_b, red_c, red_d, red_e, functools.partial(red_f, l))):
                @pl.when((i >= lag) & (i < NU + lag))
                def _():
                    stage(i - lag)

            @pl.when(l == 0)
            def _():
                @pl.when(i == RQ)
                def _():
                    w_send(1, "q", 0, 80)

                @pl.when(i == RQ + 12)
                def _():
                    w_forward(1, PQ)

                for u, each in enumerate(SU):
                    if each:
                        @pl.when(i == u)
                        def _():
                            loop(each, lambda v: w_send(1, "g", sum(SU[:u]) + v))

                for u, ps in enumerate(UNITS):
                    if ps:
                        @pl.when(i == u)
                        def _():
                            for p in ps:
                                w_forward(1, p)
        loop(NU + LAGS[-1], step)

    loop(2, layer)

    for l in range(2):
        for p in range(NPC):
            wait_for(w_size(l, p), ws.at[l, p])
            wait_for(w_size(l, p), xs.at[l, p])


def solution(mesh):
    act_spec = P("dp", None, ("row", "col"))
    weight_spec = P(None, "row", "col")

    def device_fn(x_loc, gain_loc, w_in_loc, w_kv_loc, w_out_loc):
        gain = jnp.pad(jnp.transpose(gain_loc.reshape(2, 2, HD), (2, 1, 0)).reshape(HD, 4), ((0, 0), (0, LANES - 4)))
        NPC = GP + 3
        dma = pltpu.SemaphoreType.DMA
        hbm = pl.BlockSpec(memory_space=pl.ANY)
        vmem = pl.BlockSpec(memory_space=pltpu.VMEM)
        y_t, kvo = pl.pallas_call(
            kernel,
            out_shape=(jax.ShapeDtypeStruct((2, SH, SEQ), BF), jax.ShapeDtypeStruct((2, 2, 2, SEQ // 16, HD), BF)),
            in_specs=[vmem, vmem, vmem, hbm, hbm, vmem, vmem],
            out_specs=(vmem, vmem),
            scratch_shapes=[
                pltpu.VMEM((SH, EW), BF),
                pltpu.VMEM((LANES, HD), F32),
                pltpu.VMEM((2, RW, RW), BF),
                pltpu.VMEM((NT, D, CW), BF),
                pltpu.VMEM((2, 2, D, FB), BF),
                pltpu.VMEM((2, SH, D), BF),
                pltpu.VMEM((2, 192, D), BF),
                pltpu.VMEM((2, SH + FB, D), BF),
                pltpu.VMEM((2, D, 128), BF),
                pltpu.VMEM((NT, SH + FB, CW), BF),
                pltpu.VMEM((SH, T), BF),
                pltpu.VMEM((HD, T), BF),
                pltpu.VMEM((HD, T), BF),
                pltpu.VMEM((NT, SH, CW), BF),
                pltpu.VMEM((NT, 8, SH, CW), BF),
                pltpu.VMEM((NT, 4, SH, CW), BF),
                pltpu.VMEM((NT, 3, SH, CW), BF),
                pltpu.VMEM((NT, 3, SH, CW), BF),
                pltpu.VMEM((SCN, 2, SH, CW), BF),
                pltpu.VMEM((SYN, SH, CW), BF),
                pltpu.VMEM((NT, 4, SH, CW), BF),
                dma((NC,)), dma((NC,)), dma((NC,)), dma((NC,)),
                dma((NC, 2, 3)), dma((NC,)), dma((NC,)),
                dma((4 * NT,)), dma((4 * NT,)), dma((4 * NT,)), dma((4 * NT,)),
                dma((4 * NT,)), dma((4 * NT,)), dma((4 * NT,)),
                dma((2, NPC)), dma((2, NPC, 3)), dma((2, NPC)), dma((2, NPC, 3)),
                dma((2, 6)),
            ],
            compiler_params=pltpu.CompilerParams(collective_id=0, has_side_effects=True, vmem_limit_bytes=67043328),
        )(jnp.transpose(x_loc, (0, 2, 1)), jnp.transpose(w_kv_loc, (0, 2, 1)), gain, w_in_loc, w_out_loc, *rope_tables())
        return jnp.transpose(y_t, (0, 2, 1)), kvo

    return jax.shard_map(device_fn, mesh=mesh, in_specs=(act_spec, P(None, ("row", "col")), weight_spec, weight_spec, P(None, "col", "row")), out_specs=(act_spec, P(None, None, "dp", ("row", "col"), None)), check_vma=False)
```

```python
import jax
import jax.numpy as jnp
from jax import lax
from jax.experimental import pallas as pl
from jax.experimental.pallas import tpu as pltpu
from jax.sharding import PartitionSpec as P

BF = jnp.bfloat16
F32 = jnp.float32
MESH_ID = pl.DeviceIdType.MESH
LN_EPS = 1e-6

D = 2560
SH = 160
RW = 640
FB = 640
HD = 80
HALF = HD // 2
SEQ = 1024
T = 2 * SEQ
CW = 512
NT = T // CW
NE = 512 // CW
NC = NE + NT
SPC = SEQ // CW
GP = 8
GR = RW // GP
LANES = 128
EW = 3 * LANES
HOPS = (1, 2, 3)
QB = 256
SCN, SYN = 4, 6
MR = 16
LAGS = (1, 6, 12, 4, 18)
PM = GR // MR
S0 = (0,) * 4 + (2,) * 4
GH0, GH1 = 1, 3
OEND = (4, 0)
OMID = (5, 5)
OF = (0, 4, 8)
RQ = 0
SU = (0,) + (2,) * 10
AG1 = (0,) * len(S0)
UFW, EFW = 30, 12


def weight_plan():
    sent, when = 0, []
    for i, each in enumerate(SU):
        when += [i] * each
        sent += each
    units = [[] for _ in range(4 * NT + LAGS[-1])]
    events = [[] for _ in range(3 * NT)]
    late = list(range(1, GP + 1))
    ev = []
    for e in range(2 * NT):
        ev += [e] * AG1[e]
    for p in range(1, GP + 1):
        last = PM * p - 1
        if last < sent:
            if when[last] + UFW < len(units):
                units[when[last] + UFW].append(p)
                late.remove(p)
                continue
            e = max(0, when[last] + UFW - len(units))
        elif last < sent + len(ev):
            e = ev[last - sent] + EFW
        else:
            continue
        if e < 3 * NT:
            events[e].append(p)
            late.remove(p)
    return sent, units, events, late[0] if late else GP + 1


RS0, UNITS, EVENTS, LATE = weight_plan()


def rope_tables():
    inv_freq = 1.0 / (10000.0 ** (jnp.arange(HALF, dtype=F32) * 2.0 / HD))
    angles = inv_freq[:, None] * jnp.arange(SEQ).astype(F32)[None, :]
    return jnp.cos(angles), jnp.sin(angles)


def sub(start, size):
    return pl.ds(pl.multiple_of(start, 16), size)


def lan(start, size):
    return pl.ds(pl.multiple_of(start, LANES), size)


def dot_ta(a, b):
    return lax.dot_general(a, b, (((0,), (0,)), ((), ())), preferred_element_type=F32)


def kernel(xin, kvw, gn, w_in, w_out, cos, sin, yT, kvo, EIN, KVT, WT, XA, GU, WQ, WKV, WO, GB, MT, QT, KT, VT, XO, RC, RY, RU, RD, SC, SY, SZ,
           zsu, zsd, ysn, csn, zrc, yrc, crc, rcs, rcr, rys, ryr, rzu, rzd, rsz, ws, wr, xs, xr, own):
    x = lax.axis_index("dp")
    z = lax.axis_index("row")
    c = lax.axis_index("col")
    y, k = c // 2, lax.rem(c, 2)
    me = 4 * z + c
    up = (x, jnp.minimum(z + 1, 3), c)
    down = (x, jnp.maximum(z - 1, 0), c)
    ypeer = (x, z, lax.rem(c + 2, 4))
    cpeer = (x, z, c + 1 - 2 * k)
    xpeer = (1 - x, z, c)
    zpeer = [(x, lax.rem(z + h, 4), c) for h in HOPS]

    def rcopy(src, dst, ss, rs, dev):
        return pltpu.make_async_remote_copy(src_ref=src, dst_ref=dst, send_sem=ss, recv_sem=rs, device_id=dev, device_id_type=MESH_ID)

    def wait_for(ref, sem):
        pltpu.make_async_copy(ref, ref, sem).wait()

    def rows(s):
        return sub(s * SH, SH)

    def loop(n, body):
        def step(i, carry):
            body(i)
            return carry
        lax.fori_loop(0, n, step, 0)

    barrier = pltpu.get_barrier_semaphore()
    for dev in zpeer + [ypeer, cpeer, xpeer]:
        pl.semaphore_signal(barrier, inc=1, device_id=dev, device_id_type=MESH_ID)
    pl.semaphore_wait(barrier, 6)

    def act(ch, s):
        return XA.at[ch, rows(s)]

    def ext(ch, s):
        i = 16 * ch + s
        return MT.at[i // 5, rows(lax.rem(i, 5)), pl.ds(0, EW)]

    @jax.named_scope("gather_own")
    def size(o, shards):
        return XA.at[0, pl.ds(0, shards * SH), pl.ds(0, CW if o else EW)]

    @jax.named_scope("gather_own")
    def gather_own(src, buf, ch, o):
        q = ch + o
        dst = buf(ch, me)

        @pl.when(z < 3)
        def _():
            rcopy(src, dst, zsu.at[q], zrc.at[q, 0, 0], up).start()

        @pl.when(z > 0)
        def _():
            rcopy(src, dst, zsd.at[q], zrc.at[q, 1, 0], down).start()

        rcopy(src, dst, ysn.at[q], yrc.at[q], ypeer).start()
        rcopy(src, dst, csn.at[q], crc.at[q], cpeer).start()

    @jax.named_scope("gather_hop")
    def gather_hop(buf, ch, o, hop):
        q = ch + o

        @pl.when(z - hop >= 0)
        def _():
            ref = buf(ch, jnp.maximum(me - 4 * hop, 0))
            wait_for(ref, zrc.at[q, 0, hop - 1])
            if hop < 3:
                @pl.when(z < 3)
                def _():
                    rcopy(ref, ref, zsu.at[q], zrc.at[q, 0, hop], up).start()
            rcopy(ref, ref, ysn.at[q], yrc.at[q], ypeer).start()
            rcopy(ref, ref, csn.at[q], crc.at[q], cpeer).start()

        @pl.when(z + hop <= 3)
        def _():
            ref = buf(ch, jnp.minimum(me + 4 * hop, 15))
            wait_for(ref, zrc.at[q, 1, hop - 1])
            if hop < 3:
                @pl.when(z > 0)
                def _():
                    rcopy(ref, ref, zsd.at[q], zrc.at[q, 1, hop], down).start()
            rcopy(ref, ref, ysn.at[q], yrc.at[q], ypeer).start()
            rcopy(ref, ref, csn.at[q], crc.at[q], cpeer).start()

    @jax.named_scope("gather_cross")
    def gather_cross(buf, ch, o):
        q = ch + o
        wait_for(size(o, 4), yrc.at[q])
        for zz in range(4):
            ref = buf(ch, 4 * zz + lax.rem(c + 2, 4))
            rcopy(ref, ref, csn.at[q], crc.at[q], cpeer).start()

    @jax.named_scope("gather_end")
    def gather_end(buf, ch, o):
        q = ch + o
        wait_for(size(o, 8), crc.at[q])
        for zz in range(3):
            @pl.when(z == zz)
            def _():
                wait_for(size(o, zz + 1), zsu.at[q])

            @pl.when(z == 3 - zz)
            def _():
                wait_for(size(o, zz + 1), zsd.at[q])
        wait_for(size(o, 4), ysn.at[q])
        wait_for(size(o, 8), csn.at[q])

    NPC = GP + 3

    def lane(zz):
        return lan(zz * RW, RW)

    PQ, PA, PB = 0, GP + 1, GP + 2

    def kind(p):
        return p if isinstance(p, int) and (p == PQ or p > GP) else 1

    def w_ref(l, p, zz, half):
        if kind(p) == PQ:
            return WQ.at[l, sub(80 * half, 80), lane(zz)]
        if kind(p) == PA:
            return WO.at[l, sub(400 * half, 160), lane(zz)]
        if kind(p) == PB:
            return WO.at[l, sub(160 + 400 * half, 240), lane(zz)]
        return GU.at[l, half, sub(zz * RW + GR * (p - 1), GR), :]

    def w_send(l, kind_, m, mr=MR):
        r = mr * m
        for h in HOPS:
            t = lax.rem(z + h, 4)
            if kind_ == "q":
                p, src = PQ, WT.at[l, sub(SH * t + 80 * x + r, mr), :]
                dst = WQ.at[l, sub(80 * x + r, mr), lane(z)]
            elif kind_ == "g":
                p, src = 1 + r // GR, w_in.at[l, sub(r, mr), lan(RW + D * x + FB * t, FB)]
                dst = GU.at[l, x, sub(z * RW + r, mr), :]
            elif kind_ == "a":
                p, src = PA, w_out.at[l, sub(jnp.where(x == 0, SH * t, RW + FB * t + 240) + r, mr), :]
                dst = WO.at[l, sub(400 * x + r, mr), lane(z)]
            else:
                p, src = PB, w_out.at[l, sub(RW + FB * t + 400 * x + r, mr), :]
                dst = WO.at[l, sub(160 + 400 * x + r, mr), lane(z)]
            rcopy(src, dst, ws.at[l, p], wr.at[l, p, h - 1], zpeer[h - 1]).start()

    def rest_send(l, m):
        whole = -(-m // PM)
        for v in range(m, whole * PM):
            w_send(l, "g", v)
        for v in range(whole, GP):
            w_send(l, "g", v, GR)

    @jax.named_scope("w_forward")
    def w_forward(l, p):
        for h in HOPS:
            ref = w_ref(l, p, lax.rem(z - h + 4, 4), x)
            wait_for(ref, wr.at[l, p, h - 1])
            rcopy(ref, ref, xs.at[l, p], xr.at[l, p, h - 1], xpeer).start()

    def w_size(l, p):
        if kind(p) == PQ:
            return WQ.at[l, pl.ds(0, 80), pl.ds(0, 3 * RW)]
        if kind(p) == PA:
            return WO.at[l, pl.ds(0, 160), pl.ds(0, 3 * RW)]
        if kind(p) == PB:
            return WO.at[l, pl.ds(0, 240), pl.ds(0, 3 * RW)]
        return GU.at[l, 0, pl.ds(0, 3 * GR), :]

    @jax.named_scope("w_arrive")
    def w_arrive(l, p):
        for h in HOPS:
            wait_for(w_ref(l, p, 0, 0), xr.at[l, p, h - 1])

    def w_own(l):
        return [
            None,
            pltpu.make_async_copy(w_in.at[l, :, lan(RW + FB * z, FB)], GU.at[l, 0, sub(z * RW, RW), :], own.at[l, 1]),
            pltpu.make_async_copy(w_in.at[l, :, lan(RW + D + FB * z, FB)], GU.at[l, 1, sub(z * RW, RW), :], own.at[l, 2]),
            pltpu.make_async_copy(w_out.at[l, sub(SH * z, SH), :], WO.at[l, pl.ds(0, SH), lane(z)], own.at[l, 3]),
            pltpu.make_async_copy(w_out.at[l, sub(RW + FB * z, FB), :], WO.at[l, pl.ds(SH, FB), lane(z)], own.at[l, 4]),
        ]

    def seq_part(ref, n):
        return ref.at[n // SPC, :, lan(lax.rem(n, SPC) * CW, CW)]

    q_in = [pltpu.make_async_copy(w_in.at[l, :, pl.ds(0, RW)], GU.at[1, l, sub(z * RW, RW), :], own.at[l, 5]) for l in range(2)]
    for cp in q_in:
        cp.start()
    for b in range(5):
        blk = jnp.concatenate([kvw[l, :, LANES * b:LANES * (b + 1)].astype(F32) for l in range(2)], axis=0)
        EIN[HD * (b % 2):HD * (b % 2) + HD, LANES * (b // 2):LANES * (b // 2 + 1)] = blk.astype(BF)
    EIN[HD:, 2 * LANES:] = gn[...]
    ext(0, me)[...] = EIN[...]

    def put_own(ch):
        XA[ch, rows(me)] = seq_part(xin, ch)[...]
    loop(NT, put_own)
    gather_own(EIN, ext, 0, 0)
    for ch in range(NT):
        gather_own(seq_part(xin, ch), act, ch, NE)
    for cp in w_own(0)[1:]:
        cp.start()
    for l in range(2):
        q_in[l].wait()
        WT[l] = GU[1, l, sub(z * RW, RW), :].T
        WQ[l, :, lane(z)] = WT[l, sub(SH * z, SH), :]
    w_send(0, "q", 0, 80)
    for cp in w_own(1)[1:]:
        cp.start()
    done = 0
    for e in range(2 * NT):
        if e % NT == 0:
            gather_hop(ext, 0, 0, e // NT + 1)
        gather_hop(act, e % NT, NE, e // NT + 1)
        for v in range(S0[e]):
            w_send(0, "g", done)
            done += 1

    @jax.named_scope("unpack")
    def unpack():
        loop(NE, lambda ch: gather_end(ext, ch, 0))

        def shard(s):
            zz, cc = s // 4, lax.rem(s, 4)
            for b in range(5):
                lo = 128 * (b // 2)
                i = 16 * (lo // CW) + s
                blk = MT[i // 5, sub(lax.rem(i, 5) * SH + 80 * (b % 2), 80), lo % CW:lo % CW + 128].astype(F32)
                for l in range(2):
                    WKV[l, sub(48 * cc, 40), lan(zz * RW + 128 * b, 128)] = blk[40 * l:40 * l + 40].astype(BF)
            blk = MT[s // 5, sub(lax.rem(s, 5) * SH + HD, HD), 2 * LANES:EW].astype(F32)
            for l in range(2):
                for v in range(2):
                    GB[l, sub(s * SH + HD * v, HD), :] = jnp.broadcast_to(blk[:, l + 2 * v:l + 2 * v + 1], (HD, LANES)).astype(BF)
        loop(16, shard)
        for l in range(2):
            for cc in range(4):
                WKV[l, 48 * cc + 40:48 * cc + 48, :] = jnp.zeros((8, D), BF)

    BR = 32

    @jax.named_scope("norm")
    def norm(l, n):
        def fold(v):
            return v.reshape(BR // 8, 8, CW).sum(0)

        def load(i):
            return XA[n, sub(i * BR, BR), :].astype(F32)

        tot = lax.fori_loop(0, D // BR, lambda i, a: a + fold(load(i)), jnp.zeros((8, CW), F32), unroll=4)
        mean = jnp.sum(tot, axis=0, keepdims=True) / D

        def square(i, a):
            d = load(i) - mean
            return a + fold(d * d)
        var = jnp.sum(lax.fori_loop(0, D // BR, square, jnp.zeros((8, CW), F32), unroll=4), axis=0, keepdims=True) / D
        scale = lax.rsqrt(var + LN_EPS)

        def put(i, a):
            g = jnp.concatenate([GB[l, sub(i * BR, BR), :].astype(F32)] * (CW // 128), axis=1)
            XA[n, sub(i * BR, BR), :] = ((load(i) - mean) * scale * g).astype(BF)
            return a
        lax.fori_loop(0, D // BR, put, 0, unroll=4)

    def tok(n):
        return lan(n * CW, CW)

    @jax.named_scope("qkv")
    def qkv(l, n):
        pos = lan(lax.rem(n * CW, SEQ), CW)
        co, si = cos[:, pos], sin[:, pos]
        h = XA[n]
        kv = jnp.dot(WKV[l], h, preferred_element_type=F32).astype(BF).astype(F32)

        def rot(lo, hi):
            return jnp.concatenate([lo * co - hi * si, hi * co + lo * si], axis=0)
        KT[:, tok(n)] = rot(kv[0:40], kv[48:88]).astype(BF)
        VT[:, tok(n)] = jnp.concatenate([kv[96:136], kv[144:184]], axis=0).astype(BF)
        qq = jnp.dot(WQ[l], h, preferred_element_type=F32).astype(BF).astype(F32)
        for hd in range(2):
            QT[HD * hd:HD * hd + HD, tok(n)] = (rot(qq[HD * hd:HD * hd + HALF], qq[HD * hd + HALF:HD * hd + HD]) * HD ** -0.5).astype(BF)

    @jax.named_scope("attention")
    def attention(b):
        def body(hd):
            hr = sub(hd * HD, HD)
            for i in range(SEQ // QB):
                nk = QB * (i + 1)
                ks = lan(b * SEQ, nk)
                qs = lan(b * SEQ + QB * i, QB)
                s = dot_ta(KT[:, ks], QT[hr, qs])
                keep = lax.broadcasted_iota(jnp.int32, (QB, QB), 0) <= lax.broadcasted_iota(jnp.int32, (QB, QB), 1)
                last = jnp.where(keep, s[nk - QB:], -1e30)
                s = jnp.concatenate([s[:nk - QB], last], axis=0) if i else last
                e = jnp.exp(s - jnp.max(s, axis=0, keepdims=True))
                pr = (e * (1.0 / jnp.sum(e, axis=0, keepdims=True))).astype(BF)
                MT[b * (SEQ // CW) + QB * i // CW, hr, QB * i % CW:QB * i % CW + QB] = jnp.dot(VT[:, ks], pr, preferred_element_type=F32).astype(BF)
        loop(2, body)

    @jax.named_scope("gate_up")
    def gate_up(l, n):
        h = XA[n]
        g = dot_ta(GU[l, 0], h).astype(BF).astype(F32)
        u = dot_ta(GU[l, 1], h).astype(BF).astype(F32)
        MT[n, SH:SH + FB, :] = (g * lax.logistic(g) * u).astype(BF)

    def f(ref_value):
        return ref_value.astype(F32)

    NU = 4 * NT

    def unit(i):
        j = i // NT
        return jnp.where(j == 0, 3, jnp.where(j == 1, 0, jnp.where(j == 2, 2, 1))), lax.rem(i, NT)

    @jax.named_scope("red_a")
    def red_a(l, i):
        zz, n = unit(i)
        slot = lax.rem(i, SCN)

        @pl.when(i >= SCN)
        def _():
            wait_for(SC.at[slot], rcs.at[i - SCN])

        XA[n, sub(zz * RW, RW), :] = dot_ta(WO[l, :, lane(zz)], MT[n]).astype(BF)
        for yy in range(2):
            SC[slot, yy] = XA[n, rows(4 * zz + 2 * yy + 1 - k)]
        for yy in range(2):
            rcopy(SC.at[slot, yy], RC.at[n, 2 * zz + yy], rcs.at[i], rcr.at[i], cpeer).start()

    @jax.named_scope("red_b")
    def red_b(l, i):
        zz, n = unit(i)
        slot = lax.rem(i, SYN)
        wait_for(RC.at[n, pl.ds(2 * zz, 2)], rcr.at[i])

        @pl.when(i >= SYN)
        def _():
            wait_for(SY.at[slot], rys.at[i - SYN])

        SY[slot] = (f(XA[n, rows(4 * zz + 2 * (1 - y) + k)]) + f(RC[n, 2 * zz + 1 - y])).astype(BF)
        rcopy(SY.at[slot], RY.at[n, zz], rys.at[i], ryr.at[i], ypeer).start()

    def send_up(n, zz, i):
        rcopy(SZ.at[n, zz], RU.at[n, zz - 1], rsz.at[i], rzu.at[i], up).start()

    def send_down(n, zz, i):
        rcopy(SZ.at[n, zz], RD.at[n, zz], rsz.at[i], rzd.at[i], down).start()

    @jax.named_scope("red_c")
    def red_c(l, i):
        zz, n = unit(i)
        wait_for(RY.at[n, zz], ryr.at[i])
        SZ[n, zz] = (f(XA[n, rows(4 * zz + c)]) + f(RC[n, 2 * zz + y]) + f(RY[n, zz])).astype(BF)

        @pl.when((z == 0) & (zz > 0))
        def _():
            send_up(n, zz, i)

        @pl.when((z == 3) & (zz < 3))
        def _():
            send_down(n, zz, i)

    def relay_up(i):
        zz, n = unit(i)
        wait_for(RU.at[n, zz - 1], rzu.at[i])
        SZ[n, zz] = (f(SZ[n, zz]) + f(RU[n, zz - 1])).astype(BF)
        send_up(n, zz, i)

    def relay_down(i):
        zz, n = unit(i)
        wait_for(RD.at[n, zz], rzd.at[i])
        SZ[n, zz] = (f(SZ[n, zz]) + f(RD[n, zz])).astype(BF)
        send_down(n, zz, i)

    @jax.named_scope("red_d")
    def red_d(l, i):
        zz, _ = unit(i)

        @pl.when((z == 1) & (zz > 1))
        def _():
            relay_up(i)

        @pl.when((z == 2) & (zz < 2))
        def _():
            relay_down(i)

    @jax.named_scope("red_e")
    def red_e(l, i):
        zz, _ = unit(i)

        @pl.when((z == 2) & (zz > 2))
        def _():
            relay_up(i)

        @pl.when((z == 1) & (zz < 1))
        def _():
            relay_down(i)

    @jax.named_scope("red_f")
    def red_f(l, i):
        zz, n = unit(i)

        def finish(u):
            u = u.astype(BF)

            @pl.when(l == 0)
            def _():
                out = (f(seq_part(xin, n)[...]) + f(u)).astype(BF)
                XO[n] = out
                XA[n, rows(me)] = out
                gather_own(XO.at[n], act, n, NE)

            @pl.when(l == 1)
            def _():
                seq_part(yT, n)[...] = (f(XO[n]) + f(u)).astype(BF)

        @pl.when((z == 0) & (zz == 0))
        def _():
            wait_for(RD.at[n, 0], rzd.at[i])
            finish(f(SZ[n, 0]) + f(RD[n, 0]))

        @pl.when((z == 3) & (zz == 3))
        def _():
            wait_for(RU.at[n, 2], rzu.at[i])
            finish(f(SZ[n, 3]) + f(RU[n, 2]))

        for v in (1, 2):
            @pl.when((z == v) & (zz == v))
            def _():
                wait_for(RU.at[n, v - 1], rzu.at[i])
                wait_for(RD.at[n, v], rzd.at[i])
                finish(f(SZ[n, v]) + f(RU[n, v - 1]) + f(RD[n, v]))

        @pl.when(i >= NU - SCN)
        def _():
            wait_for(SC.at[0], rcs.at[i])

        @pl.when(i >= NU - SYN)
        def _():
            wait_for(SY.at[0], rys.at[i])

        @pl.when(zz != z)
        def _():
            wait_for(SZ.at[n, zz], rsz.at[i])

    shard = me

    def o_forward(l, j):
        zz = unit(NT * j)[0]
        h = lax.rem(z - zz + 4, 4)

        @pl.when(h > 0)
        def _():
            for p in (PA, PB):
                ref = w_ref(l, p, zz, x)
                wait_for(ref, wr.at[l, p, h - 1])
                rcopy(ref, ref, xs.at[l, p], xr.at[l, p, h - 1], xpeer).start()

    def o_arrive(l, j):
        zz = unit(NT * j)[0]
        h = lax.rem(z - zz + 4, 4)

        @pl.when(h > 0)
        def _():
            for p in (PA, PB):
                wait_for(w_ref(l, p, zz, 1 - x), xr.at[l, p, h - 1])

    def o_at(l, place):
        for ll in range(2):
            for at, cond in ((OEND[ll], (z == 0) | (z == 3)), (OMID[ll], (z == 1) | (z == 2))):
                if isinstance(place, int):
                    if place == at:
                        @pl.when((l == ll) & cond)
                        def _():
                            o_send(l)
                elif 0 < at <= NT:
                    @pl.when((l == ll) & cond & (place == at))
                    def _():
                        o_send(l)

    def o_send(l):
        w_send(l, "a", 0, 160)
        w_send(l, "b", 0, 240)

    def layer(l):
        @pl.when(l == 1)
        def _():
            done = RS0
            for e in range(2 * NT):
                gather_hop(act, e % NT, NE, e // NT + 1)
                for v in range(AG1[e]):
                    w_send(1, "g", done)
                    done += 1
                for p in EVENTS[e]:
                    w_forward(1, p)

        for ll, sent in enumerate((sum(S0), RS0 + sum(AG1))):
            @pl.when(l == ll)
            def _():
                rest_send(ll, sent)
        o_at(l, 0)

        def last(n):
            @pl.when(n < NT)
            def _():
                @pl.when((l == 0) & (n == 0))
                def _():
                    gather_hop(ext, 0, 0, len(HOPS))
                gather_hop(act, n, NE, len(HOPS))
                for v in range(NT):
                    if EVENTS[2 * NT + v]:
                        @pl.when((l == 1) & (n == v))
                        def _():
                            for p in EVENTS[2 * NT + v]:
                                w_forward(1, p)

                @pl.when((l == 0) & (n == 0))
                def _():
                    gather_cross(ext, 0, 0)
                gather_cross(act, n, NE)

            @pl.when(n > 0)
            def _():
                chunk(n - 1)

        def chunk(n):
            @pl.when(n == 0)
            def _():
                @pl.when(l == 0)
                def _():
                    unpack()
                    w_forward(0, PQ)
                for cp in w_own(l)[1:]:
                    cp.wait()
            gather_end(act, n, NE)
            norm(l, n)

            @pl.when(n == 0)
            def _():
                w_arrive(l, PQ)
            qkv(l, n)

            late = jnp.where(l == 0, 1, LATE) + n

            @pl.when(late <= GP)
            def _():
                w_forward(l, late)

            @pl.when(lax.rem(n, SPC) == SPC - 1)
            def _():
                attention(n // SPC)
            o_at(l, n + 1)
        loop(NT + 1, last)
        o_at(l, NT + 1)
        for b in range(2):
            off = lan(b * SEQ + LANES * (shard // 2), LANES)
            for v, ref in enumerate((KT, VT)):
                KVT[...] = ref[:, off].astype(F32).T
                kvo[l, v, b] = KVT[sub(64 * lax.rem(shard, 2), 64), :].astype(BF)
        fwd = jnp.where(l == 0, NT, min(GP, LATE - 1 + NT))
        loop(GP - fwd, lambda p: w_forward(l, fwd + 1 + p))
        o_at(l, NT + 2)
        loop(GP, lambda p: w_arrive(l, p + 1))
        o_forward(l, 0)
        gh = jnp.where(l == 0, GH0, GH1)
        loop(gh, lambda n: gate_up(l, n))

        def head(l, i):
            for j, u in enumerate(OF):
                @pl.when(i == u)
                def _():
                    o_forward(l, j + 1)

            @pl.when(lax.rem(i, NT) == 0)
            def _():
                o_arrive(l, i // NT)

            @pl.when((i >= gh) & (i < NT))
            def _():
                gate_up(l, i)
            red_a(l, i)


        def step(i):
            for lag, stage in zip((0, *LAGS), (head, red_b, red_d, red_e, red_c, red_f)):
                @pl.when((i >= lag) & (i < NU + lag))
                def _():
                    stage(l, i - lag)

            @pl.when(l == 0)
            def _():
                @pl.when(i == RQ)
                def _():
                    w_send(1, "q", 0, 80)

                @pl.when(i == RQ + 12)
                def _():
                    w_forward(1, PQ)

                for u, each in enumerate(SU):
                    if each:
                        @pl.when(i == u)
                        def _():
                            loop(each, lambda v: w_send(1, "g", sum(SU[:u]) + v))

                for u, ps in enumerate(UNITS):
                    if ps:
                        @pl.when(i == u)
                        def _():
                            for p in ps:
                                w_forward(1, p)
        loop(NU + LAGS[-1], step)

    loop(2, layer)

    for l in range(2):
        for p in range(NPC):
            wait_for(w_size(l, p), ws.at[l, p])
            wait_for(w_size(l, p), xs.at[l, p])


def solution(mesh):
    act_spec = P("dp", None, ("row", "col"))
    weight_spec = P(None, "row", "col")

    def device_fn(x_loc, gain_loc, w_in_loc, w_kv_loc, w_out_loc):
        gain = jnp.pad(jnp.transpose(gain_loc.reshape(2, 2, HD), (2, 1, 0)).reshape(HD, 4), ((0, 0), (0, LANES - 4)))
        NPC = GP + 3
        dma = pltpu.SemaphoreType.DMA
        hbm = pl.BlockSpec(memory_space=pl.ANY)
        vmem = pl.BlockSpec(memory_space=pltpu.VMEM)
        y_t, kvo = pl.pallas_call(
            kernel,
            out_shape=(jax.ShapeDtypeStruct((2, SH, SEQ), BF), jax.ShapeDtypeStruct((2, 2, 2, SEQ // 16, HD), BF)),
            in_specs=[vmem, vmem, vmem, hbm, hbm, vmem, vmem],
            out_specs=(vmem, vmem),
            scratch_shapes=[
                pltpu.VMEM((SH, EW), BF),
                pltpu.VMEM((LANES, HD), F32),
                pltpu.VMEM((2, RW, RW), BF),
                pltpu.VMEM((NT, D, CW), BF),
                pltpu.VMEM((2, 2, D, FB), BF),
                pltpu.VMEM((2, SH, D), BF),
                pltpu.VMEM((2, 192, D), BF),
                pltpu.VMEM((2, SH + FB, D), BF),
                pltpu.VMEM((2, D, 128), BF),
                pltpu.VMEM((NT, SH + FB, CW), BF),
                pltpu.VMEM((SH, T), BF),
                pltpu.VMEM((HD, T), BF),
                pltpu.VMEM((HD, T), BF),
                pltpu.VMEM((NT, SH, CW), BF),
                pltpu.VMEM((NT, 8, SH, CW), BF),
                pltpu.VMEM((NT, 4, SH, CW), BF),
                pltpu.VMEM((NT, 3, SH, CW), BF),
                pltpu.VMEM((NT, 3, SH, CW), BF),
                pltpu.VMEM((SCN, 2, SH, CW), BF),
                pltpu.VMEM((SYN, SH, CW), BF),
                pltpu.VMEM((NT, 4, SH, CW), BF),
                dma((NC,)), dma((NC,)), dma((NC,)), dma((NC,)),
                dma((NC, 2, 3)), dma((NC,)), dma((NC,)),
                dma((4 * NT,)), dma((4 * NT,)), dma((4 * NT,)), dma((4 * NT,)),
                dma((4 * NT,)), dma((4 * NT,)), dma((4 * NT,)),
                dma((2, NPC)), dma((2, NPC, 3)), dma((2, NPC)), dma((2, NPC, 3)),
                dma((2, 6)),
            ],
            compiler_params=pltpu.CompilerParams(collective_id=0, has_side_effects=True, vmem_limit_bytes=67043328),
        )(jnp.transpose(x_loc, (0, 2, 1)), jnp.transpose(w_kv_loc, (0, 2, 1)), gain, w_in_loc, w_out_loc, *rope_tables())
        return jnp.transpose(y_t, (0, 2, 1)), kvo

    return jax.shard_map(device_fn, mesh=mesh, in_specs=(act_spec, P(None, ("row", "col")), weight_spec, weight_spec, P(None, "col", "row")), out_specs=(act_spec, P(None, None, "dp", ("row", "col"), None)), check_vma=False)
```

```python
import jax
import jax.numpy as jnp
from jax import lax
from jax.experimental import pallas as pl
from jax.experimental.pallas import tpu as pltpu
from jax.sharding import PartitionSpec as P

BF = jnp.bfloat16
F32 = jnp.float32
MESH_ID = pl.DeviceIdType.MESH
LN_EPS = 1e-6

D = 2560
SH = 160
RW = 640
FB = 640
HD = 80
HALF = HD // 2
SEQ = 1024
T = 2 * SEQ
CW = 512
NT = T // CW
NE = 512 // CW
NC = NE + NT
SPC = SEQ // CW
GP = 8
GR = RW // GP
LANES = 128
EW = 3 * LANES
HOPS = (1, 2, 3)
QB = 256
SCN, SYN = 4, 6
MR = 16
LAGS = (1, 6, 12, 4, 18)
PM = GR // MR
S0 = (0,) * 4 + (2,) * 4
GH0, GH1 = 1, 3
OEND = (4, 0)
OMID = (5, 5)
OF = (0, 4, 8)
RQ = 1
SU = (0,) + (2,) * 10
AG1 = (0,) * len(S0)
UFW, EFW = 30, 12


def weight_plan():
    sent, when = 0, []
    for i, each in enumerate(SU):
        when += [i] * each
        sent += each
    units = [[] for _ in range(4 * NT + LAGS[-1])]
    events = [[] for _ in range(3 * NT)]
    late = list(range(1, GP + 1))
    ev = []
    for e in range(2 * NT):
        ev += [e] * AG1[e]
    for p in range(1, GP + 1):
        last = PM * p - 1
        if last < sent:
            if when[last] + UFW < len(units):
                units[when[last] + UFW].append(p)
                late.remove(p)
                continue
            e = max(0, when[last] + UFW - len(units))
        elif last < sent + len(ev):
            e = ev[last - sent] + EFW
        else:
            continue
        if e < 3 * NT:
            events[e].append(p)
            late.remove(p)
    return sent, units, events, late[0] if late else GP + 1


RS0, UNITS, EVENTS, LATE = weight_plan()


def rope_tables():
    inv_freq = 1.0 / (10000.0 ** (jnp.arange(HALF, dtype=F32) * 2.0 / HD))
    angles = inv_freq[:, None] * jnp.arange(SEQ).astype(F32)[None, :]
    return jnp.cos(angles), jnp.sin(angles)


def sub(start, size):
    return pl.ds(pl.multiple_of(start, 16), size)


def lan(start, size):
    return pl.ds(pl.multiple_of(start, LANES), size)


def dot_ta(a, b):
    return lax.dot_general(a, b, (((0,), (0,)), ((), ())), preferred_element_type=F32)


def kernel(xin, kvw, gn, w_in, w_out, cos, sin, yT, kvo, EIN, KVT, WT, XA, GU, WQ, WKV, WO, GB, MT, QT, KT, VT, XO, RC, RY, RU, RD, SC, SY, SZ,
           zsu, zsd, ysn, csn, zrc, yrc, crc, rcs, rcr, rys, ryr, rzu, rzd, rsz, ws, wr, xs, xr, own):
    x = lax.axis_index("dp")
    z = lax.axis_index("row")
    c = lax.axis_index("col")
    y, k = c // 2, lax.rem(c, 2)
    me = 4 * z + c
    up = (x, jnp.minimum(z + 1, 3), c)
    down = (x, jnp.maximum(z - 1, 0), c)
    ypeer = (x, z, lax.rem(c + 2, 4))
    cpeer = (x, z, c + 1 - 2 * k)
    xpeer = (1 - x, z, c)
    zpeer = [(x, lax.rem(z + h, 4), c) for h in HOPS]

    def rcopy(src, dst, ss, rs, dev):
        return pltpu.make_async_remote_copy(src_ref=src, dst_ref=dst, send_sem=ss, recv_sem=rs, device_id=dev, device_id_type=MESH_ID)

    def wait_for(ref, sem):
        pltpu.make_async_copy(ref, ref, sem).wait()

    def rows(s):
        return sub(s * SH, SH)

    def loop(n, body):
        def step(i, carry):
            body(i)
            return carry
        lax.fori_loop(0, n, step, 0)

    barrier = pltpu.get_barrier_semaphore()
    for dev in zpeer + [ypeer, cpeer, xpeer]:
        pl.semaphore_signal(barrier, inc=1, device_id=dev, device_id_type=MESH_ID)
    pl.semaphore_wait(barrier, 6)

    def act(ch, s):
        return XA.at[ch, rows(s)]

    def ext(ch, s):
        i = 16 * ch + s
        return MT.at[i // 5, rows(lax.rem(i, 5)), pl.ds(0, EW)]

    @jax.named_scope("gather_own")
    def size(o, shards):
        return XA.at[0, pl.ds(0, shards * SH), pl.ds(0, CW if o else EW)]

    @jax.named_scope("gather_own")
    def gather_own(src, buf, ch, o):
        q = ch + o
        dst = buf(ch, me)

        @pl.when(z < 3)
        def _():
            rcopy(src, dst, zsu.at[q], zrc.at[q, 0, 0], up).start()

        @pl.when(z > 0)
        def _():
            rcopy(src, dst, zsd.at[q], zrc.at[q, 1, 0], down).start()

        rcopy(src, dst, ysn.at[q], yrc.at[q], ypeer).start()
        rcopy(src, dst, csn.at[q], crc.at[q], cpeer).start()

    @jax.named_scope("gather_hop")
    def gather_hop(buf, ch, o, hop):
        q = ch + o

        @pl.when(z - hop >= 0)
        def _():
            ref = buf(ch, jnp.maximum(me - 4 * hop, 0))
            wait_for(ref, zrc.at[q, 0, hop - 1])
            if hop < 3:
                @pl.when(z < 3)
                def _():
                    rcopy(ref, ref, zsu.at[q], zrc.at[q, 0, hop], up).start()
            rcopy(ref, ref, ysn.at[q], yrc.at[q], ypeer).start()
            rcopy(ref, ref, csn.at[q], crc.at[q], cpeer).start()

        @pl.when(z + hop <= 3)
        def _():
            ref = buf(ch, jnp.minimum(me + 4 * hop, 15))
            wait_for(ref, zrc.at[q, 1, hop - 1])
            if hop < 3:
                @pl.when(z > 0)
                def _():
                    rcopy(ref, ref, zsd.at[q], zrc.at[q, 1, hop], down).start()
            rcopy(ref, ref, ysn.at[q], yrc.at[q], ypeer).start()
            rcopy(ref, ref, csn.at[q], crc.at[q], cpeer).start()

    @jax.named_scope("gather_cross")
    def gather_cross(buf, ch, o):
        q = ch + o
        wait_for(size(o, 4), yrc.at[q])
        for zz in range(4):
            ref = buf(ch, 4 * zz + lax.rem(c + 2, 4))
            rcopy(ref, ref, csn.at[q], crc.at[q], cpeer).start()

    @jax.named_scope("gather_end")
    def gather_end(buf, ch, o):
        q = ch + o
        wait_for(size(o, 8), crc.at[q])
        for zz in range(3):
            @pl.when(z == zz)
            def _():
                wait_for(size(o, zz + 1), zsu.at[q])

            @pl.when(z == 3 - zz)
            def _():
                wait_for(size(o, zz + 1), zsd.at[q])
        wait_for(size(o, 4), ysn.at[q])
        wait_for(size(o, 8), csn.at[q])

    NPC = GP + 3

    def lane(zz):
        return lan(zz * RW, RW)

    PQ, PA, PB = 0, GP + 1, GP + 2

    def kind(p):
        return p if isinstance(p, int) and (p == PQ or p > GP) else 1

    def w_ref(l, p, zz, half):
        if kind(p) == PQ:
            return WQ.at[l, sub(80 * half, 80), lane(zz)]
        if kind(p) == PA:
            return WO.at[l, sub(400 * half, 160), lane(zz)]
        if kind(p) == PB:
            return WO.at[l, sub(160 + 400 * half, 240), lane(zz)]
        return GU.at[l, half, sub(zz * RW + GR * (p - 1), GR), :]

    def w_send(l, kind_, m, mr=MR):
        r = mr * m
        for h in HOPS:
            t = lax.rem(z + h, 4)
            if kind_ == "q":
                p, src = PQ, WT.at[l, sub(SH * t + 80 * x + r, mr), :]
                dst = WQ.at[l, sub(80 * x + r, mr), lane(z)]
            elif kind_ == "g":
                p, src = 1 + r // GR, w_in.at[l, sub(r, mr), lan(RW + D * x + FB * t, FB)]
                dst = GU.at[l, x, sub(z * RW + r, mr), :]
            elif kind_ == "a":
                p, src = PA, w_out.at[l, sub(jnp.where(x == 0, SH * t, RW + FB * t + 240) + r, mr), :]
                dst = WO.at[l, sub(400 * x + r, mr), lane(z)]
            else:
                p, src = PB, w_out.at[l, sub(RW + FB * t + 400 * x + r, mr), :]
                dst = WO.at[l, sub(160 + 400 * x + r, mr), lane(z)]
            rcopy(src, dst, ws.at[l, p], wr.at[l, p, h - 1], zpeer[h - 1]).start()

    def rest_send(l, m):
        whole = -(-m // PM)
        for v in range(m, whole * PM):
            w_send(l, "g", v)
        for v in range(whole, GP):
            w_send(l, "g", v, GR)

    @jax.named_scope("w_forward")
    def w_forward(l, p):
        for h in HOPS:
            ref = w_ref(l, p, lax.rem(z - h + 4, 4), x)
            wait_for(ref, wr.at[l, p, h - 1])
            rcopy(ref, ref, xs.at[l, p], xr.at[l, p, h - 1], xpeer).start()

    def w_size(l, p):
        if kind(p) == PQ:
            return WQ.at[l, pl.ds(0, 80), pl.ds(0, 3 * RW)]
        if kind(p) == PA:
            return WO.at[l, pl.ds(0, 160), pl.ds(0, 3 * RW)]
        if kind(p) == PB:
            return WO.at[l, pl.ds(0, 240), pl.ds(0, 3 * RW)]
        return GU.at[l, 0, pl.ds(0, 3 * GR), :]

    @jax.named_scope("w_arrive")
    def w_arrive(l, p):
        for h in HOPS:
            wait_for(w_ref(l, p, 0, 0), xr.at[l, p, h - 1])

    def w_own(l):
        return [
            None,
            pltpu.make_async_copy(w_in.at[l, :, lan(RW + FB * z, FB)], GU.at[l, 0, sub(z * RW, RW), :], own.at[l, 1]),
            pltpu.make_async_copy(w_in.at[l, :, lan(RW + D + FB * z, FB)], GU.at[l, 1, sub(z * RW, RW), :], own.at[l, 2]),
            pltpu.make_async_copy(w_out.at[l, sub(SH * z, SH), :], WO.at[l, pl.ds(0, SH), lane(z)], own.at[l, 3]),
            pltpu.make_async_copy(w_out.at[l, sub(RW + FB * z, FB), :], WO.at[l, pl.ds(SH, FB), lane(z)], own.at[l, 4]),
        ]

    def seq_part(ref, n):
        return ref.at[n // SPC, :, lan(lax.rem(n, SPC) * CW, CW)]

    q_in = [pltpu.make_async_copy(w_in.at[l, :, pl.ds(0, RW)], GU.at[1, l, sub(z * RW, RW), :], own.at[l, 5]) for l in range(2)]
    for cp in q_in:
        cp.start()
    for b in range(5):
        blk = jnp.concatenate([kvw[l, :, LANES * b:LANES * (b + 1)].astype(F32) for l in range(2)], axis=0)
        EIN[HD * (b % 2):HD * (b % 2) + HD, LANES * (b // 2):LANES * (b // 2 + 1)] = blk.astype(BF)
    EIN[HD:, 2 * LANES:] = gn[...]
    ext(0, me)[...] = EIN[...]

    def put_own(ch):
        XA[ch, rows(me)] = seq_part(xin, ch)[...]
    loop(NT, put_own)
    gather_own(EIN, ext, 0, 0)
    for ch in range(NT):
        gather_own(seq_part(xin, ch), act, ch, NE)
    for cp in w_own(0)[1:]:
        cp.start()
    for l in range(2):
        q_in[l].wait()
        WT[l] = GU[1, l, sub(z * RW, RW), :].T
        WQ[l, :, lane(z)] = WT[l, sub(SH * z, SH), :]
    w_send(0, "q", 0, 80)
    for cp in w_own(1)[1:]:
        cp.start()
    done = 0
    for e in range(2 * NT):
        if e % NT == 0:
            gather_hop(ext, 0, 0, e // NT + 1)
        gather_hop(act, e % NT, NE, e // NT + 1)
        for v in range(S0[e]):
            w_send(0, "g", done)
            done += 1

    @jax.named_scope("unpack")
    def unpack():
        loop(NE, lambda ch: gather_end(ext, ch, 0))

        def shard(s):
            zz, cc = s // 4, lax.rem(s, 4)
            for b in range(5):
                lo = 128 * (b // 2)
                i = 16 * (lo // CW) + s
                blk = MT[i // 5, sub(lax.rem(i, 5) * SH + 80 * (b % 2), 80), lo % CW:lo % CW + 128].astype(F32)
                for l in range(2):
                    WKV[l, sub(48 * cc, 40), lan(zz * RW + 128 * b, 128)] = blk[40 * l:40 * l + 40].astype(BF)
            blk = MT[s // 5, sub(lax.rem(s, 5) * SH + HD, HD), 2 * LANES:EW].astype(F32)
            for l in range(2):
                for v in range(2):
                    GB[l, sub(s * SH + HD * v, HD), :] = jnp.broadcast_to(blk[:, l + 2 * v:l + 2 * v + 1], (HD, LANES)).astype(BF)
        loop(16, shard)
        for l in range(2):
            for cc in range(4):
                WKV[l, 48 * cc + 40:48 * cc + 48, :] = jnp.zeros((8, D), BF)

    BR = 32

    @jax.named_scope("norm")
    def norm(l, n):
        def fold(v):
            return v.reshape(BR // 8, 8, CW).sum(0)

        def load(i):
            return XA[n, sub(i * BR, BR), :].astype(F32)

        tot = lax.fori_loop(0, D // BR, lambda i, a: a + fold(load(i)), jnp.zeros((8, CW), F32), unroll=4)
        mean = jnp.sum(tot, axis=0, keepdims=True) / D

        def square(i, a):
            d = load(i) - mean
            return a + fold(d * d)
        var = jnp.sum(lax.fori_loop(0, D // BR, square, jnp.zeros((8, CW), F32), unroll=4), axis=0, keepdims=True) / D
        scale = lax.rsqrt(var + LN_EPS)

        def put(i, a):
            g = jnp.concatenate([GB[l, sub(i * BR, BR), :].astype(F32)] * (CW // 128), axis=1)
            XA[n, sub(i * BR, BR), :] = ((load(i) - mean) * scale * g).astype(BF)
            return a
        lax.fori_loop(0, D // BR, put, 0, unroll=4)

    def tok(n):
        return lan(n * CW, CW)

    @jax.named_scope("qkv")
    def qkv(l, n):
        pos = lan(lax.rem(n * CW, SEQ), CW)
        co, si = cos[:, pos], sin[:, pos]
        h = XA[n]
        kv = jnp.dot(WKV[l], h, preferred_element_type=F32).astype(BF).astype(F32)

        def rot(lo, hi):
            return jnp.concatenate([lo * co - hi * si, hi * co + lo * si], axis=0)
        KT[:, tok(n)] = rot(kv[0:40], kv[48:88]).astype(BF)
        VT[:, tok(n)] = jnp.concatenate([kv[96:136], kv[144:184]], axis=0).astype(BF)
        qq = jnp.dot(WQ[l], h, preferred_element_type=F32).astype(BF).astype(F32)
        for hd in range(2):
            QT[HD * hd:HD * hd + HD, tok(n)] = (rot(qq[HD * hd:HD * hd + HALF], qq[HD * hd + HALF:HD * hd + HD]) * HD ** -0.5).astype(BF)

    @jax.named_scope("attention")
    def attention(b):
        def body(hd):
            hr = sub(hd * HD, HD)
            for i in range(SEQ // QB):
                nk = QB * (i + 1)
                ks = lan(b * SEQ, nk)
                qs = lan(b * SEQ + QB * i, QB)
                s = dot_ta(KT[:, ks], QT[hr, qs])
                keep = lax.broadcasted_iota(jnp.int32, (QB, QB), 0) <= lax.broadcasted_iota(jnp.int32, (QB, QB), 1)
                last = jnp.where(keep, s[nk - QB:], -1e30)
                s = jnp.concatenate([s[:nk - QB], last], axis=0) if i else last
                e = jnp.exp(s - jnp.max(s, axis=0, keepdims=True))
                pr = (e * (1.0 / jnp.sum(e, axis=0, keepdims=True))).astype(BF)
                MT[b * (SEQ // CW) + QB * i // CW, hr, QB * i % CW:QB * i % CW + QB] = jnp.dot(VT[:, ks], pr, preferred_element_type=F32).astype(BF)
        loop(2, body)

    @jax.named_scope("gate_up")
    def gate_up(l, n):
        h = XA[n]
        g = dot_ta(GU[l, 0], h).astype(BF).astype(F32)
        u = dot_ta(GU[l, 1], h).astype(BF).astype(F32)
        MT[n, SH:SH + FB, :] = (g * lax.logistic(g) * u).astype(BF)

    def f(ref_value):
        return ref_value.astype(F32)

    NU = 4 * NT

    def unit(i):
        j = i // NT
        return jnp.where(j == 0, 3, jnp.where(j == 1, 0, jnp.where(j == 2, 2, 1))), lax.rem(i, NT)

    @jax.named_scope("red_a")
    def red_a(l, i):
        zz, n = unit(i)
        slot = lax.rem(i, SCN)

        @pl.when(i >= SCN)
        def _():
            wait_for(SC.at[slot], rcs.at[i - SCN])

        XA[n, sub(zz * RW, RW), :] = dot_ta(WO[l, :, lane(zz)], MT[n]).astype(BF)
        for yy in range(2):
            SC[slot, yy] = XA[n, rows(4 * zz + 2 * yy + 1 - k)]
        for yy in range(2):
            rcopy(SC.at[slot, yy], RC.at[n, 2 * zz + yy], rcs.at[i], rcr.at[i], cpeer).start()

    @jax.named_scope("red_b")
    def red_b(l, i):
        zz, n = unit(i)
        slot = lax.rem(i, SYN)
        wait_for(RC.at[n, pl.ds(2 * zz, 2)], rcr.at[i])

        @pl.when(i >= SYN)
        def _():
            wait_for(SY.at[slot], rys.at[i - SYN])

        SY[slot] = (f(XA[n, rows(4 * zz + 2 * (1 - y) + k)]) + f(RC[n, 2 * zz + 1 - y])).astype(BF)
        rcopy(SY.at[slot], RY.at[n, zz], rys.at[i], ryr.at[i], ypeer).start()

    def send_up(n, zz, i):
        rcopy(SZ.at[n, zz], RU.at[n, zz - 1], rsz.at[i], rzu.at[i], up).start()

    def send_down(n, zz, i):
        rcopy(SZ.at[n, zz], RD.at[n, zz], rsz.at[i], rzd.at[i], down).start()

    @jax.named_scope("red_c")
    def red_c(l, i):
        zz, n = unit(i)
        wait_for(RY.at[n, zz], ryr.at[i])
        SZ[n, zz] = (f(XA[n, rows(4 * zz + c)]) + f(RC[n, 2 * zz + y]) + f(RY[n, zz])).astype(BF)

        @pl.when((z == 0) & (zz > 0))
        def _():
            send_up(n, zz, i)

        @pl.when((z == 3) & (zz < 3))
        def _():
            send_down(n, zz, i)

    def relay_up(i):
        zz, n = unit(i)
        wait_for(RU.at[n, zz - 1], rzu.at[i])
        SZ[n, zz] = (f(SZ[n, zz]) + f(RU[n, zz - 1])).astype(BF)
        send_up(n, zz, i)

    def relay_down(i):
        zz, n = unit(i)
        wait_for(RD.at[n, zz], rzd.at[i])
        SZ[n, zz] = (f(SZ[n, zz]) + f(RD[n, zz])).astype(BF)
        send_down(n, zz, i)

    @jax.named_scope("red_d")
    def red_d(l, i):
        zz, _ = unit(i)

        @pl.when((z == 1) & (zz > 1))
        def _():
            relay_up(i)

        @pl.when((z == 2) & (zz < 2))
        def _():
            relay_down(i)

    @jax.named_scope("red_e")
    def red_e(l, i):
        zz, _ = unit(i)

        @pl.when((z == 2) & (zz > 2))
        def _():
            relay_up(i)

        @pl.when((z == 1) & (zz < 1))
        def _():
            relay_down(i)

    @jax.named_scope("red_f")
    def red_f(l, i):
        zz, n = unit(i)

        def finish(u):
            u = u.astype(BF)

            @pl.when(l == 0)
            def _():
                out = (f(seq_part(xin, n)[...]) + f(u)).astype(BF)
                XO[n] = out
                XA[n, rows(me)] = out
                gather_own(XO.at[n], act, n, NE)

            @pl.when(l == 1)
            def _():
                seq_part(yT, n)[...] = (f(XO[n]) + f(u)).astype(BF)

        @pl.when((z == 0) & (zz == 0))
        def _():
            wait_for(RD.at[n, 0], rzd.at[i])
            finish(f(SZ[n, 0]) + f(RD[n, 0]))

        @pl.when((z == 3) & (zz == 3))
        def _():
            wait_for(RU.at[n, 2], rzu.at[i])
            finish(f(SZ[n, 3]) + f(RU[n, 2]))

        for v in (1, 2):
            @pl.when((z == v) & (zz == v))
            def _():
                wait_for(RU.at[n, v - 1], rzu.at[i])
                wait_for(RD.at[n, v], rzd.at[i])
                finish(f(SZ[n, v]) + f(RU[n, v - 1]) + f(RD[n, v]))

        @pl.when(i >= NU - SCN)
        def _():
            wait_for(SC.at[0], rcs.at[i])

        @pl.when(i >= NU - SYN)
        def _():
            wait_for(SY.at[0], rys.at[i])

        @pl.when(zz != z)
        def _():
            wait_for(SZ.at[n, zz], rsz.at[i])

    shard = me

    def o_forward(l, j):
        zz = unit(NT * j)[0]
        h = lax.rem(z - zz + 4, 4)

        @pl.when(h > 0)
        def _():
            for p in (PA, PB):
                ref = w_ref(l, p, zz, x)
                wait_for(ref, wr.at[l, p, h - 1])
                rcopy(ref, ref, xs.at[l, p], xr.at[l, p, h - 1], xpeer).start()

    def o_arrive(l, j):
        zz = unit(NT * j)[0]
        h = lax.rem(z - zz + 4, 4)

        @pl.when(h > 0)
        def _():
            for p in (PA, PB):
                wait_for(w_ref(l, p, zz, 1 - x), xr.at[l, p, h - 1])

    def o_at(l, place):
        for ll in range(2):
            for at, cond in ((OEND[ll], (z == 0) | (z == 3)), (OMID[ll], (z == 1) | (z == 2))):
                if isinstance(place, int):
                    if place == at:
                        @pl.when((l == ll) & cond)
                        def _():
                            o_send(l)
                elif 0 < at <= NT:
                    @pl.when((l == ll) & cond & (place == at))
                    def _():
                        o_send(l)

    def o_send(l):
        w_send(l, "a", 0, 160)
        w_send(l, "b", 0, 240)

    def layer(l):
        @pl.when(l == 1)
        def _():
            done = RS0
            for e in range(2 * NT):
                gather_hop(act, e % NT, NE, e // NT + 1)
                for v in range(AG1[e]):
                    w_send(1, "g", done)
                    done += 1
                for p in EVENTS[e]:
                    w_forward(1, p)

        for ll, sent in enumerate((sum(S0), RS0 + sum(AG1))):
            @pl.when(l == ll)
            def _():
                rest_send(ll, sent)
        o_at(l, 0)

        def last(n):
            @pl.when(n < NT)
            def _():
                @pl.when((l == 0) & (n == 0))
                def _():
                    gather_hop(ext, 0, 0, len(HOPS))
                gather_hop(act, n, NE, len(HOPS))
                for v in range(NT):
                    if EVENTS[2 * NT + v]:
                        @pl.when((l == 1) & (n == v))
                        def _():
                            for p in EVENTS[2 * NT + v]:
                                w_forward(1, p)

                @pl.when((l == 0) & (n == 0))
                def _():
                    gather_cross(ext, 0, 0)
                gather_cross(act, n, NE)

            @pl.when(n > 0)
            def _():
                chunk(n - 1)

        def chunk(n):
            @pl.when(n == 0)
            def _():
                @pl.when(l == 0)
                def _():
                    unpack()
                    w_forward(0, PQ)
                for cp in w_own(l)[1:]:
                    cp.wait()
            gather_end(act, n, NE)
            norm(l, n)

            @pl.when(n == 0)
            def _():
                w_arrive(l, PQ)
            qkv(l, n)

            late = jnp.where(l == 0, 1, LATE) + n

            @pl.when(late <= GP)
            def _():
                w_forward(l, late)

            @pl.when(lax.rem(n, SPC) == SPC - 1)
            def _():
                attention(n // SPC)
            o_at(l, n + 1)
        loop(NT + 1, last)
        o_at(l, NT + 1)
        for b in range(2):
            off = lan(b * SEQ + LANES * (shard // 2), LANES)
            for v, ref in enumerate((KT, VT)):
                KVT[...] = ref[:, off].astype(F32).T
                kvo[l, v, b] = KVT[sub(64 * lax.rem(shard, 2), 64), :].astype(BF)
        fwd = jnp.where(l == 0, NT, min(GP, LATE - 1 + NT))
        loop(GP - fwd, lambda p: w_forward(l, fwd + 1 + p))
        o_at(l, NT + 2)
        loop(GP, lambda p: w_arrive(l, p + 1))
        o_forward(l, 0)
        gh = jnp.where(l == 0, GH0, GH1)
        loop(gh, lambda n: gate_up(l, n))

        def head(l, i):
            for j, u in enumerate(OF):
                @pl.when(i == u)
                def _():
                    o_forward(l, j + 1)

            @pl.when(lax.rem(i, NT) == 0)
            def _():
                o_arrive(l, i // NT)

            @pl.when((i >= gh) & (i < NT))
            def _():
                gate_up(l, i)
            red_a(l, i)


        def step(i):
            for lag, stage in zip((0, *LAGS), (head, red_b, red_d, red_e, red_c, red_f)):
                @pl.when((i >= lag) & (i < NU + lag))
                def _():
                    stage(l, i - lag)

            @pl.when(l == 0)
            def _():
                @pl.when(i == RQ)
                def _():
                    w_send(1, "q", 0, 80)

                @pl.when(i == RQ + 12)
                def _():
                    w_forward(1, PQ)

                for u, each in enumerate(SU):
                    if each:
                        @pl.when(i == u)
                        def _():
                            loop(each, lambda v: w_send(1, "g", sum(SU[:u]) + v))

                for u, ps in enumerate(UNITS):
                    if ps:
                        @pl.when(i == u)
                        def _():
                            for p in ps:
                                w_forward(1, p)
        loop(NU + LAGS[-1], step)

    loop(2, layer)

    for l in range(2):
        for p in range(NPC):
            wait_for(w_size(l, p), ws.at[l, p])
            wait_for(w_size(l, p), xs.at[l, p])


def solution(mesh):
    act_spec = P("dp", None, ("row", "col"))
    weight_spec = P(None, "row", "col")

    def device_fn(x_loc, gain_loc, w_in_loc, w_kv_loc, w_out_loc):
        gain = jnp.pad(jnp.transpose(gain_loc.reshape(2, 2, HD), (2, 1, 0)).reshape(HD, 4), ((0, 0), (0, LANES - 4)))
        NPC = GP + 3
        dma = pltpu.SemaphoreType.DMA
        hbm = pl.BlockSpec(memory_space=pl.ANY)
        vmem = pl.BlockSpec(memory_space=pltpu.VMEM)
        y_t, kvo = pl.pallas_call(
            kernel,
            out_shape=(jax.ShapeDtypeStruct((2, SH, SEQ), BF), jax.ShapeDtypeStruct((2, 2, 2, SEQ // 16, HD), BF)),
            in_specs=[vmem, vmem, vmem, hbm, hbm, vmem, vmem],
            out_specs=(vmem, vmem),
            scratch_shapes=[
                pltpu.VMEM((SH, EW), BF),
                pltpu.VMEM((LANES, HD), F32),
                pltpu.VMEM((2, RW, RW), BF),
                pltpu.VMEM((NT, D, CW), BF),
                pltpu.VMEM((2, 2, D, FB), BF),
                pltpu.VMEM((2, SH, D), BF),
                pltpu.VMEM((2, 192, D), BF),
                pltpu.VMEM((2, SH + FB, D), BF),
                pltpu.VMEM((2, D, 128), BF),
                pltpu.VMEM((NT, SH + FB, CW), BF),
                pltpu.VMEM((SH, T), BF),
                pltpu.VMEM((HD, T), BF),
                pltpu.VMEM((HD, T), BF),
                pltpu.VMEM((NT, SH, CW), BF),
                pltpu.VMEM((NT, 8, SH, CW), BF),
                pltpu.VMEM((NT, 4, SH, CW), BF),
                pltpu.VMEM((NT, 3, SH, CW), BF),
                pltpu.VMEM((NT, 3, SH, CW), BF),
                pltpu.VMEM((SCN, 2, SH, CW), BF),
                pltpu.VMEM((SYN, SH, CW), BF),
                pltpu.VMEM((NT, 4, SH, CW), BF),
                dma((NC,)), dma((NC,)), dma((NC,)), dma((NC,)),
                dma((NC, 2, 3)), dma((NC,)), dma((NC,)),
                dma((4 * NT,)), dma((4 * NT,)), dma((4 * NT,)), dma((4 * NT,)),
                dma((4 * NT,)), dma((4 * NT,)), dma((4 * NT,)),
                dma((2, NPC)), dma((2, NPC, 3)), dma((2, NPC)), dma((2, NPC, 3)),
                dma((2, 6)),
            ],
            compiler_params=pltpu.CompilerParams(collective_id=0, has_side_effects=True, vmem_limit_bytes=67043328),
        )(jnp.transpose(x_loc, (0, 2, 1)), jnp.transpose(w_kv_loc, (0, 2, 1)), gain, w_in_loc, w_out_loc, *rope_tables())
        return jnp.transpose(y_t, (0, 2, 1)), kvo

    return jax.shard_map(device_fn, mesh=mesh, in_specs=(act_spec, P(None, ("row", "col")), weight_spec, weight_spec, P(None, "col", "row")), out_specs=(act_spec, P(None, None, "dp", ("row", "col"), None)), check_vma=False)
```
